32 devices in a mesh: gx: 4 (over y, x), gy: 4 (over z), gz: 2 (over core).
Axes of the slice: x: 2, y: 2, z: 4, core: 2. Of those that a mesh axis runs over, the one named last changes fastest.
Arguments:
- density: float32 [32, 256, 256], P('gx', 'gy', 'gz'), may hold values from 0.2 to 6, as said below
- momentum: float32 [3, 32, 256, 256], P(None, 'gx', 'gy', 'gz'), may hold values from -6 to 6
- energy: float32 [32, 256, 256], P('gx', 'gy', 'gz'), may hold values from 0.2 to 6, as said below
- displacement: int32 [3, 32, 256, 256], P(None, 'gx', 'gy', 'gz'), may hold values from -255 to 255
- flags: int32 [6], replicated, may hold values from 0 to 1
Outputs:
- new_density: float32 [32, 256, 256], P('gx', 'gy', 'gz')
- new_momentum: float32 [3, 32, 256, 256], P(None, 'gx', 'gy', 'gz')
- new_energy: float32 [32, 256, 256], P('gx', 'gy', 'gz')
- totals: float32 [2], replicated
The draws below stay inside these ranges and needn't reach their ends.
Inputs may be any that keep to these rules, and one draw needn't show every extreme that they name: density is positive. energy is positive.
All inputs are finite; a program needn't handle non-finite values.
Results may differ from the reference program's by a relative error of at most 0.0003.
Values sent between devices are 32-bit elements; how exact they have to be, the bound alone decides.
A program may use at most 64 MiB of HBM per device.

```python
import jax
import jax.numpy as jnp
from jax import lax

NX = 32
NY = 256
NZ = 256


def rising_field(key):
    uniform_part = jax.random.uniform(key, (NX, NY, NZ), jnp.float32)
    ramp = 1.0 + 2.0 * jnp.arange(NX, dtype=jnp.float32)[:, None, None] / NX
    base = 0.5 + uniform_part
    return base * ramp


def draw_density(key, part):
    return rising_field(jax.random.fold_in(key, 11))


def draw_energy(key, part):
    return rising_field(jax.random.fold_in(key, 23))


def with_ends(entries, own_key, least, largest):
    shape = entries.shape
    spot = [jax.random.randint(jax.random.fold_in(own_key, axis), (), 0, shape[axis]) for axis in range(len(shape))]
    entries = entries.at[tuple(spot)].set(least)
    longest = shape.index(max(shape))
    spot[longest] = (spot[longest] + 1) % shape[longest]
    return entries.at[tuple(spot)].set(largest)


def shard_levels(key, shape, cuts, least, largest):
    level = 1.0
    for position, shards_of in cuts:
        draws = jax.random.uniform(jax.random.fold_in(jax.random.fold_in(key, 6), position), (shards_of,), jnp.float32, least / len(cuts), largest / len(cuts))
        level = level * jnp.repeat(jnp.exp(draws), shape[position] // shards_of).reshape((-1,) + (1,) * (len(shape) - 1 - position))
    return level


def centred(key, extent, spread, bound, split=(), held_as=jnp.bfloat16):
    level = shard_levels(key, extent, split, -0.22, 0.18) if split else 1.0
    values = jax.random.normal(key, extent, jnp.float32) * spread * level
    return jnp.minimum(jnp.maximum(values, -bound), bound).astype(held_as)


def setup_inputs(seed: int = 0) -> dict:
    streams_of = jax.random.split(jax.random.key(seed), 6)
    return {
        "density": draw_density(jax.random.fold_in(streams_of[5], 71), 0),
        "momentum": centred(streams_of[1], (3, NX, NY, NZ), 1.0, 6.0, ((1, 4), (2, 4), (3, 2)), jnp.float32),
        "energy": draw_energy(jax.random.fold_in(streams_of[5], 71), 0),
        "displacement": with_ends(jax.random.randint(streams_of[3], (3, NX, NY, NZ), -255, 256), jax.random.fold_in(streams_of[3], 1), -255, 255).astype(jnp.int32),
        "flags": with_ends(jax.random.randint(streams_of[4], (6,), 0, 2), jax.random.fold_in(streams_of[4], 1), 0, 1).astype(jnp.int32),
    }


def minmod(left_diff, right_diff):
    return 0.5 * (jnp.sign(left_diff) + jnp.sign(right_diff)) * jnp.minimum(jnp.abs(left_diff), jnp.abs(right_diff))


def flux_change(padded, face_rows, along):
    total_len = padded.shape[along]
    upper_cells = lax.slice_in_dim(padded, 2, total_len, axis=along)
    middle = lax.slice_in_dim(padded, 1, total_len - 1, axis=along)
    lower_cells = lax.slice_in_dim(padded, 0, total_len - 2, axis=along)
    slopes = minmod(upper_cells - middle, middle - lower_cells)
    k = total_len - 2
    low_val = lax.slice_in_dim(middle, 0, k - 1, axis=along)
    high_val = lax.slice_in_dim(middle, 1, k, axis=along)
    low_slope = lax.slice_in_dim(slopes, 0, k - 1, axis=along)
    high_slope = lax.slice_in_dim(slopes, 1, k, axis=along)
    fluxes = face_rows * jnp.where(face_rows > 0, low_val + 0.5 * (1.0 - face_rows) * low_slope,
                                   high_val - 0.5 * (1.0 + face_rows) * high_slope)
    m = k - 1
    return lax.slice_in_dim(fluxes, 0, m - 1, axis=along) - lax.slice_in_dim(fluxes, 1, m, axis=along)


def axis_change(values, face_speed, low_flag, high_flag, along):
    n = values.shape[along]
    first_cell = lax.slice_in_dim(values, 0, 1, axis=along)
    last_cell = lax.slice_in_dim(values, n - 1, n, axis=along)
    padded = jnp.concatenate([first_cell, first_cell, values, last_cell, last_cell], along)
    face_rows = jnp.concatenate([lax.slice_in_dim(face_speed, 0, 1, axis=along) * low_flag,
                                 lax.slice_in_dim(face_speed, 1, n, axis=along),
                                 lax.slice_in_dim(face_speed, n - 1, n, axis=along) * high_flag], along)
    return flux_change(padded, face_rows, along)


def reference(density, momentum, energy, displacement, flags):
    face_speed = displacement.astype(jnp.float32) / 256.0
    flag_open = flags.astype(jnp.float32)

    def remap_field(values):
        updated = values
        for along in range(3):
            updated = updated + axis_change(values, face_speed[along], flag_open[2 * along], flag_open[2 * along + 1], along)
        return updated

    new_density = remap_field(density)
    new_momentum = jnp.stack([remap_field(momentum[comp]) for comp in range(3)])
    new_energy = remap_field(energy)
    cell_total = float(NX * NY * NZ)
    totals = jnp.stack([jnp.sum(new_density), jnp.sum(new_energy)]) / cell_total
    return new_density, new_momentum, new_energy, totals
```

```python
import functools

import jax
import jax.numpy as jnp
from jax import lax
from jax.experimental import pallas as pl
from jax.experimental.pallas import tpu as pltpu
from jax.sharding import PartitionSpec as P

AXES = ("gx", "gy", "gz")
SUB = 8


def minmod(p, r):
    return jnp.maximum(jnp.minimum(r, 0.0), jnp.minimum(p, jnp.maximum(r, 0.0)))


def gain(v):
    size = jnp.abs(v)
    return 0.5 * size * (1.0 - size)


def flux(v, g, q_low, q_high, s_low, s_high):
    up = v > 0
    return v * jnp.where(up, q_low, q_high) + g * jnp.where(up, s_low, s_high)


def kernel(
    sizes, flags_in, den, mom, en, disp, out_d, out_m, out_e, sums,
    flags, q, dx, dy, dz, xh, hop, xv, edge, zlo, zhi, cq, cs, part, slots, done,
    local_sem, send_sem, recv_sem, in_sem, sum_send, sum_recv,
):
    nx, ny, nz = den.shape
    pos = {a: lax.axis_index(a) for a in AXES}
    last = {a: sizes[a] - 1 for a in AXES}
    top = ny + SUB
    per = nz // 4
    parts = edge.shape[0]
    scale = 1.0 / 256.0
    xlo, xhi = xh.at[0], xh.at[1]
    own = slice(SUB, top)
    mesh_ids = pl.DeviceIdType.MESH

    locals_ = [
        pltpu.make_async_copy(flags_in, flags, local_sem.at[6]),
        pltpu.make_async_copy(den, q.at[0, :, own], local_sem.at[0]),
        pltpu.make_async_copy(en, q.at[4, :, own], local_sem.at[2]),
        pltpu.make_async_copy(disp.at[2], dz, local_sem.at[3]),
        pltpu.make_async_copy(disp.at[1], dy.at[:, own], local_sem.at[4]),
        pltpu.make_async_copy(disp.at[0], dx, local_sem.at[5]),
        pltpu.make_async_copy(mom, q.at[1:4, :, own], local_sem.at[1]),
    ]
    for c in locals_:
        c.start()

    me = pos["gx"]
    par = lax.rem(me, 2)
    odd = par == 1
    end = last["gx"]
    reach = [("gx", 1, 0, me > 0), ("gx", 2, 1, odd), ("gy", 1, 2, True), ("gz", 1, 3, True)]

    barrier = pltpu.get_barrier_semaphore()
    below = sum(jnp.where(pos[a] >= o, 1, 0) for a, o, _, _ in reach)

    @pl.when(below > 0)
    def _():
        pl.semaphore_wait(barrier, below)

    for a, o, k, told in reach:
        @pl.when(pos[a] + o <= last[a])
        def _(a=a, o=o):
            pl.semaphore_signal(
                barrier, inc=1, device_id={a: pos[a] + o}, device_id_type=mesh_ids
            )

        @pl.when((pos[a] >= o) & told)
        def _(a=a, o=o, k=k):
            pl.semaphore_signal(
                in_sem.at[k], inc=1, device_id={a: pos[a] - o}, device_id_type=mesh_ids
            )

    def is_in(a, o, k, cond=True):
        @pl.when((pos[a] + o <= last[a]) & cond)
        def _():
            pl.semaphore_wait(in_sem.at[k], 1)

    def copy(k, src, dst, axis, step):
        return pltpu.make_async_remote_copy(
            src_ref=src, dst_ref=dst, send_sem=send_sem.at[k], recv_sem=recv_sem.at[k],
            device_id={axis: pos[axis] + step}, device_id_type=mesh_ids,
        )

    leg_up = odd & (me + 2 <= end)
    leg_down = (par == 0) & (me >= 2)
    leg_out = leg_up | leg_down
    relays = (odd & (me >= 3)) | ((par == 0) & (me + 2 <= end))
    leg_in = (me + 1 <= end) & (odd | (me >= 2))
    other = 1 - par

    legs_up = [
        copy(16, q.at[1, nx - 2 : nx, own], hop.at[0:2], "gx", 2),
        copy(17, q.at[2, nx - 2 : nx, own], hop.at[2:4], "gx", 2),
        copy(18, q.at[4, nx - 2, own], hop.at[4], "gx", 2),
    ]
    legs_down = [
        copy(16, mom.at[0, 0:2], hop.at[0:2], "gx", -2),
        copy(17, mom.at[1, 0:2], hop.at[2:4], "gx", -2),
        copy(18, en.at[0], hop.at[4], "gx", -2),
    ]
    beside = 1 - 2 * par
    onward = [
        copy(19, hop.at[0:2], xh.at[other, 1], "gx", beside),
        copy(20, hop.at[2:4], xh.at[other, 2], "gx", beside),
        copy(21, hop.at[4], xh.at[other, 4, 0], "gx", beside),
    ]
    landed = [
        copy(19, hop.at[0:2], xh.at[par, 1], "gx", beside),
        copy(20, hop.at[2:4], xh.at[par, 2], "gx", beside),
        copy(21, hop.at[4], xh.at[par, 4, 0], "gx", beside),
    ]
    x_up = [
        copy(0, q.at[0, nx - 2 : nx, own], xlo.at[0], "gx", 1),
        copy(1, q.at[3, nx - 2 : nx, own], xlo.at[3], "gx", 1),
        copy(2, q.at[4, nx - 1, own], xlo.at[4, 1], "gx", 1),
    ]
    x_up_half = [
        copy(22, q.at[1:3, nx - 2 : nx, own], xlo.at[1:3], "gx", 1),
        copy(23, q.at[4, nx - 2, own], xlo.at[4, 0], "gx", 1),
    ]
    x_down = [
        copy(6, disp.at[0, 0], xv, "gx", -1),
        copy(3, den.at[0:2], xhi.at[0], "gx", -1),
        copy(4, mom.at[2, 0:2], xhi.at[3], "gx", -1),
        copy(5, en.at[1], xhi.at[4, 1], "gx", -1),
    ]
    x_down_half = [
        copy(24, mom.at[0:2, 0:2], xhi.at[1:3], "gx", -1),
        copy(25, en.at[0], xhi.at[4, 0], "gx", -1),
    ]
    up_half = (me < end) & ~leg_up
    down_half = (me > 0) & ~leg_down
    low_half = (me > 0) & ~(leg_in & (par == 0))
    high_half = (me < end) & ~(leg_in & odd)

    def each(cond, copies, act):
        @pl.when(cond)
        def _():
            for c in copies:
                act(c)

    def go(c):
        c.start()

    hi_rows = slice(top, top + SUB)
    y_up = [
        copy(7, q.at[0, :, ny:top], q.at[0, :, 0:SUB], "gy", 1),
        copy(8, q.at[1:4, :, ny:top], q.at[1:4, :, 0:SUB], "gy", 1),
        copy(9, q.at[4, :, ny:top], q.at[4, :, 0:SUB], "gy", 1),
    ]
    y_down = [
        copy(10, den.at[:, 0:SUB], q.at[0, :, hi_rows], "gy", -1),
        copy(11, mom.at[:, :, 0:SUB], q.at[1:4, :, hi_rows], "gy", -1),
        copy(12, en.at[:, 0:SUB], q.at[4, :, hi_rows], "gy", -1),
        copy(13, disp.at[1, :, 0:SUB], dy.at[:, hi_rows], "gy", -1),
    ]
    z_up = [copy(14, edge, zlo, "gz", 1)]
    z_down = [copy(15, edge, zhi, "gz", -1)]

    def arrive(axis, ups, downs, fill_low, fill_high):
        @pl.when(pos[axis] > 0)
        def _():
            for c in ups:
                c.wait_recv()

        @pl.when(pos[axis] < last[axis])
        def _():
            for c in downs:
                c.wait_recv()

        @pl.when(pos[axis] == 0)
        def _():
            fill_low()

        @pl.when(pos[axis] == last[axis])
        def _():
            fill_high()

    def sent(axis, ups, downs):
        @pl.when(pos[axis] < last[axis])
        def _():
            for c in ups:
                c.wait_send()

        @pl.when(pos[axis] > 0)
        def _():
            for c in downs:
                c.wait_send()

    below_x, below_y, below_z = me > 0, pos["gy"] > 0, pos["gz"] > 0
    above_x, above_y, above_z = (pos[a] < last[a] for a in AXES)
    each(leg_down, legs_down, go)
    each(below_x, x_down, go)
    each(down_half, x_down_half, go)
    each(below_y, y_down, go)

    for c in locals_[:-1]:
        c.wait()

    flag = [flags[i].astype(jnp.float32) for i in range(6)]

    def low_mult(a):
        return jnp.where(pos[AXES[a]] == 0, flag[2 * a], 1.0)

    def high_mult(a):
        return jnp.where(pos[AXES[a]] == last[AXES[a]], flag[2 * a + 1], 1.0)

    def outer_low(a):
        return jnp.where(pos[AXES[a]] == 0, flag[2 * a], 0.0)

    def outer_high(a):
        return jnp.where(pos[AXES[a]] == last[AXES[a]], flag[2 * a + 1], 0.0)

    lane = lax.broadcasted_iota(jnp.int32, (ny, nz), 1)
    row = lax.broadcasted_iota(jnp.int32, (ny, nz), 0)
    wz = jnp.where(lane == 0, outer_low(2), 0.0) - jnp.where(lane == nz - 1, outer_high(2), 0.0)
    wy = jnp.where(row == 0, outer_low(1), 0.0) - jnp.where(row == ny - 1, outer_high(1), 0.0)
    wx_low, wx_high = outer_low(0), outer_high(0)

    def total(x, carry):
        a, b = carry
        wx = jnp.where(x == 0, wx_low, 0.0) - jnp.where(x == nx - 1, wx_high, 0.0)
        w = 1.0 + scale * (
            wz * dz[x].astype(jnp.float32)
            + wy * dy[x, own].astype(jnp.float32)
            + wx * dx[x].astype(jnp.float32)
        )
        return (
            a + jnp.sum((q[0, x, own] * w).reshape(ny // SUB, SUB, nz), 0),
            b + jnp.sum((q[4, x, own] * w).reshape(ny // SUB, SUB, nz), 0),
        )

    zero = jnp.zeros((SUB, nz), jnp.float32)
    mass, power = lax.fori_loop(0, nx, total, (zero, zero))
    part[0:1] = jnp.sum(mass, 0, keepdims=True)
    part[1:2] = jnp.sum(power, 0, keepdims=True)

    sx, sy, sz = (sizes[a] for a in AXES)
    count = sx * sy * sz
    index = (pos["gx"] * sy + pos["gy"]) * sz + pos["gz"]
    first_device = index == 0

    def place(i):
        return {"gx": i // (sy * sz), "gy": i // sz % sy, "gz": i % sz}

    def message(src, dst, k, target):
        return pltpu.make_async_remote_copy(
            src_ref=src, dst_ref=dst, send_sem=sum_send.at[k], recv_sem=sum_recv.at[k],
            device_id=target, device_id_type=mesh_ids,
        )

    away = place(count - 1)
    inward = message(part, slots.at[index], 0, place(0))
    gathered = message(slots.at[1:count], slots.at[1:count], 0, away)
    outward = message(done, done, 1, place(0))
    scattered = message(slots.at[1:count], slots.at[1:count], 1, away)

    @pl.when(~first_device)
    def _():
        inward.start()

    locals_[-1].wait()

    def pack(x, carry):
        new = list(carry)
        for f in range(6):
            p = f * nx + x
            k = f * nx // per
            at = 4 * lax.rem(p, per)
            plane = q[f, x, own] if f < 5 else dz[x].astype(jnp.float32)
            moved = pltpu.roll(plane, at, 1)
            mine = lax.rem(lane + 2 - at + nz, nz) < 4
            new[k] = jnp.where(mine, moved, new[k])
        return tuple(new)

    packed = lax.fori_loop(0, nx, pack, tuple(jnp.zeros((ny, nz), jnp.float32) for _ in range(parts)))
    for k in range(parts):
        edge[k] = packed[k]
    each(below_z, z_down, go)
    is_in("gz", 1, 3)
    each(above_z, z_up, go)
    is_in("gx", 1, 0, me + 1 > 0)
    each(above_x, x_up, go)
    each(up_half, x_up_half, go)
    is_in("gx", 2, 1, odd)
    each(leg_up, legs_up, go)
    is_in("gy", 1, 2)
    each(above_y, y_up, go)

    outs = (
        lambda x: out_d.at[x], lambda x: out_m.at[0, x], lambda x: out_m.at[1, x],
        lambda x: out_m.at[2, x], lambda x: out_e.at[x],
    )

    def core(r, _):
        at = pl.ds(pl.multiple_of(r * SUB, SUB), SUB)
        inner = pl.ds(pl.multiple_of(r * SUB + SUB, SUB), SUB)
        vs = [dx[c, at].astype(jnp.float32) * scale for c in range(2, nx - 1)]
        gs = [gain(v) for v in vs]
        for f in range(5):
            line_q = [q[f, c, inner] for c in range(nx)]
            ds = [line_q[i + 1] - line_q[i] for i in range(nx - 1)]
            ss = [minmod(ds[i + 1], ds[i]) for i in range(nx - 2)]
            fl = [
                flux(vs[i], gs[i], line_q[i + 1], line_q[i + 2], ss[i], ss[i + 1])
                for i in range(nx - 3)
            ]
            for c in range(nx):
                new = line_q[c]
                if 2 <= c < nx - 1:
                    new = new + fl[c - 2]
                if 1 <= c < nx - 2:
                    new = new - fl[c - 1]
                outs[f](c)[at] = new
        return 0

    lax.fori_loop(0, ny // SUB, core, 0)

    def z_low():
        e = edge[...]
        zlo[...] = jnp.where(lane3 & 3 == 3, pltpu.roll(e, nz - 1, 2), pltpu.roll(e, nz - 2, 2))

    def z_high():
        e = edge[...]
        zhi[...] = jnp.where(lane3 & 3 == 0, pltpu.roll(e, 1, 2), pltpu.roll(e, 2, 2))

    lane3 = lax.broadcasted_iota(jnp.int32, (parts, ny, nz), 2)
    arrive("gz", z_up, z_down, z_low, z_high)
    low = lane & 3 == 0
    for k in range(parts):
        e, l, h = edge[k], zlo[k], zhi[k]
        r1, r2 = pltpu.roll(l, 1, 1), pltpu.roll(l, 2, 1)
        l1, l2 = pltpu.roll(h, nz - 1, 1), pltpu.roll(h, nz - 2, 1)
        cq[k] = jnp.where(low, r1, l1)
        cs[k] = jnp.where(low, minmod(e - r1, r1 - r2), minmod(l2 - l1, l1 - e))

    first, final = lane == 0, lane == nz - 1
    z_lo_mult = jnp.where(first, low_mult(2), 1.0) * scale
    z_hi_mult = high_mult(2) * scale
    def along_z(x, _):
        v = dz[x].astype(jnp.float32) * z_lo_mult
        g = gain(v)

        def ghosts(ref, f):
            back = lax.rem(nz - 4 * lax.rem(f * nx + x, per), nz)
            return pltpu.roll(ref[f * nx // per], back, 1)

        vh = ghosts(cq, 5) * z_hi_mult
        gh = gain(vh)
        for f in range(5):
            plane = q[f, x, SUB:top]
            gq, gs = ghosts(cq, f), ghosts(cs, f)
            qm = jnp.where(first, gq, pltpu.roll(plane, 1, 1))
            d = plane - qm
            s = minmod(jnp.where(final, gq - plane, pltpu.roll(d, nz - 1, 1)), d)
            sm = jnp.where(first, gs, pltpu.roll(s, 1, 1))
            fl = flux(v, g, qm, plane, sm, s)
            fh = jnp.where(final, flux(vh, gh, plane, gq, s, gs), pltpu.roll(fl, nz - 1, 1))
            outs[f](x)[...] += fl - fh
        return 0

    lax.fori_loop(0, nx, along_z, 0)

    @pl.when(relays)
    def _():
        for a, b in zip(legs_up, onward):
            a.wait_recv()
            b.start()

    def y_low():
        q[:, :, 0:SUB] = jnp.broadcast_to(q[:, :, SUB : SUB + 1], (5, nx, SUB, nz))

    def y_high():
        q[:, :, hi_rows] = jnp.broadcast_to(q[:, :, top - 1 : top], (5, nx, SUB, nz))
        dy[:, hi_rows] = jnp.broadcast_to(dy[:, top - 1 : top], (nx, SUB, nz))

    arrive("gy", y_up, y_down, y_low, y_high)
    tall = ny + 2 * SUB
    rows = lax.broadcasted_iota(jnp.int32, (tall, nz), 0)
    inside = (rows >= SUB) & (rows <= top)
    y_mult = jnp.where(
        rows == SUB, low_mult(1) * scale, jnp.where(rows == top, high_mult(1) * scale, scale)
    )

    def along_y(x, _):
        v = jnp.where(inside, dy[x].astype(jnp.float32), 0.0) * y_mult
        g = gain(v)
        for f in range(5):
            plane = q[f, x]
            qm = pltpu.roll(plane, 1, 0)
            d = plane - qm
            s = minmod(pltpu.roll(d, tall - 1, 0), d)
            fl = flux(v, g, qm, plane, pltpu.roll(s, 1, 0), s)
            ch = fl - pltpu.roll(fl, tall - 1, 0)
            outs[f](x)[...] += ch[SUB:top]
        return 0

    lax.fori_loop(0, nx, along_y, 0)

    def x_low():
        xlo[...] = jnp.broadcast_to(q[:, 0:1, SUB:top], (5, 2, ny, nz))

    def x_high():
        xhi[...] = jnp.broadcast_to(q[:, nx - 1 : nx, SUB:top], (5, 2, ny, nz))
        xv[...] = dx[nx - 1]

    arrive("gx", x_up, x_down, x_low, x_high)
    x_lo_mult, x_hi_mult = low_mult(0) * scale, high_mult(0) * scale

    def x_rows(r):
        return pl.ds(pl.multiple_of(r * SUB, SUB), SUB), pl.ds(
            pl.multiple_of(r * SUB + SUB, SUB), SUB
        )

    def x_flux(v, g, cells4):
        ds = [cells4[i + 1] - cells4[i] for i in range(3)]
        return flux(
            v, g, cells4[1], cells4[2], minmod(ds[1], ds[0]), minmod(ds[2], ds[1])
        )

    def rim(fields, r, _):
        at, inner = x_rows(r)
        faces = (0, 1, nx - 1, nx)
        vs = [
            dx[0, at].astype(jnp.float32) * x_lo_mult,
            dx[1, at].astype(jnp.float32) * scale,
            dx[nx - 1, at].astype(jnp.float32) * scale,
            xv[at].astype(jnp.float32) * x_hi_mult,
        ]
        gs = [gain(v) for v in vs]
        for f in fields:
            a = [xlo[f, 0, at], xlo[f, 1, at]] + [q[f, c, inner] for c in range(3)]
            b = [q[f, c, inner] for c in range(nx - 3, nx)] + [xhi[f, 0, at], xhi[f, 1, at]]
            fl = [x_flux(vs[i], gs[i], (a, a, b, b)[i][i % 2 : i % 2 + 4]) for i in range(4)]
            for c, change in (
                (0, fl[0] - fl[1]), (1, fl[1]), (nx - 2, -fl[2]), (nx - 1, fl[2] - fl[3]),
            ):
                ref = outs[f](c)
                ref[at] += change
        return 0

    lax.fori_loop(0, ny // SUB, functools.partial(rim, (0, 3)), 0)
    for piece, whole, fields in ((0, (0,), (1,)), (1, (), (2,)), (2, (1,), (4,))):
        each(low_half, [x_up_half[k] for k in whole], lambda c: c.wait_recv())
        each(high_half, [x_down_half[k] for k in whole], lambda c: c.wait_recv())
        each(leg_in, landed[piece : piece + 1], lambda c: c.wait_recv())
        lax.fori_loop(0, ny // SUB, functools.partial(rim, fields), 0)

    @pl.when(first_device)
    def _():
        gathered.wait_recv()
        done[...] = part[...] + jnp.sum(slots[1:count], 0)

        def tell(i, _):
            message(done, done, 1, place(i)).start()
            return 0

        lax.fori_loop(1, count, tell, 0)
        scattered.wait_send()

    @pl.when(~first_device)
    def _():
        outward.wait_recv()
        inward.wait_send()

    sums[...] = done[...]
    each(above_x, x_up, lambda c: c.wait_send())
    each(below_x, x_down, lambda c: c.wait_send())
    each(leg_out, legs_up, lambda c: c.wait_send())
    each(relays, onward, lambda c: c.wait_send())
    each(up_half, x_up_half, lambda c: c.wait_send())
    each(down_half, x_down_half, lambda c: c.wait_send())
    each(above_y, y_up, lambda c: c.wait_send())
    each(below_y, y_down, lambda c: c.wait_send())
    each(above_z, z_up, lambda c: c.wait_send())
    each(below_z, z_down, lambda c: c.wait_send())


def put(cells, den, mom, en, sums, out_d, out_m, out_e, totals, mean, sem):
    pairs = ((mom, out_m), (den, out_d), (en, out_e))
    moves = [
        pltpu.make_async_copy(src, dst, sem.at[i]) for i, (src, dst) in enumerate(pairs)
    ]
    for c in moves:
        c.start()
    mean[0] = jnp.sum(sums[0:1]) / cells
    mean[1] = jnp.sum(sums[1:2]) / cells
    moves.append(pltpu.make_async_copy(mean, totals, sem.at[3]))
    moves[-1].start()
    for c in moves:
        c.wait()


def shards(density, momentum, energy, displacement, flags):
    sizes = {a: lax.axis_size(a) for a in AXES}
    nx, ny, nz = density.shape
    tall = ny + 2 * SUB
    per = nz // 4
    parts = -(-6 * nx // per)
    f32, i32 = jnp.float32, jnp.int32
    dma = pltpu.SemaphoreType.DMA
    any_ = pl.BlockSpec(memory_space=pl.ANY)
    hbm = pl.BlockSpec(memory_space=pltpu.HBM)
    vmem = pl.BlockSpec(memory_space=pltpu.VMEM)
    devices = 1
    for a in AXES:
        devices *= sizes[a]
    cells = float(nx * ny * nz * devices)
    outputs = tuple(jax.ShapeDtypeStruct(v.shape, f32) for v in (density, momentum, energy))
    results = pl.pallas_call(
        functools.partial(kernel, sizes),
        out_shape=outputs + (jax.ShapeDtypeStruct((2, nz), f32),),
        in_specs=[hbm] * 5,
        out_specs=(vmem, vmem, vmem, vmem),
        scratch_shapes=[
            pltpu.SMEM((6,), i32),
            pltpu.VMEM((5, nx, tall, nz), f32),
            pltpu.VMEM((nx, ny, nz), i32),
            pltpu.VMEM((nx, tall, nz), i32),
            pltpu.VMEM((nx, ny, nz), i32),
            pltpu.VMEM((2, 5, 2, ny, nz), f32),
            pltpu.VMEM((5, ny, nz), f32),
            pltpu.VMEM((ny, nz), i32),
        ]
        + [pltpu.VMEM((parts, ny, nz), f32) for _ in range(5)]
        + [pltpu.VMEM((2, nz), f32), pltpu.VMEM((devices, 2, nz), f32), pltpu.VMEM((2, nz), f32)]
        + [dma((7,)), dma((26,)), dma((26,)), pltpu.SemaphoreType.REGULAR((4,)), dma((2,)), dma((2,))],
        compiler_params=pltpu.CompilerParams(
            collective_id=0, has_side_effects=True, vmem_limit_bytes=12 << 20
        ),
    )(
        *(
            pltpu.with_memory_space_constraint(v, pltpu.HBM)
            for v in (flags, density, momentum, energy, displacement)
        )
    )
    return pl.pallas_call(
        functools.partial(put, cells),
        out_shape=outputs + (jax.ShapeDtypeStruct((2,), f32),),
        in_specs=[any_, any_, any_, vmem],
        out_specs=(hbm, hbm, hbm, hbm),
        scratch_shapes=[pltpu.SMEM((2,), f32), dma((4,))],
        compiler_params=pltpu.CompilerParams(vmem_limit_bytes=2 << 20),
    )(*results)


def solution(mesh):
    return jax.shard_map(
        shards,
        mesh=mesh,
        in_specs=(
            P("gx", "gy", "gz"),
            P(None, "gx", "gy", "gz"),
            P("gx", "gy", "gz"),
            P(None, "gx", "gy", "gz"),
            P(),
        ),
        out_specs=(P("gx", "gy", "gz"), P(None, "gx", "gy", "gz"), P("gx", "gy", "gz"), P()),
        check_vma=False,
    )
```

```python
import functools

import jax
import jax.numpy as jnp
from jax import lax
from jax.experimental import pallas as pl
from jax.experimental.pallas import tpu as pltpu
from jax.sharding import PartitionSpec as P

AXES = ("gx", "gy", "gz")
SUB = 8


def minmod(p, r):
    return jnp.maximum(jnp.minimum(r, 0.0), jnp.minimum(p, jnp.maximum(r, 0.0)))


def gain(v):
    size = jnp.abs(v)
    return 0.5 * size * (1.0 - size)


def flux(v, g, q_low, q_high, s_low, s_high):
    up = v > 0
    return v * jnp.where(up, q_low, q_high) + g * jnp.where(up, s_low, s_high)


def kernel(
    sizes, flags_in, den, mom, en, disp, out_d, out_m, out_e, sums,
    flags, q, dx, dy, dz, xh, hop, xv, edge, zlo, zhi, cq, cs, part, slots, line, done,
    local_sem, send_sem, recv_sem, in_sem, sum_send, sum_recv,
):
    nx, ny, nz = den.shape
    pos = {a: lax.axis_index(a) for a in AXES}
    last = {a: sizes[a] - 1 for a in AXES}
    top = ny + SUB
    per = nz // 4
    parts = edge.shape[0]
    scale = 1.0 / 256.0
    xlo, xhi = xh.at[0], xh.at[1]
    own = slice(SUB, top)
    mesh_ids = pl.DeviceIdType.MESH

    def load(src, dst, k):
        return pltpu.make_async_copy(src, dst, local_sem.at[k])

    spans = (slice(0, 2), slice(nx - 2, nx), slice(2, nx - 2))
    planes = [
        [
            load(den.at[x], q.at[0, x, own], 3 * i),
            load(en.at[x], q.at[4, x, own], 3 * i + 1),
            load(mom.at[:, x], q.at[1:4, x, own], 3 * i + 2),
        ]
        for i, x in enumerate(spans)
    ]
    others = [
        load(disp.at[0], dx, 9),
        load(flags_in, flags, 10),
        load(disp.at[2], dz, 11),
        load(disp.at[1], dy.at[:, own], 12),
    ]
    for c in planes[0] + planes[1] + others + planes[2]:
        c.start()

    me = pos["gx"]
    par = lax.rem(me, 2)
    odd = par == 1
    end = last["gx"]
    sx, sy, sz = (sizes[a] for a in AXES)
    group = sx * sz
    leader = (me == 0) & (pos["gz"] == last["gz"])
    members = [{"gx": i // sz, "gz": last["gz"] - i % sz} for i in range(1, group)]

    def tell(sem, cond, **target):
        @pl.when(cond)
        def _():
            pl.semaphore_signal(sem, inc=1, device_id=target, device_id_type=mesh_ids)

    barrier = pltpu.get_barrier_semaphore()
    reach = [("gx", 1, par == 0, odd), ("gx", 2, True, True), ("gy", 1, True, True), ("gz", 1, True, True)]
    below = jnp.where(leader, pos["gy"], 1)
    for a, o, speaks, hears in reach:
        tell(barrier, (pos[a] + o <= last[a]) & speaks, **{a: pos[a] + o})
        below += jnp.where((pos[a] >= o) & hears, 1, 0)

    @pl.when(leader)
    def _():
        for target in members:
            tell(barrier, True, **target)
        for o in range(1, sy):
            tell(barrier, pos["gy"] + o <= last["gy"], gy=pos["gy"] + o)

    @pl.when(below > 0)
    def _():
        pl.semaphore_wait(barrier, below)

    tell(in_sem.at[0], odd, gx=me - 1)
    tell(in_sem.at[1], me >= 2, gx=me - 2)
    tell(in_sem.at[2], pos["gy"] > 0, gy=pos["gy"] - 1)
    tell(in_sem.at[3], pos["gz"] > 0, gz=pos["gz"] - 1)
    for o in range(1, sy):
        tell(in_sem.at[4], leader & (pos["gy"] >= o), gy=pos["gy"] - o)

    def is_in(k, cond, many=1):
        @pl.when(cond)
        def _():
            pl.semaphore_wait(in_sem.at[k], many)

    def copy(k, src, dst, axis, step):
        return pltpu.make_async_remote_copy(
            src_ref=src, dst_ref=dst, send_sem=send_sem.at[k], recv_sem=recv_sem.at[k],
            device_id={axis: pos[axis] + step}, device_id_type=mesh_ids,
        )

    below_x, below_y, below_z = me > 0, pos["gy"] > 0, pos["gz"] > 0
    above_x, above_y, above_z = (pos[a] < last[a] for a in AXES)
    even = ~odd
    hands_up, hands_down = odd & above_x, even & below_x
    relays = (odd & below_x & (me >= 3)) | (even & (me + 2 <= end))
    beside = 1 - 2 * par

    order = (0, 3, 1, 2, 4)
    direct = (0, 3)
    relayed = (1, 2)
    up = {f: copy(f, q.at[f, nx - 2 : nx, own], xlo.at[f], "gx", 1) for f in order}
    down = {f: copy(5 + f, q.at[f, 0:2, own], xhi.at[f], "gx", -1) for f in order}
    down_last = copy(9, q.at[4, 1, own], xhi.at[4, 1], "gx", -1)
    up_last = copy(4, q.at[4, nx - 1, own], xlo.at[4, 1], "gx", 1)
    v_down = copy(10, dx.at[0], xv, "gx", -1)
    legs_up = [
        copy(16 + i, q.at[f, nx - 2 : nx, own], hop.at[2 * i : 2 * i + 2], "gx", 2)
        for i, f in enumerate(relayed)
    ] + [copy(18, q.at[4, nx - 2, own], hop.at[4], "gx", 2)]
    legs_down = [
        copy(16 + i, q.at[f, 0:2, own], hop.at[2 * i : 2 * i + 2], "gx", -2)
        for i, f in enumerate(relayed)
    ] + [copy(18, q.at[4, 0, own], hop.at[4], "gx", -2)]

    def handed(side):
        return [
            copy(19 + i, hop.at[2 * i : 2 * i + 2], side.at[f], "gx", beside)
            for i, f in enumerate(relayed)
        ] + [copy(21, hop.at[4], side.at[4, 0], "gx", beside)]

    handed_up, handed_down = handed(xlo), handed(xhi)

    def each(cond, copies, act):
        @pl.when(cond)
        def _():
            for c in copies:
                act(c)

    def go(c):
        c.start()

    hi_rows = slice(top, top + SUB)
    y_up = [
        copy(22, q.at[0, :, ny:top], q.at[0, :, 0:SUB], "gy", 1),
        copy(23, q.at[1:4, :, ny:top], q.at[1:4, :, 0:SUB], "gy", 1),
        copy(24, q.at[4, :, ny:top], q.at[4, :, 0:SUB], "gy", 1),
    ]
    y_down = [
        copy(11, q.at[4, :, SUB : 2 * SUB], q.at[4, :, hi_rows], "gy", -1),
        copy(12, q.at[0, :, SUB : 2 * SUB], q.at[0, :, hi_rows], "gy", -1),
        copy(13, q.at[1:4, :, SUB : 2 * SUB], q.at[1:4, :, hi_rows], "gy", -1),
        copy(25, dy.at[:, SUB : 2 * SUB], dy.at[:, hi_rows], "gy", -1),
    ]
    z_up = [copy(14, edge, zlo, "gz", 1)]
    z_down = [copy(15, edge, zhi, "gz", -1)]

    def arrive(axis, ups, downs, fill_low, fill_high):
        @pl.when(pos[axis] > 0)
        def _():
            for c in ups:
                c.wait_recv()

        @pl.when(pos[axis] < last[axis])
        def _():
            for c in downs:
                c.wait_recv()

        @pl.when(pos[axis] == 0)
        def _():
            fill_low()

        @pl.when(pos[axis] == last[axis])
        def _():
            fill_high()

    def sent(axis, ups, downs):
        @pl.when(pos[axis] < last[axis])
        def _():
            for c in ups:
                c.wait_send()

        @pl.when(pos[axis] > 0)
        def _():
            for c in downs:
                c.wait_send()

    first, rest = order[0], order[1:]
    planes[0][0].wait()
    each(odd, [down[first]], go)
    for c in planes[0][1:] + planes[1] + others + planes[2]:
        c.wait()

    flag = [flags[i].astype(jnp.float32) for i in range(6)]

    def low_mult(a):
        return jnp.where(pos[AXES[a]] == 0, flag[2 * a], 1.0)

    def high_mult(a):
        return jnp.where(pos[AXES[a]] == last[AXES[a]], flag[2 * a + 1], 1.0)

    def outer_low(a):
        return jnp.where(pos[AXES[a]] == 0, flag[2 * a], 0.0)

    def outer_high(a):
        return jnp.where(pos[AXES[a]] == last[AXES[a]], flag[2 * a + 1], 0.0)

    lane = lax.broadcasted_iota(jnp.int32, (ny, nz), 1)
    row = lax.broadcasted_iota(jnp.int32, (ny, nz), 0)
    wz = jnp.where(lane == 0, outer_low(2), 0.0) - jnp.where(lane == nz - 1, outer_high(2), 0.0)
    wy = jnp.where(row == 0, outer_low(1), 0.0) - jnp.where(row == ny - 1, outer_high(1), 0.0)
    wx_low, wx_high = outer_low(0), outer_high(0)

    def total(x, carry):
        a, b = carry
        wx = jnp.where(x == 0, wx_low, 0.0) - jnp.where(x == nx - 1, wx_high, 0.0)
        w = 1.0 + scale * (
            wz * dz[x].astype(jnp.float32)
            + wy * dy[x, own].astype(jnp.float32)
            + wx * dx[x].astype(jnp.float32)
        )
        return (
            a + jnp.sum((q[0, x, own] * w).reshape(ny // SUB, SUB, nz), 0),
            b + jnp.sum((q[4, x, own] * w).reshape(ny // SUB, SUB, nz), 0),
        )

    zero = jnp.zeros((SUB, nz), jnp.float32)
    mass, power = lax.fori_loop(0, nx, total, (zero, zero))
    part[0:1] = jnp.sum(mass, 0, keepdims=True)
    part[1:2] = jnp.sum(power, 0, keepdims=True)

    def message(src, dst, k, target):
        return pltpu.make_async_remote_copy(
            src_ref=src, dst_ref=dst, send_sem=sum_send.at[k], recv_sem=sum_recv.at[k],
            device_id=target, device_id_type=mesh_ids,
        )

    inward = message(part, slots.at[me * sz + last["gz"] - pos["gz"]], 0, {"gx": 0, "gz": last["gz"]})
    gathered = message(slots.at[1:group], slots.at[1:group], 0, members[-1])
    across = [
        message(line.at[0], line.at[sy - o], 1, {"gy": lax.rem(pos["gy"] + o, sy)})
        for o in range(1, sy)
    ]
    crossed = message(line.at[1:sy], line.at[1:sy], 1, {"gy": lax.rem(pos["gy"] + 1, sy)})
    outward = [message(done, done, 2, target) for target in members]
    scattered = message(slots.at[1:group], slots.at[1:group], 2, members[-1])

    each(~leader, [inward], go)

    each(hands_down, legs_down, go)
    each(below_y, y_down, go)

    def x_sends():
        is_in(0, even & above_x)
        each(even & below_x & above_x, [up[f] for f in direct], go)
        is_in(1, me + 2 <= end)

        @pl.when(even & (me + 2 <= end))
        def _():
            tell(in_sem.at[5], True, gx=me + 1)
            tell(in_sem.at[5], True, gx=me + 2)

        each(odd, [v_down] + [down[f] for f in rest], go)
        each(odd & (me + 2 <= end), legs_up, go)
        each(~below_x & above_x, [up[f] for f in direct], go)
        is_in(5, hands_up | hands_down)
        each(hands_up, [up[f] for f in direct] + [up_last], go)
        each(hands_down, [v_down] + [down[f] for f in direct] + [down_last], go)
        each(even & above_x, [up[f] for f in relayed + (4,)], go)

    pl.when(below_x | below_y)(x_sends)

    def pack(x, carry):
        new = list(carry)
        for f in range(6):
            p = f * nx + x
            k = f * nx // per
            at = 4 * lax.rem(p, per)
            plane = q[f, x, own] if f < 5 else dz[x].astype(jnp.float32)
            moved = pltpu.roll(plane, at, 1)
            mine = lax.rem(lane + 2 - at + nz, nz) < 4
            new[k] = jnp.where(mine, moved, new[k])
        return tuple(new)

    packed = lax.fori_loop(0, nx, pack, tuple(jnp.zeros((ny, nz), jnp.float32) for _ in range(parts)))
    for k in range(parts):
        edge[k] = packed[k]
    each(below_z, z_down, go)
    is_in(3, above_z)
    each(above_z, z_up, go)
    pl.when(~below_x & ~below_y)(x_sends)
    is_in(2, above_y)
    each(above_y, y_up, go)

    outs = (
        lambda x: out_d.at[x], lambda x: out_m.at[0, x], lambda x: out_m.at[1, x],
        lambda x: out_m.at[2, x], lambda x: out_e.at[x],
    )

    def core(r, _):
        at = pl.ds(pl.multiple_of(r * SUB, SUB), SUB)
        inner = pl.ds(pl.multiple_of(r * SUB + SUB, SUB), SUB)
        vs = [dx[c, at].astype(jnp.float32) * scale for c in range(2, nx - 1)]
        gs = [gain(v) for v in vs]
        for f in range(5):
            line_q = [q[f, c, inner] for c in range(nx)]
            ds = [line_q[i + 1] - line_q[i] for i in range(nx - 1)]
            ss = [minmod(ds[i + 1], ds[i]) for i in range(nx - 2)]
            fl = [
                flux(vs[i], gs[i], line_q[i + 1], line_q[i + 2], ss[i], ss[i + 1])
                for i in range(nx - 3)
            ]
            for c in range(nx):
                new = line_q[c]
                if 2 <= c < nx - 1:
                    new = new + fl[c - 2]
                if 1 <= c < nx - 2:
                    new = new - fl[c - 1]
                outs[f](c)[at] = new
        return 0

    lax.fori_loop(0, ny // SUB, core, 0)

    def z_low():
        e = edge[...]
        zlo[...] = jnp.where(lane3 & 3 == 3, pltpu.roll(e, nz - 1, 2), pltpu.roll(e, nz - 2, 2))

    def z_high():
        e = edge[...]
        zhi[...] = jnp.where(lane3 & 3 == 0, pltpu.roll(e, 1, 2), pltpu.roll(e, 2, 2))

    lane3 = lax.broadcasted_iota(jnp.int32, (parts, ny, nz), 2)
    arrive("gz", z_up, z_down, z_low, z_high)
    low = lane & 3 == 0
    for k in range(parts):
        e, l, h = edge[k], zlo[k], zhi[k]
        r1, r2 = pltpu.roll(l, 1, 1), pltpu.roll(l, 2, 1)
        l1, l2 = pltpu.roll(h, nz - 1, 1), pltpu.roll(h, nz - 2, 1)
        cq[k] = jnp.where(low, r1, l1)
        cs[k] = jnp.where(low, minmod(e - r1, r1 - r2), minmod(l2 - l1, l1 - e))

    first, final = lane == 0, lane == nz - 1
    z_lo_mult = jnp.where(first, low_mult(2), 1.0) * scale
    z_hi_mult = high_mult(2) * scale
    def along_z(x, _):
        v = dz[x].astype(jnp.float32) * z_lo_mult
        g = gain(v)

        def ghosts(ref, f):
            back = lax.rem(nz - 4 * lax.rem(f * nx + x, per), nz)
            return pltpu.roll(ref[f * nx // per], back, 1)

        vh = ghosts(cq, 5) * z_hi_mult
        gh = gain(vh)
        for f in range(5):
            plane = q[f, x, SUB:top]
            gq, gs = ghosts(cq, f), ghosts(cs, f)
            qm = jnp.where(first, gq, pltpu.roll(plane, 1, 1))
            d = plane - qm
            s = minmod(jnp.where(final, gq - plane, pltpu.roll(d, nz - 1, 1)), d)
            sm = jnp.where(first, gs, pltpu.roll(s, 1, 1))
            fl = flux(v, g, qm, plane, sm, s)
            fh = jnp.where(final, flux(vh, gh, plane, gq, s, gs), pltpu.roll(fl, nz - 1, 1))
            outs[f](x)[...] += fl - fh
        return 0

    early = nx * 5 // 8
    lax.fori_loop(0, early, along_z, 0)

    def gather():
        gathered.wait_recv()
        line[0] = part[...] + jnp.sum(slots[1:group], 0)
        is_in(4, pos["gy"] < last["gy"], last["gy"] - pos["gy"])
        for c in across:
            c.start()

    pl.when(leader & below_y)(gather)
    lax.fori_loop(early, nx, along_z, 0)

    def hand_on(cond, legs, onward):
        @pl.when(relays & cond)
        def _():
            for a, b in zip(legs, onward):
                a.wait_recv()
                b.start()

    hand_on(odd, legs_up, handed_up)
    hand_on(even, legs_down, handed_down)

    def y_low():
        q[:, :, 0:SUB] = jnp.broadcast_to(q[:, :, SUB : SUB + 1], (5, nx, SUB, nz))

    def y_high():
        q[:, :, hi_rows] = jnp.broadcast_to(q[:, :, top - 1 : top], (5, nx, SUB, nz))
        dy[:, hi_rows] = jnp.broadcast_to(dy[:, top - 1 : top], (nx, SUB, nz))

    arrive("gy", y_up, y_down, y_low, y_high)
    pl.when(leader & ~below_y)(gather)
    tall = ny + 2 * SUB
    rows = lax.broadcasted_iota(jnp.int32, (tall, nz), 0)
    inside = (rows >= SUB) & (rows <= top)
    y_mult = jnp.where(
        rows == SUB, low_mult(1) * scale, jnp.where(rows == top, high_mult(1) * scale, scale)
    )

    def along_y(x, _):
        v = jnp.where(inside, dy[x].astype(jnp.float32), 0.0) * y_mult
        g = gain(v)
        for f in range(5):
            plane = q[f, x]
            qm = pltpu.roll(plane, 1, 0)
            d = plane - qm
            s = minmod(pltpu.roll(d, tall - 1, 0), d)
            fl = flux(v, g, qm, plane, pltpu.roll(s, 1, 0), s)
            ch = fl - pltpu.roll(fl, tall - 1, 0)
            outs[f](x)[...] += ch[SUB:top]
        return 0

    lax.fori_loop(0, nx, along_y, 0)

    @pl.when(me == 0)
    def _():
        xlo[...] = jnp.broadcast_to(q[:, 0:1, own], (5, 2, ny, nz))

    @pl.when(me == end)
    def _():
        xhi[...] = jnp.broadcast_to(q[:, nx - 1 : nx, own], (5, 2, ny, nz))
        xv[...] = dx[nx - 1]

    each(above_x, [v_down], lambda c: c.wait_recv())
    x_lo_mult, x_hi_mult = low_mult(0) * scale, high_mult(0) * scale

    def rim(high, f):
        def rows(r, _):
            at = pl.ds(pl.multiple_of(r * SUB, SUB), SUB)
            inner = pl.ds(pl.multiple_of(r * SUB + SUB, SUB), SUB)
            if high:
                cells = [q[f, c, inner] for c in range(nx - 3, nx)] + [xhi[f, i, at] for i in range(2)]
                vs = (dx[nx - 1, at].astype(jnp.float32) * scale, xv[at].astype(jnp.float32) * x_hi_mult)
            else:
                cells = [xlo[f, i, at] for i in range(2)] + [q[f, c, inner] for c in range(3)]
                vs = (dx[0, at].astype(jnp.float32) * x_lo_mult, dx[1, at].astype(jnp.float32) * scale)
            ds = [cells[i + 1] - cells[i] for i in range(4)]
            ss = [minmod(ds[i + 1], ds[i]) for i in range(3)]
            fl = [
                flux(vs[i], gain(vs[i]), cells[i + 1], cells[i + 2], ss[i], ss[i + 1])
                for i in range(2)
            ]
            if high:
                changes = ((nx - 2, -fl[0]), (nx - 1, fl[0] - fl[1]))
            else:
                changes = ((0, fl[0] - fl[1]), (1, fl[1]))
            for c, change in changes:
                ref = outs[f](c)
                ref[at] += change
            return 0

        lax.fori_loop(0, ny // SUB, rows, 0)

    def come(cond, copies):
        each(cond, copies, lambda c: c.wait_recv())

    def lower(f):
        come(odd, [up[f]])
        if f in direct:
            come(hands_down, [up[f]])
        elif f in relayed:
            come(hands_down, [handed_up[f - 1]])
        else:
            come(hands_down, [up_last, handed_up[2]])
        rim(False, f)

    def upper(f):
        come(even & above_x, [down[f]])
        if f in direct:
            come(hands_up, [down[f]])
        elif f in relayed:
            come(hands_up, [handed_down[f - 1]])
        else:
            come(hands_up, [down_last, handed_down[2]])
        rim(True, f)

    def finish():
        crossed.wait_recv()
        done[...] = jnp.sum(line[...], 0)
        for c in outward:
            c.start()

    @pl.when(hands_up)
    def _():
        for f in direct:
            upper(f)
        for f in order:
            lower(f)
        for f in relayed + (4,):
            upper(f)

    @pl.when(odd & ~above_x)
    def _():
        for f in order:
            upper(f)
        for f in order:
            lower(f)

    @pl.when(hands_down)
    def _():
        for f in order:
            upper(f)
        for f in order:
            lower(f)

    @pl.when(~below_x)
    def _():
        for f in order:
            lower(f)
        for f in direct:
            upper(f)
        pl.when(leader)(finish)
        for f in relayed + (4,):
            upper(f)

    @pl.when(~leader)
    def _():
        outward[0].wait_recv()
        inward.wait_send()

    sums[...] = done[...]

    @pl.when(leader)
    def _():
        crossed.wait_send()
        scattered.wait_send()

    def sent(cond, copies):
        each(cond, copies, lambda c: c.wait_send())

    sent(below_x, [v_down] + [down[f] for f in direct])
    sent(odd, [down[f] for f in relayed + (4,)])
    sent(above_x, [up[f] for f in direct])
    sent(even & above_x, [up[f] for f in relayed + (4,)])
    sent(hands_up, [up_last])
    sent(hands_down, [down_last])
    sent(odd & (me + 2 <= end), legs_up)
    sent(hands_down, legs_down)
    sent(relays & odd, handed_up)
    sent(relays & even, handed_down)
    sent(above_y, y_up)
    sent(below_y, y_down)
    sent(above_z, z_up)
    sent(below_z, z_down)


def put(cells, den, mom, en, sums, out_d, out_m, out_e, totals, mean, sem):
    pairs = ((mom, out_m), (den, out_d), (en, out_e))
    moves = [
        pltpu.make_async_copy(src, dst, sem.at[i]) for i, (src, dst) in enumerate(pairs)
    ]
    for c in moves:
        c.start()
    mean[0] = jnp.sum(sums[0:1]) / cells
    mean[1] = jnp.sum(sums[1:2]) / cells
    moves.append(pltpu.make_async_copy(mean, totals, sem.at[3]))
    moves[-1].start()
    for c in moves:
        c.wait()


def shards(density, momentum, energy, displacement, flags):
    sizes = {a: lax.axis_size(a) for a in AXES}
    nx, ny, nz = density.shape
    tall = ny + 2 * SUB
    per = nz // 4
    parts = -(-6 * nx // per)
    f32, i32 = jnp.float32, jnp.int32
    dma = pltpu.SemaphoreType.DMA
    any_ = pl.BlockSpec(memory_space=pl.ANY)
    hbm = pl.BlockSpec(memory_space=pltpu.HBM)
    vmem = pl.BlockSpec(memory_space=pltpu.VMEM)
    devices = 1
    for a in AXES:
        devices *= sizes[a]
    cells = float(nx * ny * nz * devices)
    outputs = tuple(jax.ShapeDtypeStruct(v.shape, f32) for v in (density, momentum, energy))
    results = pl.pallas_call(
        functools.partial(kernel, sizes),
        out_shape=outputs + (jax.ShapeDtypeStruct((2, nz), f32),),
        in_specs=[hbm] * 5,
        out_specs=(vmem, vmem, vmem, vmem),
        scratch_shapes=[
            pltpu.SMEM((6,), i32),
            pltpu.VMEM((5, nx, tall, nz), f32),
            pltpu.VMEM((nx, ny, nz), i32),
            pltpu.VMEM((nx, tall, nz), i32),
            pltpu.VMEM((nx, ny, nz), i32),
            pltpu.VMEM((2, 5, 2, ny, nz), f32),
            pltpu.VMEM((5, ny, nz), f32),
            pltpu.VMEM((ny, nz), i32),
        ]
        + [pltpu.VMEM((parts, ny, nz), f32) for _ in range(5)]
        + [pltpu.VMEM((2, nz), f32), pltpu.VMEM((sizes["gx"] * sizes["gz"], 2, nz), f32)]
        + [pltpu.VMEM((sizes["gy"], 2, nz), f32), pltpu.VMEM((2, nz), f32)]
        + [dma((13,)), dma((26,)), dma((26,)), pltpu.SemaphoreType.REGULAR((6,)), dma((3,)), dma((3,))],
        compiler_params=pltpu.CompilerParams(
            collective_id=0, has_side_effects=True, vmem_limit_bytes=12 << 20
        ),
    )(
        *(
            pltpu.with_memory_space_constraint(v, pltpu.HBM)
            for v in (flags, density, momentum, energy, displacement)
        )
    )
    return pl.pallas_call(
        functools.partial(put, cells),
        out_shape=outputs + (jax.ShapeDtypeStruct((2,), f32),),
        in_specs=[any_, any_, any_, vmem],
        out_specs=(hbm, hbm, hbm, hbm),
        scratch_shapes=[pltpu.SMEM((2,), f32), dma((4,))],
        compiler_params=pltpu.CompilerParams(vmem_limit_bytes=2 << 20),
    )(*results)


def solution(mesh):
    return jax.shard_map(
        shards,
        mesh=mesh,
        in_specs=(
            P("gx", "gy", "gz"),
            P(None, "gx", "gy", "gz"),
            P("gx", "gy", "gz"),
            P(None, "gx", "gy", "gz"),
            P(),
        ),
        out_specs=(P("gx", "gy", "gz"), P(None, "gx", "gy", "gz"), P("gx", "gy", "gz"), P()),
        check_vma=False,
    )
```

```python
import functools

import jax
import jax.numpy as jnp
from jax import lax
from jax.experimental import pallas as pl
from jax.experimental.pallas import tpu as pltpu
from jax.sharding import PartitionSpec as P

AXES = ("gx", "gy", "gz")
SUB = 8


def minmod(p, r):
    return jnp.maximum(jnp.minimum(r, 0.0), jnp.minimum(p, jnp.maximum(r, 0.0)))


def gain(v):
    size = jnp.abs(v)
    return 0.5 * size * (1.0 - size)


def flux(v, g, q_low, q_high, s_low, s_high):
    up = v > 0
    return v * jnp.where(up, q_low, q_high) + g * jnp.where(up, s_low, s_high)


def kernel(
    sizes, flags_in, den, mom, en, disp, out_d, out_m, out_e, sums,
    flags, q, dxz, dy, xh, hop, xv, edge, zlo, zhi, cq, cs, part, slots, line, done,
    local_sem, send_sem, recv_sem, in_sem, sum_send, sum_recv,
):
    nx, ny, nz = den.shape
    pos = {a: lax.axis_index(a) for a in AXES}
    last = {a: sizes[a] - 1 for a in AXES}
    top = ny + SUB
    per = nz // 4
    parts = edge.shape[0]
    scale = 1.0 / 256.0
    xlo, xhi = xh.at[0], xh.at[1]
    dx, dz = dxz.at[0], dxz.at[1]
    own = slice(SUB, top)
    mesh_ids = pl.DeviceIdType.MESH

    def load(src, dst, k):
        return pltpu.make_async_copy(src, dst, local_sem.at[k])

    spans = (slice(0, 2), slice(nx - 2, nx), slice(2, nx - 2))
    loads = []
    for i, x in enumerate(spans):
        loads += [
            load(den.at[x], q.at[0, x, own], i),
            load(en.at[x], q.at[4, x, own], max(i, 3 - 3 * i)),
            load(mom.at[:, x], q.at[1:4, x, own], max(i, 3 - 3 * i)),
        ]
    loads += [
        load(flags_in, flags, 4),
        load(disp.at[0], dx, 5),
        load(disp.at[2], dz, 5),
        load(disp.at[1], dy.at[:, own], 6),
    ]
    for c in loads:
        c.start()

    def loaded(ref, k):
        load(ref, ref, k).wait()

    me = pos["gx"]
    par = lax.rem(me, 2)
    odd = par == 1
    end = last["gx"]
    sx, sy, sz = (sizes[a] for a in AXES)
    group = sx * sz
    leader = (me == 0) & (pos["gz"] == last["gz"])
    members = [{"gx": i // sz, "gz": last["gz"] - i % sz} for i in range(1, group)]

    def tell(sem, cond, **target):
        @pl.when(cond)
        def _():
            pl.semaphore_signal(sem, inc=1, device_id=target, device_id_type=mesh_ids)

    even = ~odd
    above = {a: pos[a] < last[a] for a in AXES}
    above_x, above_y, above_z = (above[a] for a in AXES)
    below_x, below_y, below_z = me > 0, pos["gy"] > 0, pos["gz"] > 0
    over = me + 2 <= end
    inner = even & below_x
    barrier = pltpu.get_barrier_semaphore()
    greetings = [
        (even & above_x, odd, {"gx": me + 1}),
        (over, me >= 2, {"gx": me + 2}),
        (above_y, below_y, {"gy": pos["gy"] + 1}),
        (above_z, below_z, {"gz": pos["gz"] + 1}),
    ]
    heard = jnp.where(leader, pos["gy"], 1)
    for speaks, hears, target in greetings:
        tell(barrier, speaks, **target)
        heard += jnp.where(hears, 1, 0)

    @pl.when(leader)
    def _():
        for target in members:
            tell(barrier, True, **target)
        for o in range(1, sy):
            tell(barrier, pos["gy"] + o <= last["gy"], gy=pos["gy"] + o)

    @pl.when(heard > 0)
    def _():
        pl.semaphore_wait(barrier, heard)

    tell(in_sem.at[0], odd, gx=me - 1)
    tell(in_sem.at[0], me >= 2, gx=me - 2)
    tell(in_sem.at[2], below_y, gy=pos["gy"] - 1)
    tell(in_sem.at[2], below_z, gz=pos["gz"] - 1)
    for o in range(1, sy):
        tell(in_sem.at[3], leader & (pos["gy"] >= o), gy=pos["gy"] - o)

    def is_in(k, cond, many=1):
        @pl.when(cond)
        def _():
            pl.semaphore_wait(in_sem.at[k], many)

    def copy(ks, kr, src, dst, axis, step):
        return pltpu.make_async_remote_copy(
            src_ref=src, dst_ref=dst, send_sem=send_sem.at[ks], recv_sem=recv_sem.at[kr],
            device_id={axis: pos[axis] + step}, device_id_type=mesh_ids,
        )

    hands_up, hands_down = odd & above_x, inner
    relays = (odd & (me >= 3)) | (even & over)
    beside = 1 - 2 * par
    main, across_x, legs_k, hand_k = 0, 1, 3, 4

    groups = (slice(3, 5), slice(1, 3), 0)
    tops, bottoms = slice(nx - 2, nx), slice(0, 2)

    def piece(k, i, x, side, first, step):
        f = groups[i]
        return copy(k, first + i, q.at[f, x, own], side.at[f], "gx", step)

    def one(k, r, x, side, i, step):
        return copy(k, r, q.at[0, x, own], side.at[0, i], "gx", step)

    up = [piece(main, i, tops, xlo, 0, 1) for i in range(3)]
    down = [piece(main, i, bottoms, xhi, 3, -1) for i in range(3)]
    v_down = copy(2, 6, dx.at[0], xv, "gx", -1)
    up_across = [piece(across_x, 0, tops, xlo, 0, 1), one(across_x, 2, nx - 1, xlo, 1, 1)]
    down_across = [piece(across_x, 0, bottoms, xhi, 3, -1), one(across_x, 5, 1, xhi, 1, -1)]
    legs_up = [
        copy(legs_k, 7, q.at[1:3, tops, own], hop.at[0:2], "gx", 2),
        copy(legs_k, 8, q.at[0, nx - 2, own], hop.at[2, 0], "gx", 2),
    ]
    legs_down = [
        copy(legs_k, 7, q.at[1:3, bottoms, own], hop.at[0:2], "gx", -2),
        copy(legs_k, 8, q.at[0, 0, own], hop.at[2, 0], "gx", -2),
    ]

    def handed(side):
        return [
            copy(hand_k, 9, hop.at[0:2], side.at[1:3], "gx", beside),
            copy(hand_k, 10, hop.at[2, 0], side.at[0, 0], "gx", beside),
        ]

    handed_up, handed_down = handed(xlo), handed(xhi)

    def each(cond, copies, act):
        @pl.when(cond)
        def _():
            for c in copies:
                act(c)

    def go(c):
        c.start()

    hi_rows = slice(top, top + SUB)
    y_up = [copy(5, 11, q.at[:, :, ny:top], q.at[:, :, 0:SUB], "gy", 1)]
    y_down = [
        copy(6, 12, q.at[:, :, SUB : 2 * SUB], q.at[:, :, hi_rows], "gy", -1),
        copy(7, 13, dy.at[:, SUB : 2 * SUB], dy.at[:, hi_rows], "gy", -1),
    ]
    z_up = [copy(8, 14, edge, zlo, "gz", 1)]
    z_down = [copy(9, 15, edge, zhi, "gz", -1)]

    def arrive(axis, ups, downs, fill_low, fill_high):
        @pl.when(pos[axis] > 0)
        def _():
            for c in ups:
                c.wait_recv()

        @pl.when(pos[axis] < last[axis])
        def _():
            for c in downs:
                c.wait_recv()

        @pl.when(pos[axis] == 0)
        def _():
            fill_low()

        @pl.when(pos[axis] == last[axis])
        def _():
            fill_high()

    def sent(axis, ups, downs):
        @pl.when(pos[axis] < last[axis])
        def _():
            for c in ups:
                c.wait_send()

        @pl.when(pos[axis] > 0)
        def _():
            for c in downs:
                c.wait_send()

    loaded(q.at[0, bottoms, own], 0)
    each(odd, down[2:], go)
    loaded(q.at[1:5, bottoms, own], 3)
    loaded(q.at[:, tops, own], 1)
    loaded(q.at[:, 2 : nx - 2, own], 2)
    load(flags_in, flags, 4).wait()
    loaded(dxz, 5)
    loaded(dy.at[:, own], 6)

    flag = [flags[i].astype(jnp.float32) for i in range(6)]

    def low_mult(a):
        return jnp.where(pos[AXES[a]] == 0, flag[2 * a], 1.0)

    def high_mult(a):
        return jnp.where(pos[AXES[a]] == last[AXES[a]], flag[2 * a + 1], 1.0)

    def outer_low(a):
        return jnp.where(pos[AXES[a]] == 0, flag[2 * a], 0.0)

    def outer_high(a):
        return jnp.where(pos[AXES[a]] == last[AXES[a]], flag[2 * a + 1], 0.0)

    lane = lax.broadcasted_iota(jnp.int32, (ny, nz), 1)
    row = lax.broadcasted_iota(jnp.int32, (ny, nz), 0)
    wz = jnp.where(lane == 0, outer_low(2), 0.0) - jnp.where(lane == nz - 1, outer_high(2), 0.0)
    wy = jnp.where(row == 0, outer_low(1), 0.0) - jnp.where(row == ny - 1, outer_high(1), 0.0)
    wx_low, wx_high = outer_low(0), outer_high(0)

    def total(x, carry):
        a, b = carry
        wx = jnp.where(x == 0, wx_low, 0.0) - jnp.where(x == nx - 1, wx_high, 0.0)
        w = 1.0 + scale * (
            wz * dz[x].astype(jnp.float32)
            + wy * dy[x, own].astype(jnp.float32)
            + wx * dx[x].astype(jnp.float32)
        )
        return (
            a + jnp.sum((q[0, x, own] * w).reshape(ny // SUB, SUB, nz), 0),
            b + jnp.sum((q[4, x, own] * w).reshape(ny // SUB, SUB, nz), 0),
        )

    zero = jnp.zeros((SUB, nz), jnp.float32)
    mass, power = lax.fori_loop(0, nx, total, (zero, zero))
    part[0:1] = jnp.sum(mass, 0, keepdims=True)
    part[1:2] = jnp.sum(power, 0, keepdims=True)

    def message(src, dst, ks, kr, target):
        return pltpu.make_async_remote_copy(
            src_ref=src, dst_ref=dst, send_sem=sum_send.at[ks], recv_sem=sum_recv.at[kr],
            device_id=target, device_id_type=mesh_ids,
        )

    home = {"gx": 0, "gz": last["gz"]}
    inward = message(part, slots.at[me * sz + last["gz"] - pos["gz"]], 0, 0, home)
    gathered = message(slots.at[1:group], slots.at[1:group], 1, 0, members[-1])
    across = [
        message(line.at[0], line.at[sy - o], 0, 1, {"gy": lax.rem(pos["gy"] + o, sy)})
        for o in range(1, sy)
    ]
    crossed = message(line.at[1:sy], line.at[1:sy], 0, 1, {"gy": lax.rem(pos["gy"] + 1, sy)})
    outward = [message(done, done, 1, 0, target) for target in members]

    each(~leader, [inward], go)

    each(hands_down, legs_down, go)
    each(below_y, y_down, go)

    def x_sends():
        each(odd, [v_down] + down[:2], go)
        waits = jnp.where(over, 1, 0) + jnp.where(above_x, 1, 0)
        is_in(0, waits > 0, waits)

        @pl.when(even & over)
        def _():
            tell(in_sem.at[0], True, gx=me + 1)
            tell(in_sem.at[1], True, gx=me + 2)

        each(even & above_x, up[:1], go)
        each(odd & over, legs_up, go)
        each(hands_up, up_across, go)
        is_in(1, hands_down)
        each(hands_down, [v_down] + down_across, go)
        each(even & above_x, up[1:], go)

    pl.when(below_x | below_y)(x_sends)

    def pack(x, carry):
        new = list(carry)
        for f in range(6):
            p = f * nx + x
            k = f * nx // per
            at = 4 * lax.rem(p, per)
            plane = q[f, x, own] if f < 5 else dz[x].astype(jnp.float32)
            moved = pltpu.roll(plane, at, 1)
            mine = lax.rem(lane + 2 - at + nz, nz) < 4
            new[k] = jnp.where(mine, moved, new[k])
        return tuple(new)

    packed = lax.fori_loop(0, nx, pack, tuple(jnp.zeros((ny, nz), jnp.float32) for _ in range(parts)))
    for k in range(parts):
        edge[k] = packed[k]
    each(below_z, z_down, go)
    beyond = jnp.where(above_y, 1, 0) + jnp.where(above_z, 1, 0)
    is_in(2, beyond > 0, beyond)
    each(above_z, z_up, go)
    pl.when(~below_x & ~below_y)(x_sends)
    each(above_y, y_up, go)

    outs = (
        lambda x: out_d.at[x], lambda x: out_m.at[0, x], lambda x: out_m.at[1, x],
        lambda x: out_m.at[2, x], lambda x: out_e.at[x],
    )

    def core(r, _):
        at = pl.ds(pl.multiple_of(r * SUB, SUB), SUB)
        inner = pl.ds(pl.multiple_of(r * SUB + SUB, SUB), SUB)
        vs = [dx[c, at].astype(jnp.float32) * scale for c in range(2, nx - 1)]
        gs = [gain(v) for v in vs]
        for f in range(5):
            line_q = [q[f, c, inner] for c in range(nx)]
            ds = [line_q[i + 1] - line_q[i] for i in range(nx - 1)]
            ss = [minmod(ds[i + 1], ds[i]) for i in range(nx - 2)]
            fl = [
                flux(vs[i], gs[i], line_q[i + 1], line_q[i + 2], ss[i], ss[i + 1])
                for i in range(nx - 3)
            ]
            for c in range(nx):
                new = line_q[c]
                if 2 <= c < nx - 1:
                    new = new + fl[c - 2]
                if 1 <= c < nx - 2:
                    new = new - fl[c - 1]
                outs[f](c)[at] = new
        return 0

    lax.fori_loop(0, ny // SUB, core, 0)

    def z_low():
        e = edge[...]
        zlo[...] = jnp.where(lane3 & 3 == 3, pltpu.roll(e, nz - 1, 2), pltpu.roll(e, nz - 2, 2))

    def z_high():
        e = edge[...]
        zhi[...] = jnp.where(lane3 & 3 == 0, pltpu.roll(e, 1, 2), pltpu.roll(e, 2, 2))

    lane3 = lax.broadcasted_iota(jnp.int32, (parts, ny, nz), 2)
    arrive("gz", z_up, z_down, z_low, z_high)
    low = lane & 3 == 0
    for k in range(parts):
        e, l, h = edge[k], zlo[k], zhi[k]
        r1, r2 = pltpu.roll(l, 1, 1), pltpu.roll(l, 2, 1)
        l1, l2 = pltpu.roll(h, nz - 1, 1), pltpu.roll(h, nz - 2, 1)
        cq[k] = jnp.where(low, r1, l1)
        cs[k] = jnp.where(low, minmod(e - r1, r1 - r2), minmod(l2 - l1, l1 - e))

    first, final = lane == 0, lane == nz - 1
    z_lo_mult = jnp.where(first, low_mult(2), 1.0) * scale
    z_hi_mult = high_mult(2) * scale
    def along_z(x, _):
        v = dz[x].astype(jnp.float32) * z_lo_mult
        g = gain(v)

        def ghosts(ref, f):
            back = lax.rem(nz - 4 * lax.rem(f * nx + x, per), nz)
            return pltpu.roll(ref[f * nx // per], back, 1)

        vh = ghosts(cq, 5) * z_hi_mult
        gh = gain(vh)
        for f in range(5):
            plane = q[f, x, SUB:top]
            gq, gs = ghosts(cq, f), ghosts(cs, f)
            qm = jnp.where(first, gq, pltpu.roll(plane, 1, 1))
            d = plane - qm
            s = minmod(jnp.where(final, gq - plane, pltpu.roll(d, nz - 1, 1)), d)
            sm = jnp.where(first, gs, pltpu.roll(s, 1, 1))
            fl = flux(v, g, qm, plane, sm, s)
            fh = jnp.where(final, flux(vh, gh, plane, gq, s, gs), pltpu.roll(fl, nz - 1, 1))
            outs[f](x)[...] += fl - fh
        return 0

    early = nx * 5 // 8
    lax.fori_loop(0, early, along_z, 0)

    def gather():
        gathered.wait_recv()
        line[0] = part[...] + jnp.sum(slots[1:group], 0)
        is_in(3, above_y, last["gy"] - pos["gy"])
        for c in across:
            c.start()

    pl.when(leader & below_y)(gather)
    lax.fori_loop(early, nx, along_z, 0)

    def hand_on(cond, legs, onward):
        @pl.when(relays & cond)
        def _():
            for a, b in zip(legs, onward):
                a.wait_recv()
                b.start()

    hand_on(odd, legs_up, handed_up)
    hand_on(even, legs_down, handed_down)

    def y_low():
        q[:, :, 0:SUB] = jnp.broadcast_to(q[:, :, SUB : SUB + 1], (5, nx, SUB, nz))

    def y_high():
        q[:, :, hi_rows] = jnp.broadcast_to(q[:, :, top - 1 : top], (5, nx, SUB, nz))
        dy[:, hi_rows] = jnp.broadcast_to(dy[:, top - 1 : top], (nx, SUB, nz))

    arrive("gy", y_up, y_down, y_low, y_high)
    pl.when(leader & ~below_y)(gather)
    tall = ny + 2 * SUB
    rows = lax.broadcasted_iota(jnp.int32, (tall, nz), 0)
    inside = (rows >= SUB) & (rows <= top)
    y_mult = jnp.where(
        rows == SUB, low_mult(1) * scale, jnp.where(rows == top, high_mult(1) * scale, scale)
    )

    def along_y(x, _):
        v = jnp.where(inside, dy[x].astype(jnp.float32), 0.0) * y_mult
        g = gain(v)
        for f in range(5):
            plane = q[f, x]
            qm = pltpu.roll(plane, 1, 0)
            d = plane - qm
            s = minmod(pltpu.roll(d, tall - 1, 0), d)
            fl = flux(v, g, qm, plane, pltpu.roll(s, 1, 0), s)
            ch = fl - pltpu.roll(fl, tall - 1, 0)
            outs[f](x)[...] += ch[SUB:top]
        return 0

    lax.fori_loop(0, nx, along_y, 0)

    @pl.when(me == 0)
    def _():
        xlo[...] = jnp.broadcast_to(q[:, 0:1, own], (5, 2, ny, nz))

    @pl.when(me == end)
    def _():
        xhi[...] = jnp.broadcast_to(q[:, nx - 1 : nx, own], (5, 2, ny, nz))
        xv[...] = dx[nx - 1]

    each(above_x, [v_down], lambda c: c.wait_recv())
    x_lo_mult, x_hi_mult = low_mult(0) * scale, high_mult(0) * scale

    def rim(high, f):
        def rows(r, _):
            at = pl.ds(pl.multiple_of(r * SUB, SUB), SUB)
            inner = pl.ds(pl.multiple_of(r * SUB + SUB, SUB), SUB)
            if high:
                cells = [q[f, c, inner] for c in range(nx - 3, nx)] + [xhi[f, i, at] for i in range(2)]
                vs = (dx[nx - 1, at].astype(jnp.float32) * scale, xv[at].astype(jnp.float32) * x_hi_mult)
            else:
                cells = [xlo[f, i, at] for i in range(2)] + [q[f, c, inner] for c in range(3)]
                vs = (dx[0, at].astype(jnp.float32) * x_lo_mult, dx[1, at].astype(jnp.float32) * scale)
            ds = [cells[i + 1] - cells[i] for i in range(4)]
            ss = [minmod(ds[i + 1], ds[i]) for i in range(3)]
            fl = [
                flux(vs[i], gain(vs[i]), cells[i + 1], cells[i + 2], ss[i], ss[i + 1])
                for i in range(2)
            ]
            if high:
                changes = ((nx - 2, -fl[0]), (nx - 1, fl[0] - fl[1]))
            else:
                changes = ((0, fl[0] - fl[1]), (1, fl[1]))
            for c, change in changes:
                ref = outs[f](c)
                ref[at] += change
            return 0

        lax.fori_loop(0, ny // SUB, rows, 0)

    def come(cond, copies):
        each(cond, copies, lambda c: c.wait_recv())

    def rims(high, i):
        for f in ((3, 4), (1, 2), (0,))[i]:
            rim(high, f)

    def lower(i):
        come(odd, [up[i]])
        come(hands_down, ([up_across[0]], handed_up[:1], [up_across[1], handed_up[1]])[i])
        rims(False, i)

    def upper(i):
        come(even & above_x, [down[i]])
        come(hands_up, ([down_across[0]], handed_down[:1], [down_across[1], handed_down[1]])[i])
        rims(True, i)

    def finish():
        crossed.wait_recv()
        done[...] = jnp.sum(line[...], 0)
        for c in outward:
            c.start()

    @pl.when(hands_up)
    def _():
        upper(0)
        for i in range(3):
            lower(i)
        upper(1)
        upper(2)

    @pl.when(odd & ~above_x)
    def _():
        for i in range(3):
            upper(i)
        for i in range(3):
            lower(i)

    @pl.when(hands_down)
    def _():
        for i in (2, 0, 1):
            upper(i)
        for i in range(3):
            lower(i)

    @pl.when(~below_x)
    def _():
        for i in range(3):
            lower(i)
        pl.when(leader)(finish)
        for i in (2, 0, 1):
            upper(i)

    @pl.when(~leader)
    def _():
        outward[0].wait_recv()
        inward.wait_send()

    sums[...] = done[...]

    @pl.when(leader)
    def _():
        crossed.wait_send()
        gathered.wait_send()

    def sent(k, cond, ref):
        @pl.when(cond)
        def _():
            copy(k, 0, ref, ref, "gx", 1 - 2 * par).wait_send()

    sent(main, even & above_x | odd, xlo)
    sent(2, below_x, xv)
    five = q.at[:, 0, own]
    sent(across_x, hands_up | hands_down, five)
    sent(legs_k, odd & over | hands_down, five)
    sent(hand_k, relays, five)
    for cond, copies in ((above_y, y_up), (below_y, y_down), (above_z, z_up), (below_z, z_down)):
        each(cond, copies, lambda c: c.wait_send())


def put(cells, den, mom, en, sums, out_d, out_m, out_e, totals, mean, sem):
    half = den.shape[0] // 2
    pairs = ((den, out_d), (en, out_e), (mom, out_m))
    for i, (src, dst) in enumerate(pairs):
        for h in (pl.ds(0, half), pl.ds(half, den.shape[0] - half)):
            for at in ((h,),) if i < 2 else tuple((c, h) for c in range(3)):
                pltpu.make_async_copy(src.at[at], dst.at[at], sem.at[i]).start()
    mean[0] = jnp.sum(sums[0:1]) / cells
    mean[1] = jnp.sum(sums[1:2]) / cells
    last = pltpu.make_async_copy(mean, totals, sem.at[3])
    last.start()
    for i, (src, dst) in enumerate(pairs):
        pltpu.make_async_copy(src, dst, sem.at[i]).wait()
    last.wait()


def shards(density, momentum, energy, displacement, flags):
    sizes = {a: lax.axis_size(a) for a in AXES}
    nx, ny, nz = density.shape
    tall = ny + 2 * SUB
    per = nz // 4
    parts = -(-6 * nx // per)
    f32, i32 = jnp.float32, jnp.int32
    dma = pltpu.SemaphoreType.DMA
    any_ = pl.BlockSpec(memory_space=pl.ANY)
    hbm = pl.BlockSpec(memory_space=pltpu.HBM)
    vmem = pl.BlockSpec(memory_space=pltpu.VMEM)
    devices = 1
    for a in AXES:
        devices *= sizes[a]
    cells = float(nx * ny * nz * devices)
    outputs = tuple(jax.ShapeDtypeStruct(v.shape, f32) for v in (density, momentum, energy))
    results = pl.pallas_call(
        functools.partial(kernel, sizes),
        out_shape=outputs + (jax.ShapeDtypeStruct((2, nz), f32),),
        in_specs=[hbm] * 5,
        out_specs=(vmem, vmem, vmem, vmem),
        scratch_shapes=[
            pltpu.SMEM((6,), i32),
            pltpu.VMEM((5, nx, tall, nz), f32),
            pltpu.VMEM((2, nx, ny, nz), i32),
            pltpu.VMEM((nx, tall, nz), i32),
            pltpu.VMEM((2, 5, 2, ny, nz), f32),
            pltpu.VMEM((3, 2, ny, nz), f32),
            pltpu.VMEM((ny, nz), i32),
        ]
        + [pltpu.VMEM((parts, ny, nz), f32) for _ in range(5)]
        + [pltpu.VMEM((2, nz), f32), pltpu.VMEM((sizes["gx"] * sizes["gz"], 2, nz), f32)]
        + [pltpu.VMEM((sizes["gy"], 2, nz), f32), pltpu.VMEM((2, nz), f32)]
        + [dma((7,)), dma((10,)), dma((16,)), pltpu.SemaphoreType.REGULAR((4,)), dma((2,)), dma((2,))],
        compiler_params=pltpu.CompilerParams(
            collective_id=0, has_side_effects=True, vmem_limit_bytes=12 << 20
        ),
    )(
        *(
            pltpu.with_memory_space_constraint(v, pltpu.HBM)
            for v in (flags, density, momentum, energy, displacement)
        )
    )
    return pl.pallas_call(
        functools.partial(put, cells),
        out_shape=outputs + (jax.ShapeDtypeStruct((2,), f32),),
        in_specs=[any_, any_, any_, vmem],
        out_specs=(hbm, hbm, hbm, hbm),
        scratch_shapes=[pltpu.SMEM((2,), f32), dma((4,))],
        compiler_params=pltpu.CompilerParams(vmem_limit_bytes=2 << 20),
    )(*results)


def solution(mesh):
    return jax.shard_map(
        shards,
        mesh=mesh,
        in_specs=(
            P("gx", "gy", "gz"),
            P(None, "gx", "gy", "gz"),
            P("gx", "gy", "gz"),
            P(None, "gx", "gy", "gz"),
            P(),
        ),
        out_specs=(P("gx", "gy", "gz"), P(None, "gx", "gy", "gz"), P("gx", "gy", "gz"), P()),
        check_vma=False,
    )
```

```python
import functools

import jax
import jax.numpy as jnp
from jax import lax
from jax.experimental import pallas as pl
from jax.experimental.pallas import tpu as pltpu
from jax.sharding import PartitionSpec as P

AXES = ("gx", "gy", "gz")
SUB = 8


def minmod(p, r):
    return jnp.maximum(jnp.minimum(r, 0.0), jnp.minimum(p, jnp.maximum(r, 0.0)))


def gain(v):
    size = jnp.abs(v)
    return 0.5 * size * (1.0 - size)


def flux(v, g, q_low, q_high, s_low, s_high):
    up = v > 0
    return v * jnp.where(up, q_low, q_high) + g * jnp.where(up, s_low, s_high)


def kernel(
    sizes, flags_in, den, mom, en, disp, out_d, out_m, out_e, sums,
    flags, q, dxz, dy, xh, hop, xv, edge, zlo, zhi, cq, cs, part, slots, line, done,
    send_sem, recv_sem, in_sem, sum_send, sum_recv,
):
    nx, ny, nz = den.shape
    pos = {a: lax.axis_index(a) for a in AXES}
    last = {a: sizes[a] - 1 for a in AXES}
    top = ny + SUB
    per = nz // 4
    parts = edge.shape[0]
    scale = 1.0 / 256.0
    xlo, xhi = xh.at[0], xh.at[1]
    dx, dz = dxz.at[0], dxz.at[1]
    own = slice(SUB, top)
    mesh_ids = pl.DeviceIdType.MESH

    def load(src, dst, k):
        return pltpu.make_async_copy(src, dst, send_sem.at[k])

    spans = (slice(0, 2), slice(nx - 2, nx), slice(2, nx - 2))
    loads = []
    for i, x in enumerate(spans):
        loads += [
            load(den.at[x], q.at[0, x, own], i),
            load(en.at[x], q.at[4, x, own], max(i, 3 - 3 * i)),
            load(mom.at[:, x], q.at[1:4, x, own], max(i, 3 - 3 * i)),
        ]
    loads += [
        load(flags_in, flags, 4),
        load(disp.at[0], dx, 5),
        load(disp.at[2], dz, 5),
        load(disp.at[1], dy.at[:, own], 6),
    ]
    for c in loads:
        c.start()

    def loaded(ref, k):
        load(ref, ref, k).wait()

    me = pos["gx"]
    par = lax.rem(me, 2)
    odd = par == 1
    end = last["gx"]
    sx, sy, sz = (sizes[a] for a in AXES)
    group = sx * sz
    leader = (me == 0) & (pos["gz"] == last["gz"])
    members = [{"gx": i // sz, "gz": last["gz"] - i % sz} for i in range(1, group)]

    def tell(sem, cond, **target):
        @pl.when(cond)
        def _():
            pl.semaphore_signal(sem, inc=1, device_id=target, device_id_type=mesh_ids)

    even = ~odd
    above = {a: pos[a] < last[a] for a in AXES}
    above_x, above_y, above_z = (above[a] for a in AXES)
    below_x, below_y, below_z = me > 0, pos["gy"] > 0, pos["gz"] > 0
    over = me + 2 <= end
    inner = even & below_x
    barrier = pltpu.get_barrier_semaphore()
    greetings = [
        (even & above_x, odd, {"gx": me + 1}),
        (over, me >= 2, {"gx": me + 2}),
        (above_y, below_y, {"gy": pos["gy"] + 1}),
        (above_z, below_z, {"gz": pos["gz"] + 1}),
    ]
    heard = jnp.where(leader, pos["gy"], 1)
    for speaks, hears, target in greetings:
        tell(barrier, speaks, **target)
        heard += jnp.where(hears, 1, 0)

    @pl.when(leader)
    def _():
        for target in members:
            tell(barrier, True, **target)
        for o in range(1, sy):
            tell(barrier, pos["gy"] + o <= last["gy"], gy=pos["gy"] + o)

    @pl.when(heard > 0)
    def _():
        pl.semaphore_wait(barrier, heard)

    tell(in_sem.at[0], odd, gx=me - 1)
    tell(in_sem.at[0], me >= 2, gx=me - 2)
    tell(in_sem.at[2], below_y, gy=pos["gy"] - 1)
    tell(in_sem.at[2], below_z, gz=pos["gz"] - 1)
    for o in range(1, sy):
        tell(in_sem.at[3], leader & (pos["gy"] >= o), gy=pos["gy"] - o)

    def is_in(k, cond, many=1):
        @pl.when(cond)
        def _():
            pl.semaphore_wait(in_sem.at[k], many)

    def copy(ks, kr, src, dst, axis, step):
        return pltpu.make_async_remote_copy(
            src_ref=src, dst_ref=dst, send_sem=send_sem.at[ks], recv_sem=recv_sem.at[kr],
            device_id={axis: pos[axis] + step}, device_id_type=mesh_ids,
        )

    hands_up, hands_down = odd & above_x, inner
    relays = (odd & (me >= 3)) | (even & over)
    beside = 1 - 2 * par
    main, across_x, legs_k, hand_k = 0, 1, 3, 4

    groups = (slice(3, 5), slice(1, 3), 0)
    tops, bottoms = slice(nx - 2, nx), slice(0, 2)

    def piece(k, i, x, side, first, step):
        f = groups[i]
        return copy(k, first + i, q.at[f, x, own], side.at[f], "gx", step)

    def one(k, r, x, side, i, step):
        return copy(k, r, q.at[0, x, own], side.at[0, i], "gx", step)

    up = [piece(main, i, tops, xlo, 0, 1) for i in range(3)]
    down = [piece(main, i, bottoms, xhi, 3, -1) for i in range(3)]
    v_down = copy(2, 6, dx.at[0], xv, "gx", -1)
    up_across = [piece(across_x, 0, tops, xlo, 0, 1), one(across_x, 2, nx - 1, xlo, 1, 1)]
    down_across = [piece(across_x, 0, bottoms, xhi, 3, -1), one(across_x, 5, 1, xhi, 1, -1)]
    legs_up = [
        copy(legs_k, 7, q.at[1:3, tops, own], hop.at[0:2], "gx", 2),
        copy(legs_k, 7, q.at[0, nx - 2, own], hop.at[2, 0], "gx", 2),
    ]
    legs_down = [
        copy(legs_k, 7, q.at[1:3, bottoms, own], hop.at[0:2], "gx", -2),
        copy(legs_k, 7, q.at[0, 0, own], hop.at[2, 0], "gx", -2),
    ]

    def handed(side):
        return [
            copy(hand_k, 8, hop.at[0:2], side.at[1:3], "gx", beside),
            copy(hand_k, 9, hop.at[2, 0], side.at[0, 0], "gx", beside),
        ]

    handed_up, handed_down = handed(xlo), handed(xhi)

    def each(cond, copies, act):
        @pl.when(cond)
        def _():
            for c in copies:
                act(c)

    def go(c):
        c.start()

    hi_rows = slice(top, top + SUB)
    y_up = [copy(5, 10, q.at[:, :, ny:top], q.at[:, :, 0:SUB], "gy", 1)]
    y_down = [
        copy(6, 11, q.at[:, :, SUB : 2 * SUB], q.at[:, :, hi_rows], "gy", -1),
        copy(7, 12, dy.at[:, SUB : 2 * SUB], dy.at[:, hi_rows], "gy", -1),
    ]
    both = sz > 2
    z_up = [copy(8, 13, edge, zlo, "gz", 1)]
    z_down = [copy(8 + both, 13 + both, edge, zhi, "gz", -1)]

    def arrive(axis, ups, downs, fill_low, fill_high):
        @pl.when(pos[axis] > 0)
        def _():
            for c in ups:
                c.wait_recv()

        @pl.when(pos[axis] < last[axis])
        def _():
            for c in downs:
                c.wait_recv()

        @pl.when(pos[axis] == 0)
        def _():
            fill_low()

        @pl.when(pos[axis] == last[axis])
        def _():
            fill_high()

    def sent(axis, ups, downs):
        @pl.when(pos[axis] < last[axis])
        def _():
            for c in ups:
                c.wait_send()

        @pl.when(pos[axis] > 0)
        def _():
            for c in downs:
                c.wait_send()

    loaded(q.at[0, bottoms, own], 0)
    each(odd, down[2:], go)
    loaded(q.at[1:5, bottoms, own], 3)
    loaded(q.at[:, tops, own], 1)
    loaded(q.at[:, 2 : nx - 2, own], 2)
    load(flags_in, flags, 4).wait()
    loaded(dxz, 5)
    loaded(dy.at[:, own], 6)

    flag = [flags[i].astype(jnp.float32) for i in range(6)]

    def low_mult(a):
        return jnp.where(pos[AXES[a]] == 0, flag[2 * a], 1.0)

    def high_mult(a):
        return jnp.where(pos[AXES[a]] == last[AXES[a]], flag[2 * a + 1], 1.0)

    def outer_low(a):
        return jnp.where(pos[AXES[a]] == 0, flag[2 * a], 0.0)

    def outer_high(a):
        return jnp.where(pos[AXES[a]] == last[AXES[a]], flag[2 * a + 1], 0.0)

    lane = lax.broadcasted_iota(jnp.int32, (ny, nz), 1)
    row = lax.broadcasted_iota(jnp.int32, (ny, nz), 0)
    wz = jnp.where(lane == 0, outer_low(2), 0.0) - jnp.where(lane == nz - 1, outer_high(2), 0.0)
    wy = jnp.where(row == 0, outer_low(1), 0.0) - jnp.where(row == ny - 1, outer_high(1), 0.0)
    wx_low, wx_high = outer_low(0), outer_high(0)

    def total(x, carry):
        a, b = carry
        wx = jnp.where(x == 0, wx_low, 0.0) - jnp.where(x == nx - 1, wx_high, 0.0)
        w = 1.0 + scale * (
            wz * dz[x].astype(jnp.float32)
            + wy * dy[x, own].astype(jnp.float32)
            + wx * dx[x].astype(jnp.float32)
        )
        return (
            a + jnp.sum((q[0, x, own] * w).reshape(ny // SUB, SUB, nz), 0),
            b + jnp.sum((q[4, x, own] * w).reshape(ny // SUB, SUB, nz), 0),
        )

    zero = jnp.zeros((SUB, nz), jnp.float32)
    mass, power = lax.fori_loop(0, nx, total, (zero, zero))
    part[0:1] = jnp.sum(mass, 0, keepdims=True)
    part[1:2] = jnp.sum(power, 0, keepdims=True)

    def message(src, dst, ks, kr, target):
        return pltpu.make_async_remote_copy(
            src_ref=src, dst_ref=dst, send_sem=sum_send.at[ks], recv_sem=sum_recv.at[kr],
            device_id=target, device_id_type=mesh_ids,
        )

    home = {"gx": 0, "gz": last["gz"]}
    inward = message(part, slots.at[me * sz + last["gz"] - pos["gz"]], 0, 0, home)
    gathered = message(slots.at[1:group], slots.at[1:group], 1, 0, members[-1])
    across = [
        message(line.at[0], line.at[sy - o], 0, 1, {"gy": lax.rem(pos["gy"] + o, sy)})
        for o in range(1, sy)
    ]
    crossed = message(line.at[1:sy], line.at[1:sy], 0, 1, {"gy": lax.rem(pos["gy"] + 1, sy)})
    outward = [message(done, done, 1, 0, target) for target in members]

    each(~leader, [inward], go)

    each(hands_down, legs_down, go)
    each(below_y, y_down, go)

    def x_sends():
        each(odd, [v_down] + down[:2], go)
        waits = jnp.where(over, 1, 0) + jnp.where(above_x, 1, 0)
        is_in(0, waits > 0, waits)

        @pl.when(even & over)
        def _():
            tell(in_sem.at[0], True, gx=me + 1)
            tell(in_sem.at[1], True, gx=me + 2)

        each(even & above_x, up[:1], go)
        each(odd & over, legs_up, go)
        each(hands_up, up_across, go)
        is_in(1, hands_down)
        each(hands_down, [v_down] + down_across, go)
        each(even & above_x, up[1:], go)

    pl.when(below_x | below_y)(x_sends)

    def pack(x, carry):
        new = list(carry)
        for f in range(6):
            p = f * nx + x
            k = f * nx // per
            at = 4 * lax.rem(p, per)
            plane = q[f, x, own] if f < 5 else dz[x].astype(jnp.float32)
            moved = pltpu.roll(plane, at, 1)
            mine = lax.rem(lane + 2 - at + nz, nz) < 4
            new[k] = jnp.where(mine, moved, new[k])
        return tuple(new)

    packed = lax.fori_loop(0, nx, pack, tuple(jnp.zeros((ny, nz), jnp.float32) for _ in range(parts)))
    for k in range(parts):
        edge[k] = packed[k]
    each(below_z, z_down, go)
    beyond = jnp.where(above_y, 1, 0) + jnp.where(above_z, 1, 0)
    is_in(2, beyond > 0, beyond)
    each(above_z, z_up, go)
    pl.when(~below_x & ~below_y)(x_sends)
    each(above_y, y_up, go)

    outs = (
        lambda x: out_d.at[x], lambda x: out_m.at[0, x], lambda x: out_m.at[1, x],
        lambda x: out_m.at[2, x], lambda x: out_e.at[x],
    )

    def core(r, _):
        at = pl.ds(pl.multiple_of(r * SUB, SUB), SUB)
        inner = pl.ds(pl.multiple_of(r * SUB + SUB, SUB), SUB)
        vs = [dx[c, at].astype(jnp.float32) * scale for c in range(2, nx - 1)]
        gs = [gain(v) for v in vs]
        for f in range(5):
            line_q = [q[f, c, inner] for c in range(nx)]
            ds = [line_q[i + 1] - line_q[i] for i in range(nx - 1)]
            ss = [minmod(ds[i + 1], ds[i]) for i in range(nx - 2)]
            fl = [
                flux(vs[i], gs[i], line_q[i + 1], line_q[i + 2], ss[i], ss[i + 1])
                for i in range(nx - 3)
            ]
            for c in range(nx):
                new = line_q[c]
                if 2 <= c < nx - 1:
                    new = new + fl[c - 2]
                if 1 <= c < nx - 2:
                    new = new - fl[c - 1]
                outs[f](c)[at] = new
        return 0

    lax.fori_loop(0, ny // SUB, core, 0)

    def z_low():
        e = edge[...]
        zlo[...] = jnp.where(lane3 & 3 == 3, pltpu.roll(e, nz - 1, 2), pltpu.roll(e, nz - 2, 2))

    def z_high():
        e = edge[...]
        zhi[...] = jnp.where(lane3 & 3 == 0, pltpu.roll(e, 1, 2), pltpu.roll(e, 2, 2))

    lane3 = lax.broadcasted_iota(jnp.int32, (parts, ny, nz), 2)
    arrive("gz", z_up, z_down, z_low, z_high)
    low = lane & 3 == 0
    for k in range(parts):
        e, l, h = edge[k], zlo[k], zhi[k]
        r1, r2 = pltpu.roll(l, 1, 1), pltpu.roll(l, 2, 1)
        l1, l2 = pltpu.roll(h, nz - 1, 1), pltpu.roll(h, nz - 2, 1)
        cq[k] = jnp.where(low, r1, l1)
        cs[k] = jnp.where(low, minmod(e - r1, r1 - r2), minmod(l2 - l1, l1 - e))

    first, final = lane == 0, lane == nz - 1
    z_lo_mult = jnp.where(first, low_mult(2), 1.0) * scale
    z_hi_mult = high_mult(2) * scale
    def along_z(x, _):
        v = dz[x].astype(jnp.float32) * z_lo_mult
        g = gain(v)

        def ghosts(ref, f):
            back = lax.rem(nz - 4 * lax.rem(f * nx + x, per), nz)
            return pltpu.roll(ref[f * nx // per], back, 1)

        vh = ghosts(cq, 5) * z_hi_mult
        gh = gain(vh)
        for f in range(5):
            plane = q[f, x, SUB:top]
            gq, gs = ghosts(cq, f), ghosts(cs, f)
            qm = jnp.where(first, gq, pltpu.roll(plane, 1, 1))
            d = plane - qm
            s = minmod(jnp.where(final, gq - plane, pltpu.roll(d, nz - 1, 1)), d)
            sm = jnp.where(first, gs, pltpu.roll(s, 1, 1))
            fl = flux(v, g, qm, plane, sm, s)
            fh = jnp.where(final, flux(vh, gh, plane, gq, s, gs), pltpu.roll(fl, nz - 1, 1))
            outs[f](x)[...] += fl - fh
        return 0

    early = nx * 5 // 8
    lax.fori_loop(0, early, along_z, 0)

    def gather():
        gathered.wait_recv()
        line[0] = part[...] + jnp.sum(slots[1:group], 0)
        is_in(3, above_y, last["gy"] - pos["gy"])
        for c in across:
            c.start()

    pl.when(leader & below_y)(gather)
    lax.fori_loop(early, nx, along_z, 0)

    @pl.when(relays)
    def _():
        copy(legs_k, 7, q.at[:, 0, own], q.at[:, 0, own], "gx", beside).wait_recv()

    each(relays & odd, handed_up, go)
    each(relays & even, handed_down, go)

    def y_low():
        q[:, :, 0:SUB] = jnp.broadcast_to(q[:, :, SUB : SUB + 1], (5, nx, SUB, nz))

    def y_high():
        q[:, :, hi_rows] = jnp.broadcast_to(q[:, :, top - 1 : top], (5, nx, SUB, nz))
        dy[:, hi_rows] = jnp.broadcast_to(dy[:, top - 1 : top], (nx, SUB, nz))

    arrive("gy", y_up, y_down, y_low, y_high)
    pl.when(leader & ~below_y)(gather)
    tall = ny + 2 * SUB
    rows = lax.broadcasted_iota(jnp.int32, (tall, nz), 0)
    inside = (rows >= SUB) & (rows <= top)
    y_mult = jnp.where(
        rows == SUB, low_mult(1) * scale, jnp.where(rows == top, high_mult(1) * scale, scale)
    )

    def along_y(x, _):
        v = jnp.where(inside, dy[x].astype(jnp.float32), 0.0) * y_mult
        g = gain(v)
        for f in range(5):
            plane = q[f, x]
            qm = pltpu.roll(plane, 1, 0)
            d = plane - qm
            s = minmod(pltpu.roll(d, tall - 1, 0), d)
            fl = flux(v, g, qm, plane, pltpu.roll(s, 1, 0), s)
            ch = fl - pltpu.roll(fl, tall - 1, 0)
            outs[f](x)[...] += ch[SUB:top]
        return 0

    lax.fori_loop(0, nx, along_y, 0)

    @pl.when(me == 0)
    def _():
        xlo[...] = jnp.broadcast_to(q[:, 0:1, own], (5, 2, ny, nz))

    @pl.when(me == end)
    def _():
        xhi[...] = jnp.broadcast_to(q[:, nx - 1 : nx, own], (5, 2, ny, nz))
        xv[...] = dx[nx - 1]

    each(above_x, [v_down], lambda c: c.wait_recv())
    x_lo_mult, x_hi_mult = low_mult(0) * scale, high_mult(0) * scale

    tile = 4 * SUB if ny % (4 * SUB) == 0 else SUB

    def rim(high, f):
        def rows(r, _):
            at = pl.ds(pl.multiple_of(r * tile, SUB), tile)
            inner = pl.ds(pl.multiple_of(r * tile + SUB, SUB), tile)
            if high:
                cells = [q[f, c, inner] for c in range(nx - 3, nx)] + [xhi[f, i, at] for i in range(2)]
                vs = (dx[nx - 1, at].astype(jnp.float32) * scale, xv[at].astype(jnp.float32) * x_hi_mult)
            else:
                cells = [xlo[f, i, at] for i in range(2)] + [q[f, c, inner] for c in range(3)]
                vs = (dx[0, at].astype(jnp.float32) * x_lo_mult, dx[1, at].astype(jnp.float32) * scale)
            ds = [cells[i + 1] - cells[i] for i in range(4)]
            ss = [minmod(ds[i + 1], ds[i]) for i in range(3)]
            fl = [
                flux(vs[i], gain(vs[i]), cells[i + 1], cells[i + 2], ss[i], ss[i + 1])
                for i in range(2)
            ]
            if high:
                changes = ((nx - 2, -fl[0]), (nx - 1, fl[0] - fl[1]))
            else:
                changes = ((0, fl[0] - fl[1]), (1, fl[1]))
            for c, change in changes:
                ref = outs[f](c)
                ref[at] += change
            return 0

        lax.fori_loop(0, ny // tile, rows, 0)

    def come(cond, copies):
        each(cond, copies, lambda c: c.wait_recv())

    def rims(high, i):
        for f in ((3, 4), (1, 2), (0,))[i]:
            rim(high, f)

    def lower(i):
        come(odd, [up[i]])
        come(hands_down, ([up_across[0]], handed_up[:1], [up_across[1], handed_up[1]])[i])
        rims(False, i)

    def upper(i):
        come(even & above_x, [down[i]])
        come(hands_up, ([down_across[0]], handed_down[:1], [down_across[1], handed_down[1]])[i])
        rims(True, i)

    def finish():
        crossed.wait_recv()
        done[...] = jnp.sum(line[...], 0)
        for c in outward:
            c.start()

    pl.when(leader)(finish)

    def sides(turn, _):
        @pl.when((turn == 1) == hands_up)
        def _():
            for i in (2, 0, 1):
                upper(i)

        @pl.when(turn == 0)
        def _():
            for i in range(3):
                lower(i)

        return 0

    lax.fori_loop(0, 2, sides, 0)

    @pl.when(~leader)
    def _():
        outward[0].wait_recv()
        inward.wait_send()

    sums[...] = done[...]

    @pl.when(leader)
    def _():
        crossed.wait_send()
        gathered.wait_send()

    def sent(k, cond, ref):
        @pl.when(cond)
        def _():
            copy(k, 0, ref, ref, "gx", 1 - 2 * par).wait_send()

    sent(main, even & above_x | odd, xlo)
    sent(2, below_x, xv)
    five = q.at[:, 0, own]
    sent(across_x, hands_up | hands_down, five)
    sent(legs_k, odd & over | hands_down, five)
    sent(hand_k, relays, five)
    for cond, copies in ((above_y, y_up), (below_y, y_down), (above_z, z_up), (below_z, z_down)):
        each(cond, copies, lambda c: c.wait_send())


def put(cells, den, mom, en, sums, out_d, out_m, out_e, totals, mean, sem):
    half = den.shape[0] // 2
    pairs = ((den, out_d), (en, out_e), (mom, out_m))
    for i, (src, dst) in enumerate(pairs):
        for h in (pl.ds(0, half), pl.ds(half, den.shape[0] - half)):
            for at in ((h,),) if i < 2 else tuple((c, h) for c in range(3)):
                pltpu.make_async_copy(src.at[at], dst.at[at], sem.at[i]).start()
    mean[0] = jnp.sum(sums[0:1]) / cells
    mean[1] = jnp.sum(sums[1:2]) / cells
    last = pltpu.make_async_copy(mean, totals, sem.at[3])
    last.start()
    for i, (src, dst) in enumerate(pairs):
        pltpu.make_async_copy(src, dst, sem.at[i]).wait()
    last.wait()


def shards(density, momentum, energy, displacement, flags):
    sizes = {a: lax.axis_size(a) for a in AXES}
    nx, ny, nz = density.shape
    tall = ny + 2 * SUB
    per = nz // 4
    parts = -(-6 * nx // per)
    f32, i32 = jnp.float32, jnp.int32
    dma = pltpu.SemaphoreType.DMA
    any_ = pl.BlockSpec(memory_space=pl.ANY)
    hbm = pl.BlockSpec(memory_space=pltpu.HBM)
    vmem = pl.BlockSpec(memory_space=pltpu.VMEM)
    devices = 1
    for a in AXES:
        devices *= sizes[a]
    cells = float(nx * ny * nz * devices)
    outputs = tuple(jax.ShapeDtypeStruct(v.shape, f32) for v in (density, momentum, energy))
    results = pl.pallas_call(
        functools.partial(kernel, sizes),
        out_shape=outputs + (jax.ShapeDtypeStruct((2, nz), f32),),
        in_specs=[hbm] * 5,
        out_specs=(vmem, vmem, vmem, vmem),
        scratch_shapes=[
            pltpu.SMEM((6,), i32),
            pltpu.VMEM((5, nx, tall, nz), f32),
            pltpu.VMEM((2, nx, ny, nz), i32),
            pltpu.VMEM((nx, tall, nz), i32),
            pltpu.VMEM((2, 5, 2, ny, nz), f32),
            pltpu.VMEM((3, 2, ny, nz), f32),
            pltpu.VMEM((ny, nz), i32),
        ]
        + [pltpu.VMEM((parts, ny, nz), f32) for _ in range(5)]
        + [pltpu.VMEM((2, nz), f32), pltpu.VMEM((sizes["gx"] * sizes["gz"], 2, nz), f32)]
        + [pltpu.VMEM((sizes["gy"], 2, nz), f32), pltpu.VMEM((2, nz), f32)]
        + [dma((9 + (sizes["gz"] > 2),)), dma((14 + (sizes["gz"] > 2),)), pltpu.SemaphoreType.REGULAR((4,)), dma((2,)), dma((2,))],
        compiler_params=pltpu.CompilerParams(
            collective_id=0, has_side_effects=True, vmem_limit_bytes=12 << 20
        ),
    )(
        *(
            pltpu.with_memory_space_constraint(v, pltpu.HBM)
            for v in (flags, density, momentum, energy, displacement)
        )
    )
    return pl.pallas_call(
        functools.partial(put, cells),
        out_shape=outputs + (jax.ShapeDtypeStruct((2,), f32),),
        in_specs=[any_, any_, any_, vmem],
        out_specs=(hbm, hbm, hbm, hbm),
        scratch_shapes=[pltpu.SMEM((2,), f32), dma((4,))],
        compiler_params=pltpu.CompilerParams(vmem_limit_bytes=2 << 20),
    )(*results)


def solution(mesh):
    return jax.shard_map(
        shards,
        mesh=mesh,
        in_specs=(
            P("gx", "gy", "gz"),
            P(None, "gx", "gy", "gz"),
            P("gx", "gy", "gz"),
            P(None, "gx", "gy", "gz"),
            P(),
        ),
        out_specs=(P("gx", "gy", "gz"), P(None, "gx", "gy", "gz"), P("gx", "gy", "gz"), P()),
        check_vma=False,
    )
```

```python
import functools

import jax
import jax.numpy as jnp
from jax import lax
from jax.experimental import pallas as pl
from jax.experimental.pallas import tpu as pltpu
from jax.sharding import PartitionSpec as P

AXES = ("gx", "gy", "gz")
SUB = 8


def minmod(p, r):
    return jnp.maximum(jnp.minimum(r, 0.0), jnp.minimum(p, jnp.maximum(r, 0.0)))


def gain(v):
    size = jnp.abs(v)
    return 0.5 * size * (1.0 - size)


def flux(v, g, q_low, q_high, s_low, s_high):
    up = v > 0
    return v * jnp.where(up, q_low, q_high) + g * jnp.where(up, s_low, s_high)


def rim_fluxes(line_q, vs):
    ds = [line_q[i + 1] - line_q[i] for i in range(4)]
    ss = [minmod(ds[i + 1], ds[i]) for i in range(3)]
    return [
        flux(vs[i], gain(vs[i]), line_q[i + 1], line_q[i + 2], ss[i], ss[i + 1]) for i in range(2)
    ]


def kernel(
    sizes, flags_in, den, mom, en, disp, out_d, out_m, out_e, sums, ghost, cells,
    flags, q, dxz, dy, xh, hop, xv, edge, zlo, zhi, cq, cs, part, slots, line, done,
    send_sem, recv_sem, in_sem, sum_send, sum_recv,
):
    nx, ny, nz = den.shape
    pos = {a: lax.axis_index(a) for a in AXES}
    last = {a: sizes[a] - 1 for a in AXES}
    top = ny + SUB
    per = nz // 4
    parts = edge.shape[0]
    scale = 1.0 / 256.0
    xlo, xhi = xh.at[0], xh.at[1]
    dx, dz = dxz.at[0], dxz.at[1]
    own = slice(SUB, top)
    mesh_ids = pl.DeviceIdType.MESH

    def load(src, dst, k):
        return pltpu.make_async_copy(src, dst, send_sem.at[k])

    spans = (slice(0, 2), slice(nx - 2, nx), slice(2, nx - 2))
    loads = []
    for x, k, first in zip(spans, (1, 2, 2), (0, 2, 2)):
        loads += [
            load(den.at[x], q.at[0, x, own], first),
            load(en.at[x], q.at[4, x, own], k),
            load(mom.at[:, x], q.at[1:4, x, own], k),
        ]
    loads += [
        load(flags_in, flags, 3),
        load(disp.at[0], dx, 4),
        load(disp.at[2], dz, 4),
        load(disp.at[1], dy.at[:, own], 5),
    ]
    for c in loads:
        c.start()

    def loaded(ref, k):
        load(ref, ref, k).wait()

    me = pos["gx"]
    par = lax.rem(me, 2)
    odd = par == 1
    end = last["gx"]
    sx, sy, sz = (sizes[a] for a in AXES)
    group = sx * sz
    leader = (me == 0) & (pos["gz"] == last["gz"])
    members = [{"gx": i // sz, "gz": last["gz"] - i % sz} for i in range(1, group)]

    def tell(sem, cond, **target):
        @pl.when(cond)
        def _():
            pl.semaphore_signal(sem, inc=1, device_id=target, device_id_type=mesh_ids)

    even = ~odd
    above = {a: pos[a] < last[a] for a in AXES}
    above_x, above_y, above_z = (above[a] for a in AXES)
    below_x, below_y, below_z = me > 0, pos["gy"] > 0, pos["gz"] > 0
    over = me + 2 <= end
    inner = even & below_x
    barrier = pltpu.get_barrier_semaphore()
    greetings = [
        (even & above_x, odd, {"gx": me + 1}),
        (over, me >= 2, {"gx": me + 2}),
        (above_y, below_y, {"gy": pos["gy"] + 1}),
        (above_z, below_z, {"gz": pos["gz"] + 1}),
    ]
    heard = jnp.where(leader, pos["gy"], 1)
    for speaks, hears, target in greetings:
        tell(barrier, speaks, **target)
        heard += jnp.where(hears, 1, 0)

    @pl.when(leader)
    def _():
        for target in members:
            tell(barrier, True, **target)
        for o in range(1, sy):
            tell(barrier, pos["gy"] + o <= last["gy"], gy=pos["gy"] + o)

    @pl.when(heard > 0)
    def _():
        pl.semaphore_wait(barrier, heard)

    tell(in_sem.at[0], odd, gx=me - 1)
    tell(in_sem.at[0], me >= 2, gx=me - 2)
    tell(in_sem.at[2], below_y, gy=pos["gy"] - 1)
    tell(in_sem.at[2], below_z, gz=pos["gz"] - 1)
    for o in range(1, sy):
        tell(in_sem.at[3], leader & (pos["gy"] >= o), gy=pos["gy"] - o)

    def is_in(k, cond, many=1):
        @pl.when(cond)
        def _():
            pl.semaphore_wait(in_sem.at[k], many)

    def copy(ks, kr, src, dst, axis, step):
        return pltpu.make_async_remote_copy(
            src_ref=src, dst_ref=dst, send_sem=send_sem.at[ks], recv_sem=recv_sem.at[kr],
            device_id={axis: pos[axis] + step}, device_id_type=mesh_ids,
        )

    hands_up, hands_down = odd & above_x, inner
    relays = (odd & (me >= 3)) | (even & over)
    beside = 1 - 2 * par
    main, hand_k = 0, 1

    groups = (slice(3, 5), slice(1, 3), 0)
    tops, bottoms = slice(nx - 2, nx), slice(0, 2)

    def dst(side, f):
        return ghost if side is xlo and f == 0 else side.at[f]

    def piece(k, i, x, side, first, step):
        f = groups[i]
        return copy(k, first + i, q.at[f, x, own], dst(side, f), "gx", step)

    def one(k, r, x, side, i, step):
        return copy(k, r, q.at[0, x, own], dst(side, 0).at[i], "gx", step)

    up = [piece(main, i, tops, xlo, 0, 1) for i in range(3)]
    down = [piece(main, i, bottoms, xhi, 3, -1) for i in range(3)]
    v_down = copy(2, 6, dx.at[0], xv, "gx", -1)
    up_across = [piece(main, 0, tops, xlo, 0, 1), one(main, 2, nx - 1, xlo, 1, 1)]
    down_across = [piece(main, 0, bottoms, xhi, 3, -1), one(main, 5, 1, xhi, 1, -1)]
    legs_up = [
        copy(main, 7, q.at[1:3, tops, own], hop.at[0:2], "gx", 2),
        copy(main, 7, q.at[0, nx - 2, own], hop.at[2, 0], "gx", 2),
    ]
    legs_down = [
        copy(main, 7, q.at[1:3, bottoms, own], hop.at[0:2], "gx", -2),
        copy(main, 7, q.at[0, 0, own], hop.at[2, 0], "gx", -2),
    ]

    def handed(side):
        return [
            copy(hand_k, 8, hop.at[0:2], side.at[1:3], "gx", beside),
            copy(hand_k, 9, hop.at[2, 0], dst(side, 0).at[0], "gx", beside),
        ]

    handed_up, handed_down = handed(xlo), handed(xhi)

    def each(cond, copies, act):
        @pl.when(cond)
        def _():
            for c in copies:
                act(c)

    def go(c):
        c.start()

    hi_rows = slice(top, top + SUB)
    y_up = [copy(3, 10, q.at[:, :, ny:top], q.at[:, :, 0:SUB], "gy", 1)]
    y_down = [
        copy(3, 11, q.at[:, :, SUB : 2 * SUB], q.at[:, :, hi_rows], "gy", -1),
        copy(4, 12, dy.at[:, SUB : 2 * SUB], dy.at[:, hi_rows], "gy", -1),
    ]
    both = sz > 2
    z_up = [copy(5, 13, edge, zlo, "gz", 1)]
    z_down = [copy(5 + both, 13 + both, edge, zhi, "gz", -1)]

    def arrive(axis, ups, downs, fill_low, fill_high):
        @pl.when(pos[axis] > 0)
        def _():
            for c in ups:
                c.wait_recv()

        @pl.when(pos[axis] < last[axis])
        def _():
            for c in downs:
                c.wait_recv()

        @pl.when(pos[axis] == 0)
        def _():
            fill_low()

        @pl.when(pos[axis] == last[axis])
        def _():
            fill_high()

    def sent(axis, ups, downs):
        @pl.when(pos[axis] < last[axis])
        def _():
            for c in ups:
                c.wait_send()

        @pl.when(pos[axis] > 0)
        def _():
            for c in downs:
                c.wait_send()

    loaded(q.at[0, bottoms, own], 0)
    each(odd, down[2:], go)
    loaded(q.at[1:5, bottoms, own], 1)
    loaded(q.at[:, 2:nx, own], 2)
    load(flags_in, flags, 3).wait()
    loaded(dxz, 4)
    loaded(dy.at[:, own], 5)

    flag = [flags[i].astype(jnp.float32) for i in range(6)]

    def low_mult(a):
        return jnp.where(pos[AXES[a]] == 0, flag[2 * a], 1.0)

    def high_mult(a):
        return jnp.where(pos[AXES[a]] == last[AXES[a]], flag[2 * a + 1], 1.0)

    def outer_low(a):
        return jnp.where(pos[AXES[a]] == 0, flag[2 * a], 0.0)

    def outer_high(a):
        return jnp.where(pos[AXES[a]] == last[AXES[a]], flag[2 * a + 1], 0.0)

    lane = lax.broadcasted_iota(jnp.int32, (ny, nz), 1)
    row = lax.broadcasted_iota(jnp.int32, (ny, nz), 0)
    wz = jnp.where(lane == 0, outer_low(2), 0.0) - jnp.where(lane == nz - 1, outer_high(2), 0.0)
    wy = jnp.where(row == 0, outer_low(1), 0.0) - jnp.where(row == ny - 1, outer_high(1), 0.0)
    wx_low, wx_high = outer_low(0), outer_high(0)

    def total(x, carry):
        a, b = carry
        wx = jnp.where(x == 0, wx_low, 0.0) - jnp.where(x == nx - 1, wx_high, 0.0)
        w = 1.0 + scale * (
            wz * dz[x].astype(jnp.float32)
            + wy * dy[x, own].astype(jnp.float32)
            + wx * dx[x].astype(jnp.float32)
        )
        return (
            a + jnp.sum((q[0, x, own] * w).reshape(ny // SUB, SUB, nz), 0),
            b + jnp.sum((q[4, x, own] * w).reshape(ny // SUB, SUB, nz), 0),
        )

    zero = jnp.zeros((SUB, nz), jnp.float32)
    mass, power = lax.fori_loop(0, nx, total, (zero, zero))
    part[0:1] = jnp.sum(mass, 0, keepdims=True)
    part[1:2] = jnp.sum(power, 0, keepdims=True)

    def message(src, dst, ks, kr, target):
        return pltpu.make_async_remote_copy(
            src_ref=src, dst_ref=dst, send_sem=sum_send.at[ks], recv_sem=sum_recv.at[kr],
            device_id=target, device_id_type=mesh_ids,
        )

    home = {"gx": 0, "gz": last["gz"]}
    inward = message(part, slots.at[me * sz + last["gz"] - pos["gz"]], 0, 0, home)
    gathered = message(slots.at[1:group], slots.at[1:group], 1, 0, members[-1])
    across = [
        message(line.at[0], line.at[sy - o], 0, 1, {"gy": lax.rem(pos["gy"] + o, sy)})
        for o in range(1, sy)
    ]
    crossed = message(line.at[1:sy], line.at[1:sy], 0, 1, {"gy": lax.rem(pos["gy"] + 1, sy)})
    outward = [message(done, done, 1, 0, target) for target in members]

    each(~leader, [inward], go)

    each(hands_down, legs_down, go)
    each(below_y, y_down, go)

    def x_sends():
        each(odd, [v_down] + down[:2], go)
        waits = jnp.where(over, 1, 0) + jnp.where(above_x, 1, 0)
        is_in(0, waits > 0, waits)

        @pl.when(even & over)
        def _():
            tell(in_sem.at[0], True, gx=me + 1)
            tell(in_sem.at[1], True, gx=me + 2)

        each(even & above_x, up[:1], go)
        each(odd & over, legs_up, go)
        each(hands_up, up_across, go)
        is_in(1, hands_down)
        each(hands_down, [v_down] + down_across, go)
        each(even & above_x, up[1:], go)

    pl.when(below_x | below_y)(x_sends)

    def pack(x, carry):
        new = list(carry)
        for f in range(6):
            p = f * nx + x
            k = f * nx // per
            at = 4 * lax.rem(p, per)
            plane = q[f, x, own] if f < 5 else dz[x].astype(jnp.float32)
            moved = pltpu.roll(plane, at, 1)
            mine = lax.rem(lane + 2 - at + nz, nz) < 4
            new[k] = jnp.where(mine, moved, new[k])
        return tuple(new)

    packed = lax.fori_loop(0, nx, pack, tuple(jnp.zeros((ny, nz), jnp.float32) for _ in range(parts)))
    for k in range(parts):
        edge[k] = packed[k]
    each(below_z, z_down, go)
    beyond = jnp.where(above_y, 1, 0) + jnp.where(above_z, 1, 0)
    is_in(2, beyond > 0, beyond)
    each(above_z, z_up, go)
    pl.when(~below_x & ~below_y)(x_sends)
    each(above_y, y_up, go)

    outs = (
        lambda x: out_d.at[x], lambda x: out_m.at[0, x], lambda x: out_m.at[1, x],
        lambda x: out_m.at[2, x], lambda x: out_e.at[x],
    )

    def core(r, _):
        at = pl.ds(pl.multiple_of(r * SUB, SUB), SUB)
        inner = pl.ds(pl.multiple_of(r * SUB + SUB, SUB), SUB)
        vs = [dx[c, at].astype(jnp.float32) * scale for c in range(2, nx - 1)]
        gs = [gain(v) for v in vs]
        for f in range(5):
            line_q = [q[f, c, inner] for c in range(nx)]
            ds = [line_q[i + 1] - line_q[i] for i in range(nx - 1)]
            ss = [minmod(ds[i + 1], ds[i]) for i in range(nx - 2)]
            fl = [
                flux(vs[i], gs[i], line_q[i + 1], line_q[i + 2], ss[i], ss[i + 1])
                for i in range(nx - 3)
            ]
            for c in range(nx):
                new = line_q[c]
                if 2 <= c < nx - 1:
                    new = new + fl[c - 2]
                if 1 <= c < nx - 2:
                    new = new - fl[c - 1]
                outs[f](c)[at] = new
        return 0

    lax.fori_loop(0, ny // SUB, core, 0)

    def z_low():
        e = edge[...]
        zlo[...] = jnp.where(lane3 & 3 == 3, pltpu.roll(e, nz - 1, 2), pltpu.roll(e, nz - 2, 2))

    def z_high():
        e = edge[...]
        zhi[...] = jnp.where(lane3 & 3 == 0, pltpu.roll(e, 1, 2), pltpu.roll(e, 2, 2))

    lane3 = lax.broadcasted_iota(jnp.int32, (parts, ny, nz), 2)
    arrive("gz", z_up, z_down, z_low, z_high)
    low = lane & 3 == 0
    for k in range(parts):
        e, l, h = edge[k], zlo[k], zhi[k]
        r1, r2 = pltpu.roll(l, 1, 1), pltpu.roll(l, 2, 1)
        l1, l2 = pltpu.roll(h, nz - 1, 1), pltpu.roll(h, nz - 2, 1)
        cq[k] = jnp.where(low, r1, l1)
        cs[k] = jnp.where(low, minmod(e - r1, r1 - r2), minmod(l2 - l1, l1 - e))

    first, final = lane == 0, lane == nz - 1
    z_lo_mult = jnp.where(first, low_mult(2), 1.0) * scale
    z_hi_mult = high_mult(2) * scale
    def along_z(x, _):
        v = dz[x].astype(jnp.float32) * z_lo_mult
        g = gain(v)

        def ghosts(ref, f):
            back = lax.rem(nz - 4 * lax.rem(f * nx + x, per), nz)
            return pltpu.roll(ref[f * nx // per], back, 1)

        vh = ghosts(cq, 5) * z_hi_mult
        gh = gain(vh)
        for f in range(5):
            plane = q[f, x, SUB:top]
            gq, gs = ghosts(cq, f), ghosts(cs, f)
            qm = jnp.where(first, gq, pltpu.roll(plane, 1, 1))
            d = plane - qm
            s = minmod(jnp.where(final, gq - plane, pltpu.roll(d, nz - 1, 1)), d)
            sm = jnp.where(first, gs, pltpu.roll(s, 1, 1))
            fl = flux(v, g, qm, plane, sm, s)
            fh = jnp.where(final, flux(vh, gh, plane, gq, s, gs), pltpu.roll(fl, nz - 1, 1))
            outs[f](x)[...] += fl - fh
        return 0

    early = nx * 5 // 8
    lax.fori_loop(0, early, along_z, 0)

    def gather():
        gathered.wait_recv()
        line[0] = part[...] + jnp.sum(slots[1:group], 0)
        is_in(3, above_y, last["gy"] - pos["gy"])
        for c in across:
            c.start()

    pl.when(leader & below_y)(gather)
    lax.fori_loop(early, nx, along_z, 0)

    @pl.when(relays)
    def _():
        copy(hand_k, 7, q.at[:, 0, own], q.at[:, 0, own], "gx", beside).wait_recv()

    each(relays & odd, handed_up, go)
    each(relays & even, handed_down, go)

    def y_low():
        q[:, :, 0:SUB] = jnp.broadcast_to(q[:, :, SUB : SUB + 1], (5, nx, SUB, nz))

    def y_high():
        q[:, :, hi_rows] = jnp.broadcast_to(q[:, :, top - 1 : top], (5, nx, SUB, nz))
        dy[:, hi_rows] = jnp.broadcast_to(dy[:, top - 1 : top], (nx, SUB, nz))

    arrive("gy", y_up, y_down, y_low, y_high)
    pl.when(leader & ~below_y)(gather)
    tall = ny + 2 * SUB
    rows = lax.broadcasted_iota(jnp.int32, (tall, nz), 0)
    inside = (rows >= SUB) & (rows <= top)
    y_mult = jnp.where(
        rows == SUB, low_mult(1) * scale, jnp.where(rows == top, high_mult(1) * scale, scale)
    )

    def along_y(x, _):
        v = jnp.where(inside, dy[x].astype(jnp.float32), 0.0) * y_mult
        g = gain(v)
        for f in range(5):
            plane = q[f, x]
            qm = pltpu.roll(plane, 1, 0)
            d = plane - qm
            s = minmod(pltpu.roll(d, tall - 1, 0), d)
            fl = flux(v, g, qm, plane, pltpu.roll(s, 1, 0), s)
            ch = fl - pltpu.roll(fl, tall - 1, 0)
            outs[f](x)[...] += ch[SUB:top]
        return 0

    lax.fori_loop(0, nx, along_y, 0)

    @pl.when(me == 0)
    def _():
        xlo[...] = jnp.broadcast_to(q[:, 0:1, own], (5, 2, ny, nz))
        ghost[...] = jnp.broadcast_to(q[0, 0:1, own], (2, ny, nz))

    @pl.when(me == end)
    def _():
        xhi[...] = jnp.broadcast_to(q[:, nx - 1 : nx, own], (5, 2, ny, nz))
        xv[...] = dx[nx - 1]

    each(above_x, [v_down], lambda c: c.wait_recv())
    x_lo_mult, x_hi_mult = low_mult(0) * scale, high_mult(0) * scale

    tile = 4 * SUB if ny % (4 * SUB) == 0 else SUB

    cells[0:3] = q[0, 0:3, own]
    cells[3] = dx[0].astype(jnp.float32) * x_lo_mult
    cells[4] = dx[1].astype(jnp.float32) * scale

    def rim(high, f):
        def rows(r, _):
            at = pl.ds(pl.multiple_of(r * tile, SUB), tile)
            inner = pl.ds(pl.multiple_of(r * tile + SUB, SUB), tile)
            if high:
                line_q = [q[f, c, inner] for c in range(nx - 3, nx)] + [xhi[f, i, at] for i in range(2)]
                vs = (dx[nx - 1, at].astype(jnp.float32) * scale, xv[at].astype(jnp.float32) * x_hi_mult)
            else:
                line_q = [xlo[f, i, at] for i in range(2)] + [q[f, c, inner] for c in range(3)]
                vs = (dx[0, at].astype(jnp.float32) * x_lo_mult, dx[1, at].astype(jnp.float32) * scale)
            fl = rim_fluxes(line_q, vs)
            if high:
                changes = ((nx - 2, -fl[0]), (nx - 1, fl[0] - fl[1]))
            else:
                changes = ((0, fl[0] - fl[1]), (1, fl[1]))
            for c, change in changes:
                ref = outs[f](c)
                ref[at] += change
            return 0

        lax.fori_loop(0, ny // tile, rows, 0)

    def come(cond, copies):
        each(cond, copies, lambda c: c.wait_recv())

    def rims(high, i):
        for f in ((3, 4), (1, 2), (0,))[i]:
            rim(high, f)

    def lower(i):
        come(odd, [up[i]])
        come(hands_down, ([up_across[0]], handed_up[:1], [up_across[1], handed_up[1]])[i])
        if i < 2:
            rims(False, i)

    def upper(i):
        come(even & above_x, [down[i]])
        come(hands_up, ([down_across[0]], handed_down[:1], [down_across[1], handed_down[1]])[i])
        rims(True, i)

    def finish():
        crossed.wait_recv()
        done[...] = jnp.sum(line[...], 0)
        for c in outward:
            c.start()

    pl.when(leader)(finish)

    def sides(turn, _):
        @pl.when((turn == 1) == hands_up)
        def _():
            for i in (2, 0, 1):
                upper(i)

        @pl.when(turn == 0)
        def _():
            for i in range(3):
                lower(i)

        return 0

    lax.fori_loop(0, 2, sides, 0)

    @pl.when(~leader)
    def _():
        outward[0].wait_recv()
        inward.wait_send()

    sums[...] = done[...]

    @pl.when(leader)
    def _():
        crossed.wait_send()
        gathered.wait_send()

    def sent(k, cond, ref):
        @pl.when(cond)
        def _():
            copy(k, 0, ref, ref, "gx", beside).wait_send()

    pair = hands_up | hands_down
    sent(main, pair, xh)
    sent(main, ~pair, xlo)
    sent(hand_k, relays, q.at[:, 0, own])
    sent(2, below_x, xv)
    sent(3, above_y & below_y, q.at[:, :, 0 : 2 * SUB])
    sent(3, above_y ^ below_y, q.at[:, :, 0:SUB])
    sent(4, below_y, dy.at[:, 0:SUB])
    sent(5, above_z, edge)
    sent(5 + both, below_z, edge)


def put(count, den, mom, en, sums, ghost, cells, out_d, out_m, out_e, totals, edge, mean, sem):
    nx = den.shape[0]
    half = nx // 2
    moves = [
        (den.at[2:nx], out_d.at[2:nx], 0),
        (en.at[0:half], out_e.at[0:half], 1),
        (en.at[half:nx], out_e.at[half:nx], 1),
    ]
    for c in range(3):
        moves += [(mom.at[c, h], out_m.at[c, h], 2) for h in (pl.ds(0, half), pl.ds(half, nx - half))]
    for src, dst, k in moves:
        pltpu.make_async_copy(src, dst, sem.at[k]).start()

    line_q = [ghost[0], ghost[1]] + [cells[c] for c in range(3)]
    fl = rim_fluxes(line_q, (cells[3], cells[4]))
    edge[0] = den[0] + (fl[0] - fl[1])
    edge[1] = den[1] + fl[1]
    mean[0] = jnp.sum(sums[0:1]) / count
    mean[1] = jnp.sum(sums[1:2]) / count
    rest = [
        pltpu.make_async_copy(mean, totals, sem.at[3]),
        pltpu.make_async_copy(edge, out_d.at[0:2], sem.at[4]),
    ]
    for c in rest:
        c.start()
    pltpu.make_async_copy(den.at[2:nx], out_d.at[2:nx], sem.at[0]).wait()
    pltpu.make_async_copy(en, out_e, sem.at[1]).wait()
    pltpu.make_async_copy(mom, out_m, sem.at[2]).wait()
    for c in rest:
        c.wait()


def shards(density, momentum, energy, displacement, flags):
    sizes = {a: lax.axis_size(a) for a in AXES}
    nx, ny, nz = density.shape
    tall = ny + 2 * SUB
    per = nz // 4
    parts = -(-6 * nx // per)
    f32, i32 = jnp.float32, jnp.int32
    dma = pltpu.SemaphoreType.DMA
    any_ = pl.BlockSpec(memory_space=pl.ANY)
    hbm = pl.BlockSpec(memory_space=pltpu.HBM)
    vmem = pl.BlockSpec(memory_space=pltpu.VMEM)
    devices = 1
    for a in AXES:
        devices *= sizes[a]
    count = float(nx * ny * nz * devices)
    outputs = tuple(jax.ShapeDtypeStruct(v.shape, f32) for v in (density, momentum, energy))
    results = pl.pallas_call(
        functools.partial(kernel, sizes),
        out_shape=outputs + tuple(
            jax.ShapeDtypeStruct(v, f32) for v in ((2, nz), (2, ny, nz), (5, ny, nz))
        ),
        in_specs=[hbm] * 5,
        out_specs=(vmem,) * 6,
        scratch_shapes=[
            pltpu.SMEM((6,), i32),
            pltpu.VMEM((5, nx, tall, nz), f32),
            pltpu.VMEM((2, nx, ny, nz), i32),
            pltpu.VMEM((nx, tall, nz), i32),
            pltpu.VMEM((2, 5, 2, ny, nz), f32),
            pltpu.VMEM((3, 2, ny, nz), f32),
            pltpu.VMEM((ny, nz), i32),
        ]
        + [pltpu.VMEM((parts, ny, nz), f32) for _ in range(5)]
        + [pltpu.VMEM((2, nz), f32), pltpu.VMEM((sizes["gx"] * sizes["gz"], 2, nz), f32)]
        + [pltpu.VMEM((sizes["gy"], 2, nz), f32), pltpu.VMEM((2, nz), f32)]
        + [dma((6 + (sizes["gz"] > 2),)), dma((14 + (sizes["gz"] > 2),)), pltpu.SemaphoreType.REGULAR((4,)), dma((2,)), dma((2,))],
        compiler_params=pltpu.CompilerParams(
            collective_id=0, has_side_effects=True, vmem_limit_bytes=12 << 20
        ),
    )(
        *(
            pltpu.with_memory_space_constraint(v, pltpu.HBM)
            for v in (flags, density, momentum, energy, displacement)
        )
    )
    return pl.pallas_call(
        functools.partial(put, count),
        out_shape=outputs + (jax.ShapeDtypeStruct((2,), f32),),
        in_specs=[vmem, any_, any_, vmem, vmem, vmem],
        out_specs=(hbm, hbm, hbm, hbm),
        scratch_shapes=[pltpu.VMEM((2, ny, nz), f32), pltpu.SMEM((2,), f32), dma((5,))],
        compiler_params=pltpu.CompilerParams(vmem_limit_bytes=2 << 20),
    )(*results)


def solution(mesh):
    return jax.shard_map(
        shards,
        mesh=mesh,
        in_specs=(
            P("gx", "gy", "gz"),
            P(None, "gx", "gy", "gz"),
            P("gx", "gy", "gz"),
            P(None, "gx", "gy", "gz"),
            P(),
        ),
        out_specs=(P("gx", "gy", "gz"), P(None, "gx", "gy", "gz"), P("gx", "gy", "gz"), P()),
        check_vma=False,
    )
```

```python
import functools

import jax
import jax.numpy as jnp
from jax import lax
from jax.experimental import pallas as pl
from jax.experimental.pallas import tpu as pltpu
from jax.sharding import PartitionSpec as P

AXES = ("gx", "gy", "gz")
SUB = 8


def minmod(p, r):
    return jnp.maximum(jnp.minimum(r, 0.0), jnp.minimum(p, jnp.maximum(r, 0.0)))


def gain(v):
    size = jnp.abs(v)
    return 0.5 * size * (1.0 - size)


def flux(v, g, q_low, q_high, s_low, s_high):
    up = v > 0
    return v * jnp.where(up, q_low, q_high) + g * jnp.where(up, s_low, s_high)


def rim_fluxes(line_q, vs):
    ds = [line_q[i + 1] - line_q[i] for i in range(4)]
    ss = [minmod(ds[i + 1], ds[i]) for i in range(3)]
    return [
        flux(vs[i], gain(vs[i]), line_q[i + 1], line_q[i + 2], ss[i], ss[i + 1]) for i in range(2)
    ]


def kernel(
    sizes, flags_in, den, mom, en, disp, out_d, out_m, out_e, sums, ghost, cells,
    flags, q, dxz, dy, xh, hop, xv, edge, zlo, zhi, cq, cs, part, slots, line, done,
    send_sem, recv_sem, in_sem, sum_send, sum_recv,
):
    nx, ny, nz = den.shape
    pos = {a: lax.axis_index(a) for a in AXES}
    last = {a: sizes[a] - 1 for a in AXES}
    top = ny + SUB
    per = nz // 4
    parts = edge.shape[0]
    scale = 1.0 / 256.0
    xlo, xhi = xh.at[0], xh.at[1]
    dx, dz = dxz.at[0], dxz.at[1]
    own = slice(SUB, top)
    mesh_ids = pl.DeviceIdType.MESH

    def load(src, dst, k):
        return pltpu.make_async_copy(src, dst, send_sem.at[k])

    spans = (slice(0, 2), slice(nx - 2, nx), slice(2, nx - 2))
    loads = []
    for x, k, first in zip(spans, (1, 2, 2), (0, 2, 2)):
        loads += [
            load(den.at[x], q.at[0, x, own], first),
            load(en.at[x], q.at[4, x, own], k),
            load(mom.at[:, x], q.at[1:4, x, own], k),
        ]
    loads += [
        load(flags_in, flags, 3),
        load(disp.at[0], dx, 4),
        load(disp.at[2], dz, 4),
        load(disp.at[1], dy.at[:, own], 5),
    ]
    for c in loads:
        c.start()

    def loaded(ref, k):
        load(ref, ref, k).wait()

    me = pos["gx"]
    par = lax.rem(me, 2)
    odd = par == 1
    end = last["gx"]
    sx, sy, sz = (sizes[a] for a in AXES)
    group = sx * sz
    leader = (me == 0) & (pos["gz"] == last["gz"])
    members = [{"gx": i // sz, "gz": last["gz"] - i % sz} for i in range(1, group)]

    def tell(sem, cond, **target):
        @pl.when(cond)
        def _():
            pl.semaphore_signal(sem, inc=1, device_id=target, device_id_type=mesh_ids)

    even = ~odd
    above = {a: pos[a] < last[a] for a in AXES}
    above_x, above_y, above_z = (above[a] for a in AXES)
    below_x, below_y, below_z = me > 0, pos["gy"] > 0, pos["gz"] > 0
    over = me + 2 <= end
    inner = even & below_x
    barrier = pltpu.get_barrier_semaphore()
    greetings = [
        (even & above_x, odd, {"gx": me + 1}),
        (over, me >= 2, {"gx": me + 2}),
        (above_y, below_y, {"gy": pos["gy"] + 1}),
        (above_z, below_z, {"gz": pos["gz"] + 1}),
    ]
    heard = jnp.where(leader, pos["gy"], 1)
    for speaks, hears, target in greetings:
        tell(barrier, speaks, **target)
        heard += jnp.where(hears, 1, 0)

    @pl.when(leader)
    def _():
        for target in members:
            tell(barrier, True, **target)
        for o in range(1, sy):
            tell(barrier, pos["gy"] + o <= last["gy"], gy=pos["gy"] + o)

    @pl.when(heard > 0)
    def _():
        pl.semaphore_wait(barrier, heard)

    tell(in_sem.at[0], odd, gx=me - 1)
    tell(in_sem.at[0], me >= 2, gx=me - 2)
    tell(in_sem.at[2], below_y, gy=pos["gy"] - 1)
    tell(in_sem.at[2], below_z, gz=pos["gz"] - 1)
    for o in range(1, sy):
        tell(in_sem.at[3], leader & (pos["gy"] >= o), gy=pos["gy"] - o)

    def is_in(k, cond, many=1):
        @pl.when(cond)
        def _():
            pl.semaphore_wait(in_sem.at[k], many)

    def copy(ks, kr, src, dst, axis, step):
        return pltpu.make_async_remote_copy(
            src_ref=src, dst_ref=dst, send_sem=send_sem.at[ks], recv_sem=recv_sem.at[kr],
            device_id={axis: pos[axis] + step}, device_id_type=mesh_ids,
        )

    hands_up, hands_down = odd & above_x, inner
    relays = (odd & (me >= 3)) | (even & over)
    beside = 1 - 2 * par
    main, hand_k = 0, 1

    groups = (slice(3, 5), slice(1, 3), 0)
    tops, bottoms = slice(nx - 2, nx), slice(0, 2)

    def dst(side, f):
        return ghost if side is xlo and f == 0 else side.at[f]

    def piece(k, i, x, side, first, step):
        f = groups[i]
        return copy(k, first + i, q.at[f, x, own], dst(side, f), "gx", step)

    def one(k, r, x, side, i, step):
        return copy(k, r, q.at[0, x, own], dst(side, 0).at[i], "gx", step)

    up = [piece(main, i, tops, xlo, 0, 1) for i in range(3)]
    down = [piece(main, i, bottoms, xhi, 3, -1) for i in range(3)]
    v_down = copy(2, 6, dx.at[0], xv, "gx", -1)
    up_across = [piece(main, 0, tops, xlo, 0, 1), one(main, 2, nx - 1, xlo, 1, 1)]
    down_across = [piece(main, 0, bottoms, xhi, 3, -1), one(main, 5, 1, xhi, 1, -1)]
    legs_up = [
        copy(main, 7, q.at[1:3, tops, own], hop.at[0:2], "gx", 2),
        copy(main, 7, q.at[0, nx - 2, own], hop.at[2, 0], "gx", 2),
    ]
    legs_down = [
        copy(main, 7, q.at[1:3, bottoms, own], hop.at[0:2], "gx", -2),
        copy(main, 7, q.at[0, 0, own], hop.at[2, 0], "gx", -2),
    ]

    def handed(side):
        return [
            copy(hand_k, 8, hop.at[0:2], side.at[1:3], "gx", beside),
            copy(hand_k, 9, hop.at[2, 0], dst(side, 0).at[0], "gx", beside),
        ]

    handed_up, handed_down = handed(xlo), handed(xhi)

    def each(cond, copies, act):
        @pl.when(cond)
        def _():
            for c in copies:
                act(c)

    def go(c):
        c.start()

    hi_rows = slice(top, top + SUB)
    y_up = [copy(3, 10, q.at[:, :, ny:top], q.at[:, :, 0:SUB], "gy", 1)]
    y_down = [
        copy(3, 11, q.at[:, :, SUB : 2 * SUB], q.at[:, :, hi_rows], "gy", -1),
        copy(4, 12, dy.at[:, SUB : 2 * SUB], dy.at[:, hi_rows], "gy", -1),
    ]
    both = sz > 2
    z_up = [copy(5, 13, edge, zlo, "gz", 1)]
    z_down = [copy(5 + both, 13 + both, edge, zhi, "gz", -1)]

    def arrive(axis, ups, downs, fill_low, fill_high):
        @pl.when(pos[axis] > 0)
        def _():
            for c in ups:
                c.wait_recv()

        @pl.when(pos[axis] < last[axis])
        def _():
            for c in downs:
                c.wait_recv()

        @pl.when(pos[axis] == 0)
        def _():
            fill_low()

        @pl.when(pos[axis] == last[axis])
        def _():
            fill_high()

    def sent(axis, ups, downs):
        @pl.when(pos[axis] < last[axis])
        def _():
            for c in ups:
                c.wait_send()

        @pl.when(pos[axis] > 0)
        def _():
            for c in downs:
                c.wait_send()

    loaded(q.at[0, bottoms, own], 0)
    each(odd, down[2:], go)
    loaded(q.at[1:5, bottoms, own], 1)
    loaded(q.at[:, 2:nx, own], 2)
    load(flags_in, flags, 3).wait()
    loaded(dxz, 4)
    loaded(dy.at[:, own], 5)

    flag = [flags[i].astype(jnp.float32) for i in range(6)]

    def low_mult(a):
        return jnp.where(pos[AXES[a]] == 0, flag[2 * a], 1.0)

    def high_mult(a):
        return jnp.where(pos[AXES[a]] == last[AXES[a]], flag[2 * a + 1], 1.0)

    def outer_low(a):
        return jnp.where(pos[AXES[a]] == 0, flag[2 * a], 0.0)

    def outer_high(a):
        return jnp.where(pos[AXES[a]] == last[AXES[a]], flag[2 * a + 1], 0.0)

    lane = lax.broadcasted_iota(jnp.int32, (ny, nz), 1)
    row = lax.broadcasted_iota(jnp.int32, (ny, nz), 0)
    wz = jnp.where(lane == 0, outer_low(2), 0.0) - jnp.where(lane == nz - 1, outer_high(2), 0.0)
    wy = jnp.where(row == 0, outer_low(1), 0.0) - jnp.where(row == ny - 1, outer_high(1), 0.0)
    wx_low, wx_high = outer_low(0), outer_high(0)

    def total(x, carry):
        a, b = carry
        wx = jnp.where(x == 0, wx_low, 0.0) - jnp.where(x == nx - 1, wx_high, 0.0)
        w = 1.0 + scale * (
            wz * dz[x].astype(jnp.float32)
            + wy * dy[x, own].astype(jnp.float32)
            + wx * dx[x].astype(jnp.float32)
        )
        return (
            a + jnp.sum((q[0, x, own] * w).reshape(ny // SUB, SUB, nz), 0),
            b + jnp.sum((q[4, x, own] * w).reshape(ny // SUB, SUB, nz), 0),
        )

    zero = jnp.zeros((SUB, nz), jnp.float32)
    mass, power = lax.fori_loop(0, nx, total, (zero, zero))
    part[0:1] = jnp.sum(mass, 0, keepdims=True)
    part[1:2] = jnp.sum(power, 0, keepdims=True)

    def message(src, dst, ks, kr, target):
        return pltpu.make_async_remote_copy(
            src_ref=src, dst_ref=dst, send_sem=sum_send.at[ks], recv_sem=sum_recv.at[kr],
            device_id=target, device_id_type=mesh_ids,
        )

    home = {"gx": 0, "gz": last["gz"]}
    inward = message(part, slots.at[me * sz + last["gz"] - pos["gz"]], 0, 0, home)
    gathered = message(slots.at[1:group], slots.at[1:group], 1, 0, members[-1])
    across = [
        message(line.at[0], line.at[sy - o], 0, 1, {"gy": lax.rem(pos["gy"] + o, sy)})
        for o in range(1, sy)
    ]
    crossed = message(line.at[1:sy], line.at[1:sy], 0, 1, {"gy": lax.rem(pos["gy"] + 1, sy)})
    outward = [message(done, done, 1, 0, target) for target in members]

    each(~leader, [inward], go)

    each(hands_down, legs_down, go)
    each(below_y, y_down, go)

    def x_sends():
        each(odd, [v_down] + down[:2], go)
        waits = jnp.where(over, 1, 0) + jnp.where(above_x, 1, 0)
        is_in(0, waits > 0, waits)

        @pl.when(even & over)
        def _():
            tell(in_sem.at[0], True, gx=me + 1)
            tell(in_sem.at[1], True, gx=me + 2)

        each(even & above_x, up[:1], go)
        each(odd & over, legs_up, go)
        each(hands_up, up_across, go)
        is_in(1, hands_down)
        each(hands_down, [v_down] + down_across, go)
        each(even & above_x, up[1:], go)

    pl.when(below_x | below_y)(x_sends)

    def pack(x, carry):
        new = list(carry)
        for f in range(6):
            p = f * nx + x
            k = f * nx // per
            at = 4 * lax.rem(p, per)
            plane = q[f, x, own] if f < 5 else dz[x].astype(jnp.float32)
            moved = pltpu.roll(plane, at, 1)
            mine = lax.rem(lane + 2 - at + nz, nz) < 4
            new[k] = jnp.where(mine, moved, new[k])
        return tuple(new)

    packed = lax.fori_loop(0, nx, pack, tuple(jnp.zeros((ny, nz), jnp.float32) for _ in range(parts)))
    for k in range(parts):
        edge[k] = packed[k]
    each(below_z, z_down, go)
    beyond = jnp.where(above_y, 1, 0) + jnp.where(above_z, 1, 0)
    is_in(2, beyond > 0, beyond)
    each(above_z, z_up, go)
    pl.when(~below_x & ~below_y)(x_sends)
    each(above_y, y_up, go)

    outs = (
        lambda x: out_d.at[x], lambda x: out_m.at[0, x], lambda x: out_m.at[1, x],
        lambda x: out_m.at[2, x], lambda x: out_e.at[x],
    )

    def core(r, _):
        at = pl.ds(pl.multiple_of(r * SUB, SUB), SUB)
        inner = pl.ds(pl.multiple_of(r * SUB + SUB, SUB), SUB)
        vs = [dx[c, at].astype(jnp.float32) * scale for c in range(2, nx - 1)]
        gs = [gain(v) for v in vs]
        for f in range(5):
            line_q = [q[f, c, inner] for c in range(nx)]
            ds = [line_q[i + 1] - line_q[i] for i in range(nx - 1)]
            ss = [minmod(ds[i + 1], ds[i]) for i in range(nx - 2)]
            fl = [
                flux(vs[i], gs[i], line_q[i + 1], line_q[i + 2], ss[i], ss[i + 1])
                for i in range(nx - 3)
            ]
            for c in range(nx):
                new = line_q[c]
                if 2 <= c < nx - 1:
                    new = new + fl[c - 2]
                if 1 <= c < nx - 2:
                    new = new - fl[c - 1]
                outs[f](c)[at] = new
        return 0

    lax.fori_loop(0, ny // SUB, core, 0)

    def z_low():
        e = edge[...]
        zlo[...] = jnp.where(lane3 & 3 == 3, pltpu.roll(e, nz - 1, 2), pltpu.roll(e, nz - 2, 2))

    def z_high():
        e = edge[...]
        zhi[...] = jnp.where(lane3 & 3 == 0, pltpu.roll(e, 1, 2), pltpu.roll(e, 2, 2))

    lane3 = lax.broadcasted_iota(jnp.int32, (parts, ny, nz), 2)
    arrive("gz", z_up, z_down, z_low, z_high)
    low = lane & 3 == 0
    for k in range(parts):
        e, l, h = edge[k], zlo[k], zhi[k]
        r1, r2 = pltpu.roll(l, 1, 1), pltpu.roll(l, 2, 1)
        l1, l2 = pltpu.roll(h, nz - 1, 1), pltpu.roll(h, nz - 2, 1)
        cq[k] = jnp.where(low, r1, l1)
        cs[k] = jnp.where(low, minmod(e - r1, r1 - r2), minmod(l2 - l1, l1 - e))

    first, final = lane == 0, lane == nz - 1
    z_lo_mult = jnp.where(first, low_mult(2), 1.0) * scale
    z_hi_mult = high_mult(2) * scale
    def along_z(x, _):
        v = dz[x].astype(jnp.float32) * z_lo_mult
        g = gain(v)

        def ghosts(ref, f):
            back = lax.rem(nz - 4 * lax.rem(f * nx + x, per), nz)
            return pltpu.roll(ref[f * nx // per], back, 1)

        vh = ghosts(cq, 5) * z_hi_mult
        gh = gain(vh)
        for f in range(5):
            plane = q[f, x, SUB:top]
            gq, gs = ghosts(cq, f), ghosts(cs, f)
            qm = jnp.where(first, gq, pltpu.roll(plane, 1, 1))
            d = plane - qm
            s = minmod(jnp.where(final, gq - plane, pltpu.roll(d, nz - 1, 1)), d)
            sm = jnp.where(first, gs, pltpu.roll(s, 1, 1))
            fl = flux(v, g, qm, plane, sm, s)
            fh = jnp.where(final, flux(vh, gh, plane, gq, s, gs), pltpu.roll(fl, nz - 1, 1))
            outs[f](x)[...] += fl - fh
        return 0

    early = nx * 5 // 8
    lax.fori_loop(0, early, along_z, 0)

    def gather():
        gathered.wait_recv()
        line[0] = part[...] + jnp.sum(slots[1:group], 0)
        is_in(3, above_y, last["gy"] - pos["gy"])
        for c in across:
            c.start()

    pl.when(leader & below_y)(gather)
    lax.fori_loop(early, nx, along_z, 0)

    @pl.when(relays)
    def _():
        copy(hand_k, 7, q.at[:, 0, own], q.at[:, 0, own], "gx", beside).wait_recv()

    each(relays & odd, handed_up, go)
    each(relays & even, handed_down, go)

    def y_low():
        q[:, :, 0:SUB] = jnp.broadcast_to(q[:, :, SUB : SUB + 1], (5, nx, SUB, nz))

    def y_high():
        q[:, :, hi_rows] = jnp.broadcast_to(q[:, :, top - 1 : top], (5, nx, SUB, nz))
        dy[:, hi_rows] = jnp.broadcast_to(dy[:, top - 1 : top], (nx, SUB, nz))

    arrive("gy", y_up, y_down, y_low, y_high)
    pl.when(leader & ~below_y)(gather)
    tall = ny + 2 * SUB
    rows = lax.broadcasted_iota(jnp.int32, (tall, nz), 0)
    inside = (rows >= SUB) & (rows <= top)
    y_mult = jnp.where(
        rows == SUB, low_mult(1) * scale, jnp.where(rows == top, high_mult(1) * scale, scale)
    )

    def along_y(x, _):
        v = jnp.where(inside, dy[x].astype(jnp.float32), 0.0) * y_mult
        g = gain(v)
        for f in range(5):
            plane = q[f, x]
            qm = pltpu.roll(plane, 1, 0)
            d = plane - qm
            s = minmod(pltpu.roll(d, tall - 1, 0), d)
            fl = flux(v, g, qm, plane, pltpu.roll(s, 1, 0), s)
            ch = fl - pltpu.roll(fl, tall - 1, 0)
            outs[f](x)[...] += ch[SUB:top]
        return 0

    lax.fori_loop(0, nx, along_y, 0)

    @pl.when(me == 0)
    def _():
        xlo[...] = jnp.broadcast_to(q[:, 0:1, own], (5, 2, ny, nz))
        ghost[...] = jnp.broadcast_to(q[0, 0:1, own], (2, ny, nz))

    @pl.when(me == end)
    def _():
        xhi[...] = jnp.broadcast_to(q[:, nx - 1 : nx, own], (5, 2, ny, nz))
        xv[...] = dx[nx - 1]

    each(above_x, [v_down], lambda c: c.wait_recv())
    x_lo_mult, x_hi_mult = low_mult(0) * scale, high_mult(0) * scale

    tile = 4 * SUB if ny % (4 * SUB) == 0 else SUB

    cells[0:3] = q[0, 0:3, own]
    cells[3] = dx[0].astype(jnp.float32) * x_lo_mult
    cells[4] = dx[1].astype(jnp.float32) * scale

    def rim(high, f):
        def rows(r, _):
            at = pl.ds(pl.multiple_of(r * tile, SUB), tile)
            inner = pl.ds(pl.multiple_of(r * tile + SUB, SUB), tile)
            if high:
                line_q = [q[f, c, inner] for c in range(nx - 3, nx)] + [xhi[f, i, at] for i in range(2)]
                vs = (dx[nx - 1, at].astype(jnp.float32) * scale, xv[at].astype(jnp.float32) * x_hi_mult)
            else:
                line_q = [xlo[f, i, at] for i in range(2)] + [q[f, c, inner] for c in range(3)]
                vs = (dx[0, at].astype(jnp.float32) * x_lo_mult, dx[1, at].astype(jnp.float32) * scale)
            fl = rim_fluxes(line_q, vs)
            if high:
                changes = ((nx - 2, -fl[0]), (nx - 1, fl[0] - fl[1]))
            else:
                changes = ((0, fl[0] - fl[1]), (1, fl[1]))
            for c, change in changes:
                ref = outs[f](c)
                ref[at] += change
            return 0

        lax.fori_loop(0, ny // tile, rows, 0)

    def come(cond, copies):
        each(cond, copies, lambda c: c.wait_recv())

    def rims(high, i):
        for f in ((3, 4), (1, 2), (0,))[i]:
            rim(high, f)

    def lower(i):
        come(odd, [up[i]])
        come(hands_down, ([up_across[0]], handed_up[:1], [up_across[1], handed_up[1]])[i])
        if i < 2:
            rims(False, i)

    def upper(i):
        come(even & above_x, [down[i]])
        come(hands_up, ([down_across[0]], handed_down[:1], [down_across[1], handed_down[1]])[i])
        rims(True, i)

    def finish():
        crossed.wait_recv()
        done[...] = jnp.sum(line[...], 0)
        for c in outward:
            c.start()

    pl.when(leader)(finish)

    def sent(k, cond, ref):
        @pl.when(cond)
        def _():
            copy(k, 0, ref, ref, "gx", beside).wait_send()

    sent(2, below_x, xv)
    sent(3, above_y & below_y, q.at[:, :, 0 : 2 * SUB])
    sent(3, above_y ^ below_y, q.at[:, :, 0:SUB])
    sent(4, below_y, dy.at[:, 0:SUB])
    sent(5, above_z, edge)
    sent(5 + both, below_z, edge)
    each(~leader, [inward], lambda c: c.wait_send())
    each(leader, [crossed], lambda c: c.wait_send())

    def sides(turn, _):
        @pl.when((turn == 1) == hands_up)
        def _():
            for i in (2, 0, 1):
                upper(i)

        @pl.when(turn == 0)
        def _():
            for i in range(3):
                lower(i)

        return 0

    lax.fori_loop(0, 2, sides, 0)

    @pl.when(~leader)
    def _():
        outward[0].wait_recv()

    sums[...] = done[...]

    @pl.when(leader)
    def _():
        gathered.wait_send()

    pair = hands_up | hands_down
    sent(main, pair, xh)
    sent(main, ~pair, xlo)
    sent(hand_k, relays, q.at[:, 0, own])


def put(count, den, mom, en, sums, ghost, cells, out_d, out_m, out_e, totals, edge, mean, sem):
    nx = den.shape[0]
    half = nx // 2
    moves = [
        (den.at[2:nx], out_d.at[2:nx], 0),
        (en.at[0:half], out_e.at[0:half], 1),
        (en.at[half:nx], out_e.at[half:nx], 1),
    ]
    for c in range(3):
        moves += [(mom.at[c, h], out_m.at[c, h], 2) for h in (pl.ds(0, half), pl.ds(half, nx - half))]
    for src, dst, k in moves:
        pltpu.make_async_copy(src, dst, sem.at[k]).start()

    line_q = [ghost[0], ghost[1]] + [cells[c] for c in range(3)]
    fl = rim_fluxes(line_q, (cells[3], cells[4]))
    edge[0] = den[0] + (fl[0] - fl[1])
    edge[1] = den[1] + fl[1]
    mean[0] = jnp.sum(sums[0:1]) / count
    mean[1] = jnp.sum(sums[1:2]) / count
    rest = [
        pltpu.make_async_copy(mean, totals, sem.at[3]),
        pltpu.make_async_copy(edge, out_d.at[0:2], sem.at[4]),
    ]
    for c in rest:
        c.start()
    pltpu.make_async_copy(den.at[2:nx], out_d.at[2:nx], sem.at[0]).wait()
    pltpu.make_async_copy(en, out_e, sem.at[1]).wait()
    pltpu.make_async_copy(mom, out_m, sem.at[2]).wait()
    for c in rest:
        c.wait()


def shards(density, momentum, energy, displacement, flags):
    sizes = {a: lax.axis_size(a) for a in AXES}
    nx, ny, nz = density.shape
    tall = ny + 2 * SUB
    per = nz // 4
    parts = -(-6 * nx // per)
    f32, i32 = jnp.float32, jnp.int32
    dma = pltpu.SemaphoreType.DMA
    any_ = pl.BlockSpec(memory_space=pl.ANY)
    hbm = pl.BlockSpec(memory_space=pltpu.HBM)
    vmem = pl.BlockSpec(memory_space=pltpu.VMEM)
    devices = 1
    for a in AXES:
        devices *= sizes[a]
    count = float(nx * ny * nz * devices)
    outputs = tuple(jax.ShapeDtypeStruct(v.shape, f32) for v in (density, momentum, energy))
    results = pl.pallas_call(
        functools.partial(kernel, sizes),
        out_shape=outputs + tuple(
            jax.ShapeDtypeStruct(v, f32) for v in ((2, nz), (2, ny, nz), (5, ny, nz))
        ),
        in_specs=[hbm] * 5,
        out_specs=(vmem,) * 6,
        scratch_shapes=[
            pltpu.SMEM((6,), i32),
            pltpu.VMEM((5, nx, tall, nz), f32),
            pltpu.VMEM((2, nx, ny, nz), i32),
            pltpu.VMEM((nx, tall, nz), i32),
            pltpu.VMEM((2, 5, 2, ny, nz), f32),
            pltpu.VMEM((3, 2, ny, nz), f32),
            pltpu.VMEM((ny, nz), i32),
        ]
        + [pltpu.VMEM((parts, ny, nz), f32) for _ in range(5)]
        + [pltpu.VMEM((2, nz), f32), pltpu.VMEM((sizes["gx"] * sizes["gz"], 2, nz), f32)]
        + [pltpu.VMEM((sizes["gy"], 2, nz), f32), pltpu.VMEM((2, nz), f32)]
        + [dma((6 + (sizes["gz"] > 2),)), dma((14 + (sizes["gz"] > 2),)), pltpu.SemaphoreType.REGULAR((4,)), dma((2,)), dma((2,))],
        compiler_params=pltpu.CompilerParams(
            collective_id=0, has_side_effects=True, vmem_limit_bytes=12 << 20
        ),
    )(
        *(
            pltpu.with_memory_space_constraint(v, pltpu.HBM)
            for v in (flags, density, momentum, energy, displacement)
        )
    )
    return pl.pallas_call(
        functools.partial(put, count),
        out_shape=outputs + (jax.ShapeDtypeStruct((2,), f32),),
        in_specs=[vmem, any_, any_, vmem, vmem, vmem],
        out_specs=(hbm, hbm, hbm, hbm),
        scratch_shapes=[pltpu.VMEM((2, ny, nz), f32), pltpu.SMEM((2,), f32), dma((5,))],
        compiler_params=pltpu.CompilerParams(vmem_limit_bytes=2 << 20),
    )(*results)


def solution(mesh):
    return jax.shard_map(
        shards,
        mesh=mesh,
        in_specs=(
            P("gx", "gy", "gz"),
            P(None, "gx", "gy", "gz"),
            P("gx", "gy", "gz"),
            P(None, "gx", "gy", "gz"),
            P(),
        ),
        out_specs=(P("gx", "gy", "gz"), P(None, "gx", "gy", "gz"), P("gx", "gy", "gz"), P()),
        check_vma=False,
    )
```

```python
import functools

import jax
import jax.numpy as jnp
from jax import lax
from jax.experimental import pallas as pl
from jax.experimental.pallas import tpu as pltpu
from jax.sharding import PartitionSpec as P

AXES = ("gx", "gy", "gz")
SUB = 8


def minmod(p, r):
    return jnp.maximum(jnp.minimum(r, 0.0), jnp.minimum(p, jnp.maximum(r, 0.0)))


def gain(v):
    size = jnp.abs(v)
    return 0.5 * size * (1.0 - size)


def flux(v, g, q_low, q_high, s_low, s_high):
    up = v > 0
    return v * jnp.where(up, q_low, q_high) + g * jnp.where(up, s_low, s_high)


def rim_fluxes(line_q, vs):
    ds = [line_q[i + 1] - line_q[i] for i in range(4)]
    ss = [minmod(ds[i + 1], ds[i]) for i in range(3)]
    return [
        flux(vs[i], gain(vs[i]), line_q[i + 1], line_q[i + 2], ss[i], ss[i + 1]) for i in range(2)
    ]


def kernel(
    sizes, flags_in, den, mom, en, disp, out_d, out_m, out_e, sums, ghost, cells,
    flags, q, dxz, dy, xh, hop, xv, edge, zlo, zhi, cq, cs, part, slots, line, done,
    send_sem, recv_sem, in_sem, sum_send, sum_recv,
):
    nx, ny, nz = den.shape
    pos = {a: lax.axis_index(a) for a in AXES}
    last = {a: sizes[a] - 1 for a in AXES}
    top = ny + SUB
    per = nz // 4
    parts = edge.shape[0]
    scale = 1.0 / 256.0
    xlo, xhi = xh.at[0], xh.at[1]
    dx, dz = dxz.at[0], dxz.at[1]
    own = slice(SUB, top)
    mesh_ids = pl.DeviceIdType.MESH

    def load(src, dst, k):
        return pltpu.make_async_copy(src, dst, send_sem.at[k])

    spans = (slice(0, 2), slice(nx - 2, nx), slice(2, nx - 2))
    loads = []
    for x, k, first in zip(spans, (1, 2, 2), (0, 2, 2)):
        loads += [
            load(den.at[x], q.at[0, x, own], first),
            load(en.at[x], q.at[4, x, own], k),
            load(mom.at[:, x], q.at[1:4, x, own], k),
        ]
    loads += [
        load(flags_in, flags, 3),
        load(disp.at[0], dx, 4),
        load(disp.at[2], dz, 4),
        load(disp.at[1], dy.at[:, own], 5),
    ]
    for c in loads:
        c.start()

    def loaded(ref, k):
        load(ref, ref, k).wait()

    me = pos["gx"]
    par = lax.rem(me, 2)
    odd = par == 1
    end = last["gx"]
    sx, sy, sz = (sizes[a] for a in AXES)
    group = sx * sz
    leader = (me == 0) & (pos["gz"] == last["gz"])
    members = [{"gx": i // sz, "gz": last["gz"] - i % sz} for i in range(1, group)]

    def tell(sem, cond, **target):
        @pl.when(cond)
        def _():
            pl.semaphore_signal(sem, inc=1, device_id=target, device_id_type=mesh_ids)

    even = ~odd
    above = {a: pos[a] < last[a] for a in AXES}
    above_x, above_y, above_z = (above[a] for a in AXES)
    below_x, below_y, below_z = me > 0, pos["gy"] > 0, pos["gz"] > 0
    over = me + 2 <= end
    inner = even & below_x
    barrier = pltpu.get_barrier_semaphore()
    greetings = [
        (even & above_x, odd, {"gx": me + 1}),
        (over, me >= 2, {"gx": me + 2}),
        (above_y, below_y, {"gy": pos["gy"] + 1}),
        (above_z, below_z, {"gz": pos["gz"] + 1}),
    ]
    heard = jnp.where(leader, pos["gy"], 1)
    for speaks, hears, target in greetings:
        tell(barrier, speaks, **target)
        heard += jnp.where(hears, 1, 0)

    @pl.when(leader)
    def _():
        for target in members:
            tell(barrier, True, **target)
        for o in range(1, sy):
            tell(barrier, pos["gy"] + o <= last["gy"], gy=pos["gy"] + o)

    @pl.when(heard > 0)
    def _():
        pl.semaphore_wait(barrier, heard)

    tell(in_sem.at[0], odd, gx=me - 1)
    tell(in_sem.at[0], me >= 2, gx=me - 2)
    tell(in_sem.at[2], below_y, gy=pos["gy"] - 1)
    tell(in_sem.at[2], below_z, gz=pos["gz"] - 1)
    for o in range(1, sy):
        tell(in_sem.at[3], leader & (pos["gy"] >= o), gy=pos["gy"] - o)

    def is_in(k, cond, many=1):
        @pl.when(cond)
        def _():
            pl.semaphore_wait(in_sem.at[k], many)

    def copy(ks, kr, src, dst, axis, step):
        return pltpu.make_async_remote_copy(
            src_ref=src, dst_ref=dst, send_sem=send_sem.at[ks], recv_sem=recv_sem.at[kr],
            device_id={axis: pos[axis] + step}, device_id_type=mesh_ids,
        )

    hands_up, hands_down = odd & above_x, inner
    relays = (odd & (me >= 3)) | (even & over)
    beside = 1 - 2 * par
    main, hand_k, last_k = 0, 1, 5

    groups = (slice(3, 5), slice(1, 3), 0)
    tops, bottoms = slice(nx - 2, nx), slice(0, 2)

    def dst(side, f):
        return ghost if side is xlo and f == 0 else side.at[f]

    def piece(k, i, x, side, first, step):
        f = groups[i]
        return copy(k, first + i, q.at[f, x, own], dst(side, f), "gx", step)

    def one(k, r, x, side, i, step):
        return copy(k, r, q.at[0, x, own], dst(side, 0).at[i], "gx", step)

    up = [piece(main, i, tops, xlo, 0, 1) for i in range(3)]
    down = [piece(main, i, bottoms, xhi, 3, -1) for i in range(3)]
    v_down = copy(2, 6, dx.at[0], xv, "gx", -1)
    keep = ny - SUB
    far, far_last = slice(0, keep), slice(keep, ny)
    up_across = [
        piece(main, 0, tops, xlo, 0, 1),
        one(main, 2, nx - 1, xlo, 1, 1),
        copy(main, 1, q.at[0, nx - 2, SUB + keep : top], ghost.at[0, far_last], "gx", 1),
    ]
    down_across = [piece(main, 0, bottoms, xhi, 3, -1), one(main, 5, 1, xhi, 1, -1)]
    legs_up = [
        copy(main, 7, q.at[1:3, tops, own], hop.at[0:2], "gx", 2),
        copy(main, 4, q.at[0, nx - 2, SUB : SUB + keep], hop.at[2, 0, far], "gx", 2),
    ]
    legs_down = [
        copy(main, 7, q.at[1:3, bottoms, own], hop.at[0:2], "gx", -2),
        copy(main, 7, q.at[0, 0, own], hop.at[2, 0], "gx", -2),
    ]

    def handed(side, rows):
        return [
            copy(hand_k, 8, hop.at[0:2], side.at[1:3], "gx", beside),
            copy(last_k, 9, hop.at[2, 0, rows], dst(side, 0).at[0, rows], "gx", beside),
        ]

    handed_up, handed_down = handed(xlo, far), handed(xhi, slice(0, ny))

    def each(cond, copies, act):
        @pl.when(cond)
        def _():
            for c in copies:
                act(c)

    def go(c):
        c.start()

    hi_rows = slice(top, top + SUB)
    y_up = [copy(3, 10, q.at[:, :, ny:top], q.at[:, :, 0:SUB], "gy", 1)]
    y_down = [
        copy(3, 11, q.at[:, :, SUB : 2 * SUB], q.at[:, :, hi_rows], "gy", -1),
        copy(4, 12, dy.at[:, SUB : 2 * SUB], dy.at[:, hi_rows], "gy", -1),
    ]
    both = sz > 2
    z_up = [copy(6, 13, edge, zlo, "gz", 1)]
    z_down = [copy(6 + both, 13 + both, edge, zhi, "gz", -1)]

    def arrive(axis, ups, downs, fill_low, fill_high):
        @pl.when(pos[axis] > 0)
        def _():
            for c in ups:
                c.wait_recv()

        @pl.when(pos[axis] < last[axis])
        def _():
            for c in downs:
                c.wait_recv()

        @pl.when(pos[axis] == 0)
        def _():
            fill_low()

        @pl.when(pos[axis] == last[axis])
        def _():
            fill_high()

    def sent(axis, ups, downs):
        @pl.when(pos[axis] < last[axis])
        def _():
            for c in ups:
                c.wait_send()

        @pl.when(pos[axis] > 0)
        def _():
            for c in downs:
                c.wait_send()

    loaded(q.at[0, bottoms, own], 0)
    each(odd, down[2:], go)
    loaded(q.at[1:5, bottoms, own], 1)
    loaded(q.at[:, 2:nx, own], 2)
    load(flags_in, flags, 3).wait()
    loaded(dxz, 4)
    loaded(dy.at[:, own], 5)

    flag = [flags[i].astype(jnp.float32) for i in range(6)]

    def low_mult(a):
        return jnp.where(pos[AXES[a]] == 0, flag[2 * a], 1.0)

    def high_mult(a):
        return jnp.where(pos[AXES[a]] == last[AXES[a]], flag[2 * a + 1], 1.0)

    def outer_low(a):
        return jnp.where(pos[AXES[a]] == 0, flag[2 * a], 0.0)

    def outer_high(a):
        return jnp.where(pos[AXES[a]] == last[AXES[a]], flag[2 * a + 1], 0.0)

    lane = lax.broadcasted_iota(jnp.int32, (ny, nz), 1)
    row = lax.broadcasted_iota(jnp.int32, (ny, nz), 0)
    wz = jnp.where(lane == 0, outer_low(2), 0.0) - jnp.where(lane == nz - 1, outer_high(2), 0.0)
    wy = jnp.where(row == 0, outer_low(1), 0.0) - jnp.where(row == ny - 1, outer_high(1), 0.0)
    wx_low, wx_high = outer_low(0), outer_high(0)

    def total(x, carry):
        a, b = carry
        wx = jnp.where(x == 0, wx_low, 0.0) - jnp.where(x == nx - 1, wx_high, 0.0)
        w = 1.0 + scale * (
            wz * dz[x].astype(jnp.float32)
            + wy * dy[x, own].astype(jnp.float32)
            + wx * dx[x].astype(jnp.float32)
        )
        return (
            a + jnp.sum((q[0, x, own] * w).reshape(ny // SUB, SUB, nz), 0),
            b + jnp.sum((q[4, x, own] * w).reshape(ny // SUB, SUB, nz), 0),
        )

    zero = jnp.zeros((SUB, nz), jnp.float32)
    mass, power = lax.fori_loop(0, nx, total, (zero, zero))
    part[0:1] = jnp.sum(mass, 0, keepdims=True)
    part[1:2] = jnp.sum(power, 0, keepdims=True)

    def message(src, dst, ks, kr, target):
        return pltpu.make_async_remote_copy(
            src_ref=src, dst_ref=dst, send_sem=sum_send.at[ks], recv_sem=sum_recv.at[kr],
            device_id=target, device_id_type=mesh_ids,
        )

    home = {"gx": 0, "gz": last["gz"]}
    inward = message(part, slots.at[me * sz + last["gz"] - pos["gz"]], 0, 0, home)
    gathered = message(slots.at[1:group], slots.at[1:group], 1, 0, members[-1])
    across = [
        message(line.at[0], line.at[sy - o], 0, 1, {"gy": lax.rem(pos["gy"] + o, sy)})
        for o in range(1, sy)
    ]
    crossed = message(line.at[1:sy], line.at[1:sy], 0, 1, {"gy": lax.rem(pos["gy"] + 1, sy)})
    outward = [message(done, done, 1, 0, target) for target in members]

    each(~leader, [inward], go)

    each(hands_down, legs_down, go)
    each(below_y, y_down, go)

    def x_sends():
        each(odd, [v_down] + down[:2], go)
        waits = jnp.where(over, 1, 0) + jnp.where(above_x, 1, 0)
        is_in(0, waits > 0, waits)

        @pl.when(even & over)
        def _():
            tell(in_sem.at[0], True, gx=me + 1)
            tell(in_sem.at[1], True, gx=me + 2)

        each(even & above_x, up[:1], go)
        each(odd & over, legs_up, go)
        each(hands_up, up_across, go)
        is_in(1, hands_down)
        each(hands_down, [v_down] + down_across, go)
        each(even & above_x, up[1:], go)

    pl.when(below_x | below_y)(x_sends)

    def pack(x, carry):
        new = list(carry)
        for f in range(6):
            p = f * nx + x
            k = f * nx // per
            at = 4 * lax.rem(p, per)
            plane = q[f, x, own] if f < 5 else dz[x].astype(jnp.float32)
            moved = pltpu.roll(plane, at, 1)
            mine = lax.rem(lane + 2 - at + nz, nz) < 4
            new[k] = jnp.where(mine, moved, new[k])
        return tuple(new)

    packed = lax.fori_loop(0, nx, pack, tuple(jnp.zeros((ny, nz), jnp.float32) for _ in range(parts)))
    for k in range(parts):
        edge[k] = packed[k]
    each(below_z, z_down, go)
    beyond = jnp.where(above_y, 1, 0) + jnp.where(above_z, 1, 0)
    is_in(2, beyond > 0, beyond)
    each(above_z, z_up, go)
    pl.when(~below_x & ~below_y)(x_sends)
    each(above_y, y_up, go)

    outs = (
        lambda x: out_d.at[x], lambda x: out_m.at[0, x], lambda x: out_m.at[1, x],
        lambda x: out_m.at[2, x], lambda x: out_e.at[x],
    )

    def core(r, _):
        at = pl.ds(pl.multiple_of(r * SUB, SUB), SUB)
        inner = pl.ds(pl.multiple_of(r * SUB + SUB, SUB), SUB)
        vs = [dx[c, at].astype(jnp.float32) * scale for c in range(2, nx - 1)]
        gs = [gain(v) for v in vs]
        for f in range(5):
            line_q = [q[f, c, inner] for c in range(nx)]
            ds = [line_q[i + 1] - line_q[i] for i in range(nx - 1)]
            ss = [minmod(ds[i + 1], ds[i]) for i in range(nx - 2)]
            fl = [
                flux(vs[i], gs[i], line_q[i + 1], line_q[i + 2], ss[i], ss[i + 1])
                for i in range(nx - 3)
            ]
            for c in range(nx):
                new = line_q[c]
                if 2 <= c < nx - 1:
                    new = new + fl[c - 2]
                if 1 <= c < nx - 2:
                    new = new - fl[c - 1]
                outs[f](c)[at] = new
        return 0

    lax.fori_loop(0, ny // SUB, core, 0)

    def z_low():
        e = edge[...]
        zlo[...] = jnp.where(lane3 & 3 == 3, pltpu.roll(e, nz - 1, 2), pltpu.roll(e, nz - 2, 2))

    def z_high():
        e = edge[...]
        zhi[...] = jnp.where(lane3 & 3 == 0, pltpu.roll(e, 1, 2), pltpu.roll(e, 2, 2))

    lane3 = lax.broadcasted_iota(jnp.int32, (parts, ny, nz), 2)
    arrive("gz", z_up, z_down, z_low, z_high)
    low = lane & 3 == 0
    for k in range(parts):
        e, l, h = edge[k], zlo[k], zhi[k]
        r1, r2 = pltpu.roll(l, 1, 1), pltpu.roll(l, 2, 1)
        l1, l2 = pltpu.roll(h, nz - 1, 1), pltpu.roll(h, nz - 2, 1)
        cq[k] = jnp.where(low, r1, l1)
        cs[k] = jnp.where(low, minmod(e - r1, r1 - r2), minmod(l2 - l1, l1 - e))

    first, final = lane == 0, lane == nz - 1
    z_lo_mult = jnp.where(first, low_mult(2), 1.0) * scale
    z_hi_mult = high_mult(2) * scale
    def along_z(x, _):
        v = dz[x].astype(jnp.float32) * z_lo_mult
        g = gain(v)

        def ghosts(ref, f):
            back = lax.rem(nz - 4 * lax.rem(f * nx + x, per), nz)
            return pltpu.roll(ref[f * nx // per], back, 1)

        vh = ghosts(cq, 5) * z_hi_mult
        gh = gain(vh)
        for f in range(5):
            plane = q[f, x, SUB:top]
            gq, gs = ghosts(cq, f), ghosts(cs, f)
            qm = jnp.where(first, gq, pltpu.roll(plane, 1, 1))
            d = plane - qm
            s = minmod(jnp.where(final, gq - plane, pltpu.roll(d, nz - 1, 1)), d)
            sm = jnp.where(first, gs, pltpu.roll(s, 1, 1))
            fl = flux(v, g, qm, plane, sm, s)
            fh = jnp.where(final, flux(vh, gh, plane, gq, s, gs), pltpu.roll(fl, nz - 1, 1))
            outs[f](x)[...] += fl - fh
        return 0

    early = nx * 5 // 8
    lax.fori_loop(0, early, along_z, 0)

    def gather():
        gathered.wait_recv()
        line[0] = part[...] + jnp.sum(slots[1:group], 0)
        is_in(3, above_y, last["gy"] - pos["gy"])
        for c in across:
            c.start()

    pl.when(leader & below_y)(gather)
    lax.fori_loop(early, nx, along_z, 0)

    each(relays & odd, legs_up, lambda c: c.wait_recv())

    @pl.when(relays & even)
    def _():
        copy(hand_k, 7, q.at[:, 0, own], q.at[:, 0, own], "gx", beside).wait_recv()

    each(relays & odd, handed_up, go)
    each(relays & even, handed_down, go)

    def y_low():
        q[:, :, 0:SUB] = jnp.broadcast_to(q[:, :, SUB : SUB + 1], (5, nx, SUB, nz))

    def y_high():
        q[:, :, hi_rows] = jnp.broadcast_to(q[:, :, top - 1 : top], (5, nx, SUB, nz))
        dy[:, hi_rows] = jnp.broadcast_to(dy[:, top - 1 : top], (nx, SUB, nz))

    arrive("gy", y_up, y_down, y_low, y_high)
    pl.when(leader & ~below_y)(gather)
    tall = ny + 2 * SUB
    rows = lax.broadcasted_iota(jnp.int32, (tall, nz), 0)
    inside = (rows >= SUB) & (rows <= top)
    y_mult = jnp.where(
        rows == SUB, low_mult(1) * scale, jnp.where(rows == top, high_mult(1) * scale, scale)
    )

    def along_y(x, _):
        v = jnp.where(inside, dy[x].astype(jnp.float32), 0.0) * y_mult
        g = gain(v)
        for f in range(5):
            plane = q[f, x]
            qm = pltpu.roll(plane, 1, 0)
            d = plane - qm
            s = minmod(pltpu.roll(d, tall - 1, 0), d)
            fl = flux(v, g, qm, plane, pltpu.roll(s, 1, 0), s)
            ch = fl - pltpu.roll(fl, tall - 1, 0)
            outs[f](x)[...] += ch[SUB:top]
        return 0

    lax.fori_loop(0, nx, along_y, 0)

    @pl.when(me == 0)
    def _():
        xlo[...] = jnp.broadcast_to(q[:, 0:1, own], (5, 2, ny, nz))
        ghost[...] = jnp.broadcast_to(q[0, 0:1, own], (2, ny, nz))

    @pl.when(me == end)
    def _():
        xhi[...] = jnp.broadcast_to(q[:, nx - 1 : nx, own], (5, 2, ny, nz))
        xv[...] = dx[nx - 1]

    each(above_x, [v_down], lambda c: c.wait_recv())
    x_lo_mult, x_hi_mult = low_mult(0) * scale, high_mult(0) * scale

    tile = 4 * SUB if ny % (4 * SUB) == 0 else SUB

    cells[0:3] = q[0, 0:3, own]
    cells[3] = dx[0].astype(jnp.float32) * x_lo_mult
    cells[4] = dx[1].astype(jnp.float32) * scale

    def rim(high, f):
        def rows(r, _):
            at = pl.ds(pl.multiple_of(r * tile, SUB), tile)
            inner = pl.ds(pl.multiple_of(r * tile + SUB, SUB), tile)
            if high:
                line_q = [q[f, c, inner] for c in range(nx - 3, nx)] + [xhi[f, i, at] for i in range(2)]
                vs = (dx[nx - 1, at].astype(jnp.float32) * scale, xv[at].astype(jnp.float32) * x_hi_mult)
            else:
                line_q = [xlo[f, i, at] for i in range(2)] + [q[f, c, inner] for c in range(3)]
                vs = (dx[0, at].astype(jnp.float32) * x_lo_mult, dx[1, at].astype(jnp.float32) * scale)
            fl = rim_fluxes(line_q, vs)
            if high:
                changes = ((nx - 2, -fl[0]), (nx - 1, fl[0] - fl[1]))
            else:
                changes = ((0, fl[0] - fl[1]), (1, fl[1]))
            for c, change in changes:
                ref = outs[f](c)
                ref[at] += change
            return 0

        lax.fori_loop(0, ny // tile, rows, 0)

    def come(cond, copies):
        each(cond, copies, lambda c: c.wait_recv())

    def rims(high, i):
        for f in ((3, 4), (1, 2), (0,))[i]:
            rim(high, f)

    def lower(i):
        come(odd, [up[i]])
        come(hands_down, ([up_across[0]], handed_up[:1], up_across[1:] + handed_up[1:])[i])
        if i < 2:
            rims(False, i)

    def upper(i):
        come(even & above_x, [down[i]])
        come(hands_up, ([down_across[0]], handed_down[:1], [down_across[1], handed_down[1]])[i])
        rims(True, i)

    def finish():
        crossed.wait_recv()
        done[...] = jnp.sum(line[...], 0)
        for c in outward:
            c.start()

    pl.when(leader)(finish)

    def sides(turn, _):
        @pl.when((turn == 1) == hands_up)
        def _():
            for i in (2, 0, 1):
                upper(i)

        @pl.when(turn == 0)
        def _():
            for i in range(3):
                lower(i)

        return 0

    lax.fori_loop(0, 2, sides, 0)

    @pl.when(~leader)
    def _():
        outward[0].wait_recv()
        inward.wait_send()

    sums[...] = done[...]

    @pl.when(leader)
    def _():
        crossed.wait_send()
        gathered.wait_send()

    def sent(k, cond, ref):
        @pl.when(cond)
        def _():
            copy(k, 0, ref, ref, "gx", beside).wait_send()

    pair = hands_up | hands_down
    sent(main, pair, xh)
    sent(main, ~pair, xlo)
    each(relays & odd, handed_up, lambda c: c.wait_send())
    each(relays & even, handed_down, lambda c: c.wait_send())
    sent(2, below_x, xv)
    sent(3, above_y & below_y, q.at[:, :, 0 : 2 * SUB])
    sent(3, above_y ^ below_y, q.at[:, :, 0:SUB])
    sent(4, below_y, dy.at[:, 0:SUB])
    sent(6, above_z, edge)
    sent(6 + both, below_z, edge)


def put(count, den, mom, en, sums, ghost, cells, out_d, out_m, out_e, totals, edge, mean, sem):
    nx = den.shape[0]
    half = nx // 2
    moves = [
        (den.at[2:nx], out_d.at[2:nx], 0),
        (en.at[0:half], out_e.at[0:half], 1),
        (en.at[half:nx], out_e.at[half:nx], 1),
    ]
    for c in range(3):
        moves += [(mom.at[c, h], out_m.at[c, h], 2) for h in (pl.ds(0, half), pl.ds(half, nx - half))]
    for src, dst, k in moves:
        pltpu.make_async_copy(src, dst, sem.at[k]).start()

    line_q = [ghost[0], ghost[1]] + [cells[c] for c in range(3)]
    fl = rim_fluxes(line_q, (cells[3], cells[4]))
    edge[0] = den[0] + (fl[0] - fl[1])
    edge[1] = den[1] + fl[1]
    mean[0] = jnp.sum(sums[0:1]) / count
    mean[1] = jnp.sum(sums[1:2]) / count
    rest = [
        pltpu.make_async_copy(mean, totals, sem.at[3]),
        pltpu.make_async_copy(edge, out_d.at[0:2], sem.at[4]),
    ]
    for c in rest:
        c.start()
    pltpu.make_async_copy(den.at[2:nx], out_d.at[2:nx], sem.at[0]).wait()
    pltpu.make_async_copy(en, out_e, sem.at[1]).wait()
    pltpu.make_async_copy(mom, out_m, sem.at[2]).wait()
    for c in rest:
        c.wait()


def shards(density, momentum, energy, displacement, flags):
    sizes = {a: lax.axis_size(a) for a in AXES}
    nx, ny, nz = density.shape
    tall = ny + 2 * SUB
    per = nz // 4
    parts = -(-6 * nx // per)
    f32, i32 = jnp.float32, jnp.int32
    dma = pltpu.SemaphoreType.DMA
    any_ = pl.BlockSpec(memory_space=pl.ANY)
    hbm = pl.BlockSpec(memory_space=pltpu.HBM)
    vmem = pl.BlockSpec(memory_space=pltpu.VMEM)
    devices = 1
    for a in AXES:
        devices *= sizes[a]
    count = float(nx * ny * nz * devices)
    outputs = tuple(jax.ShapeDtypeStruct(v.shape, f32) for v in (density, momentum, energy))
    results = pl.pallas_call(
        functools.partial(kernel, sizes),
        out_shape=outputs + tuple(
            jax.ShapeDtypeStruct(v, f32) for v in ((2, nz), (2, ny, nz), (5, ny, nz))
        ),
        in_specs=[hbm] * 5,
        out_specs=(vmem,) * 6,
        scratch_shapes=[
            pltpu.SMEM((6,), i32),
            pltpu.VMEM((5, nx, tall, nz), f32),
            pltpu.VMEM((2, nx, ny, nz), i32),
            pltpu.VMEM((nx, tall, nz), i32),
            pltpu.VMEM((2, 5, 2, ny, nz), f32),
            pltpu.VMEM((3, 2, ny, nz), f32),
            pltpu.VMEM((ny, nz), i32),
        ]
        + [pltpu.VMEM((parts, ny, nz), f32) for _ in range(5)]
        + [pltpu.VMEM((2, nz), f32), pltpu.VMEM((sizes["gx"] * sizes["gz"], 2, nz), f32)]
        + [pltpu.VMEM((sizes["gy"], 2, nz), f32), pltpu.VMEM((2, nz), f32)]
        + [dma((7 + (sizes["gz"] > 2),)), dma((14 + (sizes["gz"] > 2),)), pltpu.SemaphoreType.REGULAR((4,)), dma((2,)), dma((2,))],
        compiler_params=pltpu.CompilerParams(
            collective_id=0, has_side_effects=True, vmem_limit_bytes=12 << 20
        ),
    )(
        *(
            pltpu.with_memory_space_constraint(v, pltpu.HBM)
            for v in (flags, density, momentum, energy, displacement)
        )
    )
    return pl.pallas_call(
        functools.partial(put, count),
        out_shape=outputs + (jax.ShapeDtypeStruct((2,), f32),),
        in_specs=[vmem, any_, any_, vmem, vmem, vmem],
        out_specs=(hbm, hbm, hbm, hbm),
        scratch_shapes=[pltpu.VMEM((2, ny, nz), f32), pltpu.SMEM((2,), f32), dma((5,))],
        compiler_params=pltpu.CompilerParams(vmem_limit_bytes=2 << 20),
    )(*results)


def solution(mesh):
    return jax.shard_map(
        shards,
        mesh=mesh,
        in_specs=(
            P("gx", "gy", "gz"),
            P(None, "gx", "gy", "gz"),
            P("gx", "gy", "gz"),
            P(None, "gx", "gy", "gz"),
            P(),
        ),
        out_specs=(P("gx", "gy", "gz"), P(None, "gx", "gy", "gz"), P("gx", "gy", "gz"), P()),
        check_vma=False,
    )
```

```python
import functools

import jax
import jax.numpy as jnp
from jax import lax
from jax.experimental import pallas as pl
from jax.experimental.pallas import tpu as pltpu
from jax.sharding import PartitionSpec as P

AXES = ("gx", "gy", "gz")
SUB = 8


def minmod(p, r):
    return jnp.maximum(jnp.minimum(r, 0.0), jnp.minimum(p, jnp.maximum(r, 0.0)))


def gain(v):
    size = jnp.abs(v)
    return 0.5 * size * (1.0 - size)


def flux(v, g, q_low, q_high, s_low, s_high):
    up = v > 0
    return v * jnp.where(up, q_low, q_high) + g * jnp.where(up, s_low, s_high)


def rim_fluxes(line_q, vs):
    ds = [line_q[i + 1] - line_q[i] for i in range(4)]
    ss = [minmod(ds[i + 1], ds[i]) for i in range(3)]
    return [
        flux(vs[i], gain(vs[i]), line_q[i + 1], line_q[i + 2], ss[i], ss[i + 1]) for i in range(2)
    ]


def kernel(
    sizes, flags_in, den, mom, en, disp, out_d, out_m, out_e, sums, ghost, cells,
    flags, q, dxz, dy, xh, hop, xv, edge, zlo, zhi, cq, cs, part, slots, line, done,
    send_sem, recv_sem, in_sem, sum_send, sum_recv,
):
    nx, ny, nz = den.shape
    pos = {a: lax.axis_index(a) for a in AXES}
    last = {a: sizes[a] - 1 for a in AXES}
    top = ny + SUB
    per = nz // 4
    parts = edge.shape[0]
    scale = 1.0 / 256.0
    xlo, xhi = xh.at[0], xh.at[1]
    dx, dz = dxz.at[0], dxz.at[1]
    own = slice(SUB, top)
    mesh_ids = pl.DeviceIdType.MESH

    def load(src, dst, k):
        return pltpu.make_async_copy(src, dst, send_sem.at[k])

    spans = (slice(0, 2), slice(nx - 2, nx), slice(2, nx - 2))
    loads = []
    for x, k, first in zip(spans, (1, 2, 2), (0, 2, 2)):
        loads += [
            load(den.at[x], q.at[0, x, own], first),
            load(en.at[x], q.at[4, x, own], k),
            load(mom.at[:, x], q.at[1:4, x, own], k),
        ]
    loads += [
        load(flags_in, flags, 3),
        load(disp.at[0], dx, 4),
        load(disp.at[2], dz, 4),
        load(disp.at[1], dy.at[:, own], 5),
    ]
    for c in loads:
        c.start()

    def loaded(ref, k):
        load(ref, ref, k).wait()

    me = pos["gx"]
    par = lax.rem(me, 2)
    odd = par == 1
    end = last["gx"]
    sx, sy, sz = (sizes[a] for a in AXES)
    group = sx * sz
    leader = (me == 0) & (pos["gz"] == last["gz"])
    members = [{"gx": i // sz, "gz": last["gz"] - i % sz} for i in range(1, group)]

    def tell(sem, cond, **target):
        @pl.when(cond)
        def _():
            pl.semaphore_signal(sem, inc=1, device_id=target, device_id_type=mesh_ids)

    even = ~odd
    above = {a: pos[a] < last[a] for a in AXES}
    above_x, above_y, above_z = (above[a] for a in AXES)
    below_x, below_y, below_z = me > 0, pos["gy"] > 0, pos["gz"] > 0
    over = me + 2 <= end
    inner = even & below_x
    barrier = pltpu.get_barrier_semaphore()
    greetings = [
        (even & above_x, odd, {"gx": me + 1}),
        (over, me >= 2, {"gx": me + 2}),
        (above_y, below_y, {"gy": pos["gy"] + 1}),
        (above_z, below_z, {"gz": pos["gz"] + 1}),
    ]
    heard = jnp.where(leader, pos["gy"], 1)
    for speaks, hears, target in greetings:
        tell(barrier, speaks, **target)
        heard += jnp.where(hears, 1, 0)

    @pl.when(leader)
    def _():
        for target in members:
            tell(barrier, True, **target)
        for o in range(1, sy):
            tell(barrier, pos["gy"] + o <= last["gy"], gy=pos["gy"] + o)

    @pl.when(heard > 0)
    def _():
        pl.semaphore_wait(barrier, heard)

    tell(in_sem.at[0], odd, gx=me - 1)
    tell(in_sem.at[0], me >= 2, gx=me - 2)
    tell(in_sem.at[2], below_y, gy=pos["gy"] - 1)
    tell(in_sem.at[2], below_z, gz=pos["gz"] - 1)
    for o in range(1, sy):
        tell(in_sem.at[3], leader & (pos["gy"] >= o), gy=pos["gy"] - o)

    def is_in(k, cond, many=1):
        @pl.when(cond)
        def _():
            pl.semaphore_wait(in_sem.at[k], many)

    def copy(ks, kr, src, dst, axis, step):
        return pltpu.make_async_remote_copy(
            src_ref=src, dst_ref=dst, send_sem=send_sem.at[ks], recv_sem=recv_sem.at[kr],
            device_id={axis: pos[axis] + step}, device_id_type=mesh_ids,
        )

    hands_up, hands_down = odd & above_x, inner
    relays = (odd & (me >= 3)) | (even & over)
    beside = 1 - 2 * par
    main, hand_k, last_k = 0, 1, 5

    groups = (slice(3, 5), slice(1, 3), 0)
    tops, bottoms = slice(nx - 2, nx), slice(0, 2)

    def dst(side, f):
        return ghost if side is xlo and f == 0 else side.at[f]

    def piece(k, i, x, side, first, step):
        f = groups[i]
        return copy(k, first + i, q.at[f, x, own], dst(side, f), "gx", step)

    def one(k, r, x, side, i, step):
        return copy(k, r, q.at[0, x, own], dst(side, 0).at[i], "gx", step)

    up = [piece(main, i, tops, xlo, 0, 1) for i in range(3)]
    down = [piece(main, i, bottoms, xhi, 3, -1) for i in range(3)]
    v_down = copy(2, 6, dx.at[0], xv, "gx", -1)
    keep = ny - SUB
    far, far_last = slice(0, keep), slice(keep, ny)
    up_across = [
        piece(main, 0, tops, xlo, 0, 1),
        one(main, 2, nx - 1, xlo, 1, 1),
        copy(main, 1, q.at[0, nx - 2, SUB + keep : top], ghost.at[0, far_last], "gx", 1),
    ]
    down_across = [piece(main, 0, bottoms, xhi, 3, -1), one(main, 5, 1, xhi, 1, -1)]
    legs_up = [
        copy(main, 7, q.at[1:3, tops, own], hop.at[0:2], "gx", 2),
        copy(main, 4, q.at[0, nx - 2, SUB : SUB + keep], hop.at[2, 0, far], "gx", 2),
    ]
    legs_down = [
        copy(main, 7, q.at[1:3, bottoms, own], hop.at[0:2], "gx", -2),
        copy(main, 7, q.at[0, 0, own], hop.at[2, 0], "gx", -2),
    ]

    def handed(side, rows):
        return [
            copy(hand_k, 8, hop.at[0:2], side.at[1:3], "gx", beside),
            copy(last_k, 9, hop.at[2, 0, rows], dst(side, 0).at[0, rows], "gx", beside),
        ]

    handed_up, handed_down = handed(xlo, far), handed(xhi, slice(0, ny))

    def each(cond, copies, act):
        @pl.when(cond)
        def _():
            for c in copies:
                act(c)

    def go(c):
        c.start()

    hi_rows = slice(top, top + SUB)
    y_up = [copy(3, 10, q.at[:, :, ny:top], q.at[:, :, 0:SUB], "gy", 1)]
    y_down = [
        copy(3, 11, q.at[:, :, SUB : 2 * SUB], q.at[:, :, hi_rows], "gy", -1),
        copy(4, 12, dy.at[:, SUB : 2 * SUB], dy.at[:, hi_rows], "gy", -1),
    ]
    both = sz > 2
    z_up = [copy(6, 13, edge, zlo, "gz", 1)]
    z_down = [copy(6 + both, 13 + both, edge, zhi, "gz", -1)]

    def arrive(axis, ups, downs, fill_low, fill_high):
        @pl.when(pos[axis] > 0)
        def _():
            for c in ups:
                c.wait_recv()

        @pl.when(pos[axis] < last[axis])
        def _():
            for c in downs:
                c.wait_recv()

        @pl.when(pos[axis] == 0)
        def _():
            fill_low()

        @pl.when(pos[axis] == last[axis])
        def _():
            fill_high()

    def sent(axis, ups, downs):
        @pl.when(pos[axis] < last[axis])
        def _():
            for c in ups:
                c.wait_send()

        @pl.when(pos[axis] > 0)
        def _():
            for c in downs:
                c.wait_send()

    loaded(q.at[0, bottoms, own], 0)
    each(odd, down[2:], go)
    loaded(q.at[1:5, bottoms, own], 1)
    loaded(q.at[:, 2:nx, own], 2)
    load(flags_in, flags, 3).wait()
    loaded(dxz, 4)
    loaded(dy.at[:, own], 5)

    flag = [flags[i].astype(jnp.float32) for i in range(6)]

    def low_mult(a):
        return jnp.where(pos[AXES[a]] == 0, flag[2 * a], 1.0)

    def high_mult(a):
        return jnp.where(pos[AXES[a]] == last[AXES[a]], flag[2 * a + 1], 1.0)

    def outer_low(a):
        return jnp.where(pos[AXES[a]] == 0, flag[2 * a], 0.0)

    def outer_high(a):
        return jnp.where(pos[AXES[a]] == last[AXES[a]], flag[2 * a + 1], 0.0)

    lane = lax.broadcasted_iota(jnp.int32, (ny, nz), 1)
    row = lax.broadcasted_iota(jnp.int32, (ny, nz), 0)
    wz = jnp.where(lane == 0, outer_low(2), 0.0) - jnp.where(lane == nz - 1, outer_high(2), 0.0)
    wy = jnp.where(row == 0, outer_low(1), 0.0) - jnp.where(row == ny - 1, outer_high(1), 0.0)
    wx_low, wx_high = outer_low(0), outer_high(0)

    def total(x, carry):
        a, b = carry
        wx = jnp.where(x == 0, wx_low, 0.0) - jnp.where(x == nx - 1, wx_high, 0.0)
        w = 1.0 + scale * (
            wz * dz[x].astype(jnp.float32)
            + wy * dy[x, own].astype(jnp.float32)
            + wx * dx[x].astype(jnp.float32)
        )
        return (
            a + jnp.sum((q[0, x, own] * w).reshape(ny // SUB, SUB, nz), 0),
            b + jnp.sum((q[4, x, own] * w).reshape(ny // SUB, SUB, nz), 0),
        )

    zero = jnp.zeros((SUB, nz), jnp.float32)
    mass, power = lax.fori_loop(0, nx, total, (zero, zero))
    part[0:1] = jnp.sum(mass, 0, keepdims=True)
    part[1:2] = jnp.sum(power, 0, keepdims=True)

    def message(src, dst, ks, kr, target):
        return pltpu.make_async_remote_copy(
            src_ref=src, dst_ref=dst, send_sem=sum_send.at[ks], recv_sem=sum_recv.at[kr],
            device_id=target, device_id_type=mesh_ids,
        )

    home = {"gx": 0, "gz": last["gz"]}
    inward = message(part, slots.at[me * sz + last["gz"] - pos["gz"]], 0, 0, home)
    gathered = message(slots.at[1:group], slots.at[1:group], 1, 0, members[-1])
    across = [
        message(line.at[0], line.at[sy - o], 0, 1, {"gy": lax.rem(pos["gy"] + o, sy)})
        for o in range(1, sy)
    ]
    crossed = message(line.at[1:sy], line.at[1:sy], 0, 1, {"gy": lax.rem(pos["gy"] + 1, sy)})
    outward = [message(done, done, 1, 0, target) for target in members]

    each(~leader, [inward], go)

    each(hands_down, legs_down, go)
    each(below_y, y_down, go)

    def x_sends():
        each(odd, [v_down] + down[:2], go)
        waits = jnp.where(over, 1, 0) + jnp.where(above_x, 1, 0)
        is_in(0, waits > 0, waits)

        @pl.when(even & over)
        def _():
            tell(in_sem.at[0], True, gx=me + 1)
            tell(in_sem.at[1], True, gx=me + 2)

        each(even & above_x, up[:1], go)
        each(odd & over, legs_up, go)
        each(hands_up, up_across, go)
        is_in(1, hands_down)
        each(hands_down, [v_down] + down_across, go)
        each(even & above_x, up[1:], go)

    pl.when(below_x | below_y)(x_sends)

    def pack(x, carry):
        new = list(carry)
        for f in range(6):
            p = f * nx + x
            k = f * nx // per
            at = 4 * lax.rem(p, per)
            plane = q[f, x, own] if f < 5 else dz[x].astype(jnp.float32)
            moved = pltpu.roll(plane, at, 1)
            mine = lax.rem(lane + 2 - at + nz, nz) < 4
            new[k] = jnp.where(mine, moved, new[k])
        return tuple(new)

    packed = lax.fori_loop(0, nx, pack, tuple(jnp.zeros((ny, nz), jnp.float32) for _ in range(parts)))
    for k in range(parts):
        edge[k] = packed[k]
    each(below_z, z_down, go)
    beyond = jnp.where(above_y, 1, 0) + jnp.where(above_z, 1, 0)
    is_in(2, beyond > 0, beyond)
    each(above_z, z_up, go)
    pl.when(~below_x & ~below_y)(x_sends)
    each(above_y, y_up, go)

    outs = (
        lambda x: out_d.at[x], lambda x: out_m.at[0, x], lambda x: out_m.at[1, x],
        lambda x: out_m.at[2, x], lambda x: out_e.at[x],
    )

    def core(r, _):
        at = pl.ds(pl.multiple_of(r * SUB, SUB), SUB)
        inner = pl.ds(pl.multiple_of(r * SUB + SUB, SUB), SUB)
        vs = [dx[c, at].astype(jnp.float32) * scale for c in range(2, nx - 1)]
        gs = [gain(v) for v in vs]
        for f in range(5):
            line_q = [q[f, c, inner] for c in range(nx)]
            ds = [line_q[i + 1] - line_q[i] for i in range(nx - 1)]
            ss = [minmod(ds[i + 1], ds[i]) for i in range(nx - 2)]
            fl = [
                flux(vs[i], gs[i], line_q[i + 1], line_q[i + 2], ss[i], ss[i + 1])
                for i in range(nx - 3)
            ]
            for c in range(nx):
                new = line_q[c]
                if 2 <= c < nx - 1:
                    new = new + fl[c - 2]
                if 1 <= c < nx - 2:
                    new = new - fl[c - 1]
                outs[f](c)[at] = new
        return 0

    lax.fori_loop(0, ny // SUB, core, 0)

    def z_low():
        e = edge[...]
        zlo[...] = jnp.where(lane3 & 3 == 3, pltpu.roll(e, nz - 1, 2), pltpu.roll(e, nz - 2, 2))

    def z_high():
        e = edge[...]
        zhi[...] = jnp.where(lane3 & 3 == 0, pltpu.roll(e, 1, 2), pltpu.roll(e, 2, 2))

    lane3 = lax.broadcasted_iota(jnp.int32, (parts, ny, nz), 2)
    arrive("gz", z_up, z_down, z_low, z_high)
    low = lane & 3 == 0
    for k in range(parts):
        e, l, h = edge[k], zlo[k], zhi[k]
        r1, r2 = pltpu.roll(l, 1, 1), pltpu.roll(l, 2, 1)
        l1, l2 = pltpu.roll(h, nz - 1, 1), pltpu.roll(h, nz - 2, 1)
        cq[k] = jnp.where(low, r1, l1)
        cs[k] = jnp.where(low, minmod(e - r1, r1 - r2), minmod(l2 - l1, l1 - e))

    first, final = lane == 0, lane == nz - 1
    z_lo_mult = jnp.where(first, low_mult(2), 1.0) * scale
    z_hi_mult = high_mult(2) * scale
    def along_z(x, _):
        v = dz[x].astype(jnp.float32) * z_lo_mult
        g = gain(v)

        def ghosts(ref, f):
            back = lax.rem(nz - 4 * lax.rem(f * nx + x, per), nz)
            return pltpu.roll(ref[f * nx // per], back, 1)

        vh = ghosts(cq, 5) * z_hi_mult
        gh = gain(vh)
        for f in range(5):
            plane = q[f, x, SUB:top]
            gq, gs = ghosts(cq, f), ghosts(cs, f)
            qm = jnp.where(first, gq, pltpu.roll(plane, 1, 1))
            d = plane - qm
            s = minmod(jnp.where(final, gq - plane, pltpu.roll(d, nz - 1, 1)), d)
            sm = jnp.where(first, gs, pltpu.roll(s, 1, 1))
            fl = flux(v, g, qm, plane, sm, s)
            fh = jnp.where(final, flux(vh, gh, plane, gq, s, gs), pltpu.roll(fl, nz - 1, 1))
            outs[f](x)[...] += fl - fh
        return 0

    early = nx * 5 // 8
    lax.fori_loop(0, early, along_z, 0)

    def gather():
        gathered.wait_recv()
        line[0] = part[...] + jnp.sum(slots[1:group], 0)
        is_in(3, above_y, last["gy"] - pos["gy"])
        for c in across:
            c.start()

    pl.when(leader & below_y)(gather)
    lax.fori_loop(early, nx, along_z, 0)

    each(relays & odd, legs_up, lambda c: c.wait_recv())

    @pl.when(relays & even)
    def _():
        copy(hand_k, 7, q.at[:, 0, own], q.at[:, 0, own], "gx", beside).wait_recv()

    each(relays & odd, handed_up, go)
    each(relays & even, handed_down, go)

    def y_low():
        q[:, :, 0:SUB] = jnp.broadcast_to(q[:, :, SUB : SUB + 1], (5, nx, SUB, nz))

    def y_high():
        q[:, :, hi_rows] = jnp.broadcast_to(q[:, :, top - 1 : top], (5, nx, SUB, nz))
        dy[:, hi_rows] = jnp.broadcast_to(dy[:, top - 1 : top], (nx, SUB, nz))

    arrive("gy", y_up, y_down, y_low, y_high)
    pl.when(leader & ~below_y)(gather)
    tall = ny + 2 * SUB
    rows = lax.broadcasted_iota(jnp.int32, (tall, nz), 0)
    inside = (rows >= SUB) & (rows <= top)
    y_mult = jnp.where(
        rows == SUB, low_mult(1) * scale, jnp.where(rows == top, high_mult(1) * scale, scale)
    )

    def along_y(x, _):
        v = jnp.where(inside, dy[x].astype(jnp.float32), 0.0) * y_mult
        g = gain(v)
        for f in range(5):
            plane = q[f, x]
            qm = pltpu.roll(plane, 1, 0)
            d = plane - qm
            s = minmod(pltpu.roll(d, tall - 1, 0), d)
            fl = flux(v, g, qm, plane, pltpu.roll(s, 1, 0), s)
            ch = fl - pltpu.roll(fl, tall - 1, 0)
            outs[f](x)[...] += ch[SUB:top]
        return 0

    lax.fori_loop(0, nx, along_y, 0)

    @pl.when(me == 0)
    def _():
        xlo[...] = jnp.broadcast_to(q[:, 0:1, own], (5, 2, ny, nz))
        ghost[...] = jnp.broadcast_to(q[0, 0:1, own], (2, ny, nz))

    @pl.when(me == end)
    def _():
        xhi[...] = jnp.broadcast_to(q[:, nx - 1 : nx, own], (5, 2, ny, nz))
        xv[...] = dx[nx - 1]

    each(above_x, [v_down], lambda c: c.wait_recv())
    x_lo_mult, x_hi_mult = low_mult(0) * scale, high_mult(0) * scale

    tile = 4 * SUB if ny % (4 * SUB) == 0 else SUB

    cells[0:3] = q[0, 0:3, own]
    cells[3] = dx[0].astype(jnp.float32) * x_lo_mult
    cells[4] = dx[1].astype(jnp.float32) * scale

    def rim(high, f):
        def rows(r, _):
            at = pl.ds(pl.multiple_of(r * tile, SUB), tile)
            inner = pl.ds(pl.multiple_of(r * tile + SUB, SUB), tile)
            if high:
                line_q = [q[f, c, inner] for c in range(nx - 3, nx)] + [xhi[f, i, at] for i in range(2)]
                vs = (dx[nx - 1, at].astype(jnp.float32) * scale, xv[at].astype(jnp.float32) * x_hi_mult)
            else:
                line_q = [xlo[f, i, at] for i in range(2)] + [q[f, c, inner] for c in range(3)]
                vs = (dx[0, at].astype(jnp.float32) * x_lo_mult, dx[1, at].astype(jnp.float32) * scale)
            fl = rim_fluxes(line_q, vs)
            if high:
                changes = ((nx - 2, -fl[0]), (nx - 1, fl[0] - fl[1]))
            else:
                changes = ((0, fl[0] - fl[1]), (1, fl[1]))
            for c, change in changes:
                ref = outs[f](c)
                ref[at] += change
            return 0

        lax.fori_loop(0, ny // tile, rows, 0)

    def come(cond, copies):
        each(cond, copies, lambda c: c.wait_recv())

    def rims(high, i):
        for f in ((3, 4), (1, 2), (0,))[i]:
            rim(high, f)

    def lower(i):
        come(odd, [up[i]])
        come(hands_down, ([up_across[0]], handed_up[:1], up_across[1:] + handed_up[1:])[i])
        if i < 2:
            rims(False, i)

    def upper(i):
        come(even & above_x, [down[i]])
        come(hands_up, ([down_across[0]], handed_down[:1], [down_across[1], handed_down[1]])[i])
        rims(True, i)

    def finish():
        crossed.wait_recv()
        done[...] = jnp.sum(line[...], 0)
        for c in outward:
            c.start()

    pl.when(leader)(finish)

    def sent(k, cond, ref):
        @pl.when(cond)
        def _():
            copy(k, 0, ref, ref, "gx", beside).wait_send()

    sent(2, below_x, xv)
    sent(3, above_y & below_y, q.at[:, :, 0 : 2 * SUB])
    sent(3, above_y ^ below_y, q.at[:, :, 0:SUB])
    sent(4, below_y, dy.at[:, 0:SUB])
    sent(6, above_z, edge)
    sent(6 + both, below_z, edge)
    each(~leader, [inward], lambda c: c.wait_send())
    each(leader, [crossed], lambda c: c.wait_send())

    def sides(turn, _):
        @pl.when((turn == 1) == hands_up)
        def _():
            for i in (2, 0, 1):
                upper(i)

        @pl.when(turn == 0)
        def _():
            for i in range(3):
                lower(i)

        return 0

    lax.fori_loop(0, 2, sides, 0)

    @pl.when(~leader)
    def _():
        outward[0].wait_recv()

    sums[...] = done[...]

    @pl.when(leader)
    def _():
        gathered.wait_send()

    pair = hands_up | hands_down
    sent(main, pair, xh)
    sent(main, ~pair, xlo)
    each(relays & odd, handed_up, lambda c: c.wait_send())
    each(relays & even, handed_down, lambda c: c.wait_send())


def put(count, den, mom, en, sums, ghost, cells, out_d, out_m, out_e, totals, edge, mean, sem):
    nx = den.shape[0]
    half = nx // 2
    moves = [
        (den.at[2:nx], out_d.at[2:nx], 0),
        (en.at[0:half], out_e.at[0:half], 1),
        (en.at[half:nx], out_e.at[half:nx], 1),
    ]
    for c in range(3):
        moves += [(mom.at[c, h], out_m.at[c, h], 2) for h in (pl.ds(0, half), pl.ds(half, nx - half))]
    for src, dst, k in moves:
        pltpu.make_async_copy(src, dst, sem.at[k]).start()

    line_q = [ghost[0], ghost[1]] + [cells[c] for c in range(3)]
    fl = rim_fluxes(line_q, (cells[3], cells[4]))
    edge[0] = den[0] + (fl[0] - fl[1])
    edge[1] = den[1] + fl[1]
    mean[0] = jnp.sum(sums[0:1]) / count
    mean[1] = jnp.sum(sums[1:2]) / count
    rest = [
        pltpu.make_async_copy(mean, totals, sem.at[3]),
        pltpu.make_async_copy(edge, out_d.at[0:2], sem.at[4]),
    ]
    for c in rest:
        c.start()
    pltpu.make_async_copy(den.at[2:nx], out_d.at[2:nx], sem.at[0]).wait()
    pltpu.make_async_copy(en, out_e, sem.at[1]).wait()
    pltpu.make_async_copy(mom, out_m, sem.at[2]).wait()
    for c in rest:
        c.wait()


def shards(density, momentum, energy, displacement, flags):
    sizes = {a: lax.axis_size(a) for a in AXES}
    nx, ny, nz = density.shape
    tall = ny + 2 * SUB
    per = nz // 4
    parts = -(-6 * nx // per)
    f32, i32 = jnp.float32, jnp.int32
    dma = pltpu.SemaphoreType.DMA
    any_ = pl.BlockSpec(memory_space=pl.ANY)
    hbm = pl.BlockSpec(memory_space=pltpu.HBM)
    vmem = pl.BlockSpec(memory_space=pltpu.VMEM)
    devices = 1
    for a in AXES:
        devices *= sizes[a]
    count = float(nx * ny * nz * devices)
    outputs = tuple(jax.ShapeDtypeStruct(v.shape, f32) for v in (density, momentum, energy))
    results = pl.pallas_call(
        functools.partial(kernel, sizes),
        out_shape=outputs + tuple(
            jax.ShapeDtypeStruct(v, f32) for v in ((2, nz), (2, ny, nz), (5, ny, nz))
        ),
        in_specs=[hbm] * 5,
        out_specs=(vmem,) * 6,
        scratch_shapes=[
            pltpu.SMEM((6,), i32),
            pltpu.VMEM((5, nx, tall, nz), f32),
            pltpu.VMEM((2, nx, ny, nz), i32),
            pltpu.VMEM((nx, tall, nz), i32),
            pltpu.VMEM((2, 5, 2, ny, nz), f32),
            pltpu.VMEM((3, 2, ny, nz), f32),
            pltpu.VMEM((ny, nz), i32),
        ]
        + [pltpu.VMEM((parts, ny, nz), f32) for _ in range(5)]
        + [pltpu.VMEM((2, nz), f32), pltpu.VMEM((sizes["gx"] * sizes["gz"], 2, nz), f32)]
        + [pltpu.VMEM((sizes["gy"], 2, nz), f32), pltpu.VMEM((2, nz), f32)]
        + [dma((7 + (sizes["gz"] > 2),)), dma((14 + (sizes["gz"] > 2),)), pltpu.SemaphoreType.REGULAR((4,)), dma((2,)), dma((2,))],
        compiler_params=pltpu.CompilerParams(
            collective_id=0, has_side_effects=True, vmem_limit_bytes=12 << 20
        ),
    )(
        *(
            pltpu.with_memory_space_constraint(v, pltpu.HBM)
            for v in (flags, density, momentum, energy, displacement)
        )
    )
    return pl.pallas_call(
        functools.partial(put, count),
        out_shape=outputs + (jax.ShapeDtypeStruct((2,), f32),),
        in_specs=[vmem, any_, any_, vmem, vmem, vmem],
        out_specs=(hbm, hbm, hbm, hbm),
        scratch_shapes=[pltpu.VMEM((2, ny, nz), f32), pltpu.SMEM((2,), f32), dma((5,))],
        compiler_params=pltpu.CompilerParams(vmem_limit_bytes=2 << 20),
    )(*results)


def solution(mesh):
    return jax.shard_map(
        shards,
        mesh=mesh,
        in_specs=(
            P("gx", "gy", "gz"),
            P(None, "gx", "gy", "gz"),
            P("gx", "gy", "gz"),
            P(None, "gx", "gy", "gz"),
            P(),
        ),
        out_specs=(P("gx", "gy", "gz"), P(None, "gx", "gy", "gz"), P("gx", "gy", "gz"), P()),
        check_vma=False,
    )
```
